32 devices in a mesh: dp: 4 (over y, z), sp: 8 (over x, core).
Axes of the slice: x: 4, y: 2, z: 2, core: 2. Of those that a mesh axis runs over, the one named last changes fastest.
The devices are a block of a 4x4x8 slice.
Arguments:
- dec_hidden: bfloat16 [4096, 768], P(('dp', 'sp')), parts along dimension 0
- enc_memory: bfloat16 [32768, 768], P(('dp', 'sp')), parts along dimension 0
- mem_len: int32 [4], P('dp'), parts along dimension 0
- norm_self: bfloat16 [2, 768], replicated
- norm_cross: bfloat16 [2, 768], replicated
- norm_mlp: bfloat16 [2, 768], replicated
- self_q: bfloat16 [2, 768, 768], replicated
- self_k: bfloat16 [2, 768, 768], replicated
- self_v: bfloat16 [2, 768, 768], replicated
- self_o: bfloat16 [2, 12, 64, 768], replicated
- cross_q: bfloat16 [2, 768, 768], replicated
- cross_k: bfloat16 [2, 768, 768], replicated
- cross_v: bfloat16 [2, 768, 768], replicated
- cross_o: bfloat16 [2, 12, 64, 768], replicated
- mlp_gate: bfloat16 [2, 768, 3072], replicated
- mlp_up: bfloat16 [2, 768, 3072], replicated
- mlp_down: bfloat16 [2, 3072, 768], replicated
Outputs:
- output: bfloat16 [4096, 768], P(('dp', 'sp')), parts along dimension 0
There are 4 independent parts. The reference program is written for one: setup_inputs(seed, part) draws one part's arguments, and reference() takes and returns one part's arrays. A program takes and returns all parts, laid end to end along the dimension named above; an argument that names none is the same for every part.
All inputs are finite; a program needn't handle non-finite values.
Results may differ from the reference program's by a relative error of at most 0.0154436.
Values are sent between devices in bfloat16 or wider.
A program may use at most 768 MiB of HBM per device.

```python
import jax
import jax.numpy as jnp
from jax import lax

D = 768
HEADS = 12
KV_HEADS = 12
HEAD = 64
FF = 3072
LAYERS = 2
TQ = 1024
TM = 8192
WAVES = 4
EPS = 1e-6
NEG_BIG = -1e30
SOFT_SCALE = HEAD ** -0.5
DKV = KV_HEADS * HEAD


def smooth_field(wave_key, n_rows, n_cols):
    directions = jax.random.normal(wave_key, (WAVES, n_cols), jnp.float32)
    positions = jnp.arange(n_rows, dtype=jnp.float32) / n_rows
    freq_list = jnp.arange(1, WAVES + 1, dtype=jnp.float32)
    wave_rows = jnp.cos(jnp.pi * positions[:, None] * freq_list[None, :])
    return jnp.dot(wave_rows, directions)


def setup_inputs(seed: int = 0, part: int = 0) -> dict:
    part_key = jax.random.fold_in(jax.random.key(seed), part)
    part_keys = jax.random.split(part_key, 5)
    shared = jax.random.split(jax.random.key(seed + 1), 16)

    def weight(key_index, shape_tail, fan_in):
        raw_draw = jax.random.normal(shared[key_index], (LAYERS,) + shape_tail, jnp.float32)
        return (raw_draw * fan_in ** -0.5).astype(jnp.bfloat16)

    def gain(key_index):
        return jax.random.uniform(shared[key_index], (LAYERS, D), jnp.float32, 0.5, 1.5).astype(jnp.bfloat16)

    dec_hidden = jax.random.normal(part_keys[0], (TQ, D), jnp.float32) + smooth_field(part_keys[1], TQ, D)
    enc_memory = jax.random.normal(part_keys[2], (TM, D), jnp.float32) + smooth_field(part_keys[3], TM, D)
    mem_len = jax.random.randint(part_keys[4], (1,), TM // 4, 3 * TM // 4 + 1, dtype=jnp.int32)
    return {
        'dec_hidden': dec_hidden.astype(jnp.bfloat16),
        'enc_memory': enc_memory.astype(jnp.bfloat16),
        'mem_len': mem_len,
        'norm_self': gain(0),
        'norm_cross': gain(1),
        'norm_mlp': gain(2),
        'self_q': weight(3, (D, D), D),
        'self_k': weight(4, (D, D), D),
        'self_v': weight(5, (D, D), D),
        'self_o': weight(6, (HEADS, HEAD, D), D),
        'cross_q': weight(7, (D, D), D),
        'cross_k': weight(8, (D, DKV), D),
        'cross_v': weight(9, (D, DKV), D),
        'cross_o': weight(10, (HEADS, HEAD, D), D),
        'mlp_gate': weight(11, (D, FF), D),
        'mlp_up': weight(12, (D, FF), D),
        'mlp_down': weight(13, (FF, D), FF),
    }


def rms_norm(hidden, gain_vec):
    hidden32 = hidden.astype(jnp.float32)
    inv_rms = lax.rsqrt(jnp.mean(hidden32 * hidden32, axis=-1, keepdims=True) + EPS)
    return (hidden32 * inv_rms * gain_vec.astype(jnp.float32)).astype(jnp.bfloat16)


def project(acts, weight_mat):
    return jnp.dot(acts, weight_mat, preferred_element_type=jnp.float32).astype(jnp.bfloat16)


def add_residual(hidden, update):
    return (hidden.astype(jnp.float32) + update).astype(jnp.bfloat16)


def head_attend(query_h, key_h, value_h, allowed):
    scores = jnp.dot(query_h, key_h.T, preferred_element_type=jnp.float32) * SOFT_SCALE
    scores = jnp.where(allowed, scores, NEG_BIG)
    weights = jnp.exp(scores - jnp.max(scores, axis=-1, keepdims=True))
    numerator = jnp.dot(weights.astype(jnp.bfloat16), value_h, preferred_element_type=jnp.float32)
    return numerator / jnp.sum(weights, axis=-1, keepdims=True)


def multi_head(queries, keys_all, values_all, allowed):
    q_rows = queries.shape[0]
    k_rows = keys_all.shape[0]
    kv_count = keys_all.shape[1] // HEAD
    q_heads = queries.reshape(q_rows, HEADS, HEAD).transpose(1, 0, 2)
    k_heads = jnp.repeat(keys_all.reshape(k_rows, kv_count, HEAD).transpose(1, 0, 2), HEADS // kv_count, axis=0)
    v_heads = jnp.repeat(values_all.reshape(k_rows, kv_count, HEAD).transpose(1, 0, 2), HEADS // kv_count, axis=0)
    per_head = lax.map(lambda head_trio: head_attend(head_trio[0], head_trio[1], head_trio[2], allowed), (q_heads, k_heads, v_heads))
    return per_head.transpose(1, 0, 2).astype(jnp.bfloat16)


def reference(dec_hidden, enc_memory, mem_len, norm_self, norm_cross, norm_mlp, self_q, self_k, self_v, self_o, cross_q, cross_k, cross_v, cross_o, mlp_gate, mlp_up, mlp_down):
    causal = jnp.arange(TQ)[:, None] >= jnp.arange(TQ)[None, :]
    mem_valid = (jnp.arange(TM) < mem_len[0])[None, :]
    stacked = {
        'norm_self': norm_self, 'norm_cross': norm_cross, 'norm_mlp': norm_mlp,
        'self_q': self_q, 'self_k': self_k, 'self_v': self_v, 'self_o': self_o,
        'cross_q': cross_q, 'cross_k': cross_k, 'cross_v': cross_v, 'cross_o': cross_o,
        'mlp_gate': mlp_gate, 'mlp_up': mlp_up, 'mlp_down': mlp_down,
    }

    def layer_step(hidden, params):
        normed = rms_norm(hidden, params['norm_self'])
        attended = multi_head(project(normed, params['self_q']), project(normed, params['self_k']), project(normed, params['self_v']), causal)
        update = jnp.einsum('thd,hdo->to', attended.astype(jnp.float32), params['self_o'].astype(jnp.float32))
        hidden = add_residual(hidden, update)
        normed = rms_norm(hidden, params['norm_cross'])
        attended = multi_head(project(normed, params['cross_q']), project(enc_memory, params['cross_k']), project(enc_memory, params['cross_v']), mem_valid)
        update = jnp.einsum('thd,hdo->to', attended.astype(jnp.float32), params['cross_o'].astype(jnp.float32))
        hidden = add_residual(hidden, update)
        normed = rms_norm(hidden, params['norm_mlp'])
        gate_pre = jnp.dot(normed, params['mlp_gate'], preferred_element_type=jnp.float32)
        up_proj = jnp.dot(normed, params['mlp_up'], preferred_element_type=jnp.float32)
        hidden_act = (jax.nn.silu(gate_pre) * up_proj).astype(jnp.bfloat16)
        update = jnp.dot(hidden_act, params['mlp_down'], preferred_element_type=jnp.float32)
        return add_residual(hidden, update), None

    final_hidden, _ = lax.scan(layer_step, dec_hidden, stacked)
    return final_hidden
```

```python
import functools

import jax
import jax.numpy as jnp
from jax import lax
from jax.experimental import pallas as pl
from jax.experimental.pallas import tpu as pltpu
from jax.sharding import PartitionSpec as P

EPS = 1e-6
NEG_BIG = -1e30
LOG2E = 1.4426950408889634
F32 = jnp.float32
BF16 = jnp.bfloat16
MESH = pl.DeviceIdType.MESH


def rms_norm(hidden, gain_vec):
    hidden32 = hidden.astype(F32)
    inv_rms = lax.rsqrt(jnp.mean(hidden32 * hidden32, axis=-1, keepdims=True) + EPS)
    return (hidden32 * inv_rms * gain_vec.astype(F32)).astype(BF16)


def mm(a, b):
    return jnp.dot(a, b, preferred_element_type=F32)


def mm_nt(a, b):
    return lax.dot_general(a, b, (((1,), (1,)), ((), ())), preferred_element_type=F32)


def decoder_kernel(dims, *refs):
    (n_chips, layers, rows, width, heads, head_dim, mem_rows, ffl) = dims
    (hid_in, mem_in, mem_len, norm_self, norm_cross, norm_mlp,
     w_sq, w_sk, w_sv, w_so, w_cq, w_ck, w_cv, w_co, w_g, w_u, w_d, out,
     wsq, wsk, wsv, wso, wcq, wck, wcv, wco, wg, wu, wd,
     hbuf, mbuf, ybuf, wvt, qself, kself, vself, kc, vc, qc, s_even, s_odd,
     own_o, own_st, res_s, st_s, res_r, st_r, att, mlp_s, mlp_r,
     w_sem, l_sem, h_ss, h_rs, m_ss, m_rs, a_ss, a_rs, q_ss, q_rs, r_ss, r_rs, f_ss, f_rs) = refs
    T = 2 * rows
    half_w = width // 2
    hl = heads // 2
    pairs = hl // 2
    half = rows // 2
    mem_all = 2 * mem_rows
    exp_c = head_dim ** -0.5 * LOG2E
    neg = NEG_BIG * head_dim ** 0.5

    me = lax.axis_index("sp")
    c = me // 2
    h = me % 2
    sib = c * 2 + (1 - h)

    def peer(step):
        return lax.rem(c + step, n_chips) * 2 + h

    right, left, across = peer(1), peer(n_chips - 1), peer(2)
    back = (None, left, right, across)
    mirror = (0, 2, 1, 3)
    chip_of = (c, lax.rem(c + n_chips - 1, n_chips), lax.rem(c + 1, n_chips), lax.rem(c + 2, n_chips))

    def remote(src, dst, ss, rs, dev):
        return pltpu.make_async_remote_copy(src_ref=src, dst_ref=dst, send_sem=ss, recv_sem=rs,
                                            device_id={"sp": dev}, device_id_type=MESH)

    my_rows = pl.ds(pl.multiple_of(h * rows, rows), rows)
    sib_rows = pl.ds(pl.multiple_of((1 - h) * rows, rows), rows)
    my_a = pl.ds(pl.multiple_of(h * rows, half), half)
    my_b = pl.ds(pl.multiple_of(h * rows + half, half), half)
    my_cols = pl.ds(pl.multiple_of(h * half_w, 128), half_w)
    my_ff = pl.ds(pl.multiple_of(h * ffl, 128), ffl)

    hid_cp = pltpu.make_async_copy(hid_in, hbuf.at[0, 0, my_rows], l_sem.at[0])
    mem_cp = pltpu.make_async_copy(mem_in, mbuf.at[0], l_sem.at[1])
    hid_cp.start()
    mem_cp.start()

    plans = (
        (w_ck, wck, "c"), (w_cv, wcv, "c"), (w_sq, wsq, "c"), (w_sk, wsk, "c"), (w_sv, wsv, "c"), (w_so, wso, "f"),
        (w_cq, wcq, "c"), (w_co, wco, "f"), (w_g, wg, "m"), (w_u, wu, "m"), (w_d, wd, "r"),
    )
    CK, CV, SQ, SK, SV, SO, CQ, CO, G, U, DN = range(11)

    def w_copy(k, l):
        src, dst, kind = plans[k]
        if kind == "c":
            s = src.at[l, :, my_cols]
        elif kind == "m":
            s = src.at[l, :, my_ff]
        elif kind == "r":
            s = src.at[l, my_ff]
        else:
            s = src.at[l]
        return pltpu.make_async_copy(s, dst.at[l], w_sem.at[l, k])

    for l0 in range(layers):
        for k in range(len(plans)):
            w_copy(k, l0).start()

    barrier = pltpu.get_barrier_semaphore()
    for dev in (sib, right, left, across):
        pl.semaphore_signal(barrier, inc=1, device_id={"sp": dev}, device_id_type=MESH)
    pl.semaphore_wait(barrier, 4)

    def h_copy(l, k):
        spec = (
            (0, my_rows, 0, sib),
            (0, my_rows, 1, right),
            (0, my_rows, 2, left),
            (1, my_rows, 1, sib),
            (2, my_rows, 2, sib),
            (1, my_a, 3, right),
            (2, my_b, 3, left),
            (3, my_a, 3, sib),
            (3, my_b, 3, sib),
        )[k]
        s, rr, d, dev = spec
        return remote(hbuf.at[l, s, rr], hbuf.at[l, d, rr], h_ss.at[l, k], h_rs.at[l, k], dev)

    def h_recv(l, k):
        spec = ((0, sib_rows), (1, my_rows), (2, my_rows), (1, sib_rows), (2, sib_rows), (3, my_a), (3, my_b))
        if k < 7:
            s, rr = spec[k]
        else:
            off = (1 - h) * rows + (half if k == 8 else 0)
            s, rr = 3, pl.ds(pl.multiple_of(off, half), half)
        ref = hbuf.at[l, s, rr]
        return remote(ref, ref, h_ss.at[l, k], h_rs.at[l, k], sib)

    mem_send = remote(mbuf.at[0], mbuf.at[1], m_ss, m_rs, sib)

    def att_copy(l, k):
        ref = att.at[l, k, my_cols]
        return remote(ref, ref, a_ss.at[l, k], a_rs.at[l, k], sib)

    def q_copy(l, k):
        dev = (None, right, left, across)[k]
        return remote(qc.at[l, 0], qc.at[l, k], q_ss.at[l, k], q_rs.at[l, k], dev)

    def r_copy(l, k):
        return remote(res_s.at[l, k], res_r.at[l, mirror[k]], r_ss.at[l, 0, k], r_rs.at[l, 0, mirror[k]], back[k])

    def st_copy(l, k):
        return remote(st_s.at[l, k], st_r.at[l, mirror[k]], r_ss.at[l, 1, k], r_rs.at[l, 1, mirror[k]], back[k])

    def mlp_copy(l):
        return remote(mlp_s.at[l, sib_rows], mlp_r.at[l], f_ss.at[l], f_rs.at[l], sib)

    def attend(qref, kref, vref, nk, allowed, put):
        big = 512
        small = 256

        def rhs_of(pair, odd):
            start = pl.multiple_of(pair * 2 * head_dim + odd * head_dim, head_dim)
            q = qref[pl.ds(start, head_dim), :]
            z = jnp.zeros_like(q)
            return jnp.concatenate([z, q] if odd else [q, z], axis=0)

        def score(pair, rhs, s_ref, j, top):
            s = mm(kref[pair, j * big:(j + 1) * big, :], rhs)
            s = jnp.where(allowed(j * big, big), s, neg)
            s_ref[j * big:(j + 1) * big, :] = s
            t = jnp.max(s.reshape(big // 8, 8, T), axis=0)
            return t if top is None else jnp.maximum(top, t)

        def accumulate(head, s_ref, j, top, total, o):
            p = jnp.exp2((s_ref[j * small:(j + 1) * small, :] - top) * exp_c)
            t = jnp.sum(p.reshape(small // 8, 8, T), axis=0)
            v = mm(vref[head, :, j * small:(j + 1) * small], p.astype(BF16))
            return (t, v) if total is None else (total + t, o + v)

        def step(next_pair, next_odd, next_ref, head, cur_ref, cur_top):
            rhs = rhs_of(next_pair, next_odd)
            top = total = o = None
            for j in range(nk // big):
                top = score(next_pair, rhs, next_ref, j, top)
                for i in range(big // small):
                    total, o = accumulate(head, cur_ref, j * (big // small) + i, cur_top, total, o)
            put(head, o, cur_top, jnp.sum(total, axis=0, keepdims=True))
            return jnp.max(top, axis=0, keepdims=True)

        rhs0 = rhs_of(0, 0)
        top = None
        for j in range(nk // big):
            top = score(0, rhs0, s_even, j, top)
        top = jnp.max(top, axis=0, keepdims=True)

        def pair_body(pair, top_even):
            top_odd = step(pair, 1, s_odd, 2 * pair, s_even, top_even)
            return step(jnp.minimum(pair + 1, pairs - 1), 0, s_even, 2 * pair + 1, s_odd, top_odd)

        lax.fori_loop(0, pairs, pair_body, top)

    def gain(ref, l):
        g = ref[0:1, :].astype(F32)
        for i in range(1, layers):
            g = jnp.where(l == i, ref[i:i + 1, :].astype(F32), g)
        return g

    def project_t(x, w):
        return mm(x, w).astype(BF16).T

    def layer(l, carry):
        first = l == 0
        @pl.when(first)
        def _():
            hid_cp.wait()

        for k in range(3):
            h_copy(l, k).start()

        @pl.when(first)
        def _():
            mem_cp.wait()
            mem_send.start()

        w_copy(CK, l).wait()
        w_copy(CV, l).wait()
        wvt[...] = wcv[l].T
        blk = 512

        def mem_proj(part):
            def body(b, cc):
                r0 = pl.multiple_of(b * blk, blk)
                m = mbuf[part, pl.ds(r0, blk), :]
                k = mm(m, wck[l]).astype(BF16)
                d0 = pl.multiple_of(part * mem_rows + b * blk, blk)
                for p in range(pairs):
                    kc[p, pl.ds(d0, blk), :] = k[:, p * 128:(p + 1) * 128]
                v = mm_nt(wvt[...], m).astype(BF16)
                vc[:, :, pl.ds(d0, blk)] = v.reshape(hl, head_dim, blk)
                return cc

            lax.fori_loop(0, mem_rows // blk, body, 0)

        mem_proj(0)

        @pl.when(first)
        def _():
            mem_send.wait_recv()

        mem_proj(1)

        g_self = gain(norm_self, l)
        for k in (SQ, SK, SV):
            w_copy(k, l).wait()
        wvt[...] = wsv[l].T

        def self_proj(r, with_q):
            x = rms_norm(hbuf[l, r], g_self)
            if with_q:
                qself[...] = project_t(x, wsq[l])
            k = mm(x, wsk[l]).astype(BF16)
            for p in range(pairs):
                kself[p, r * T:(r + 1) * T, :] = k[:, p * 128:(p + 1) * 128]
            v = mm_nt(wvt[...], x).astype(BF16)
            vself[:, :, r * T:(r + 1) * T] = v.reshape(hl, head_dim, T)

        h_recv(l, 1).wait_recv()
        h_copy(l, 3).start()
        h_copy(l, 5).start()
        h_recv(l, 2).wait_recv()
        h_copy(l, 4).start()
        h_copy(l, 6).start()
        h_recv(l, 0).wait_recv()
        self_proj(0, True)
        h_recv(l, 3).wait_recv()
        self_proj(1, False)
        h_recv(l, 4).wait_recv()
        self_proj(2, False)
        h_recv(l, 5).wait_recv()
        h_copy(l, 7).start()
        h_recv(l, 6).wait_recv()
        h_copy(l, 8).start()
        h_recv(l, 7).wait_recv()
        h_recv(l, 8).wait_recv()
        self_proj(3, False)

        def causal(start, size):
            parts = []
            kio = lax.broadcasted_iota(jnp.int32, (T, T), 0)
            qio = lax.broadcasted_iota(jnp.int32, (T, T), 1)
            for r in range(start // T, (start + size) // T):
                parts.append(kio + (chip_of[r] - c) * T <= qio)
            return jnp.concatenate(parts, axis=0)

        def put_self(head, o, top, total):
            r0 = pl.multiple_of(h * half_w + head * head_dim, head_dim)
            att[l, 0, pl.ds(r0, head_dim), :] = (o / total).astype(BF16)

        attend(qself, kself, vself, n_chips * T, causal, put_self)
        att_copy(l, 0).start()
        w_copy(SO, l).wait()
        w_copy(CQ, l).wait()
        att_copy(l, 0).wait_recv()
        y = (hbuf[l, 0].astype(F32) + mm(att[l, 0].T, wso[l])).astype(BF16)
        ybuf[...] = y

        x = rms_norm(y, gain(norm_cross, l))
        qc[l, 0] = project_t(x, wcq[l])
        for k in range(1, 4):
            q_copy(l, k).start()
        limit = mem_len[0]

        def valid(start, size):
            core = h if start < mem_rows else 1 - h
            base = (2 * c + core) * mem_rows + start % mem_rows
            return lax.broadcasted_iota(jnp.int32, (size, T), 0) < limit - base

        def put_own(head, o, top, total):
            own_o[pl.ds(pl.multiple_of(head * head_dim, head_dim), head_dim), :] = o
            own_st[pl.ds(head, 1), :] = top
            own_st[pl.ds(8 + head, 1), :] = total

        attend(qc.at[l, 0], kc, vc, mem_all, valid, put_own)
        for r in (1, 2, 3):
            def put_far(head, o, top, total, r=r):
                res_s[l, r, pl.ds(pl.multiple_of(head * head_dim, head_dim), head_dim), :] = o.astype(BF16)
                st_s[l, r, pl.ds(head, 1), :] = top
                st_s[l, r, pl.ds(8 + head, 1), :] = total

            q_copy(l, r).wait_recv()
            attend(qc.at[l, r], kc, vc, mem_all, valid, put_far)
            r_copy(l, r).start()
            st_copy(l, r).start()

        for r in (1, 2, 3):
            r_copy(l, mirror[r]).wait_recv()
            st_copy(l, mirror[r]).wait_recv()
        for head in range(hl):
            hs = slice(head * head_dim, (head + 1) * head_dim)
            tops = [own_st[head:head + 1, :]] + [st_r[l, r, head:head + 1, :] for r in (1, 2, 3)]
            sums = [own_st[8 + head:9 + head, :]] + [st_r[l, r, 8 + head:9 + head, :] for r in (1, 2, 3)]
            nums = [own_o[hs, :]] + [res_r[l, r, hs, :].astype(F32) for r in (1, 2, 3)]
            top = functools.reduce(jnp.maximum, tops)
            scale = [jnp.exp2((t - top) * exp_c) for t in tops]
            den = sum(s * t for s, t in zip(scale, sums))
            num = sum(s * t for s, t in zip(scale, nums))
            r0 = pl.multiple_of(h * half_w + head * head_dim, head_dim)
            att[l, 1, pl.ds(r0, head_dim), :] = (num / den).astype(BF16)
        att_copy(l, 1).start()
        w_copy(CO, l).wait()
        w_copy(G, l).wait()
        w_copy(U, l).wait()
        w_copy(DN, l).wait()
        att_copy(l, 1).wait_recv()
        y = (ybuf[...].astype(F32) + mm(att[l, 1].T, wco[l])).astype(BF16)
        ybuf[...] = y

        x = rms_norm(y, gain(norm_mlp, l))
        step = 512
        acc = None
        for s in range(ffl // step):
            sl = slice(s * step, (s + 1) * step)
            gate = mm(x, wg[l, :, sl])
            act = (jax.nn.silu(gate) * mm(x, wu[l, :, sl])).astype(BF16)
            part = mm(act, wd[l, sl, :])
            acc = part if acc is None else acc + part
        mlp_s[l] = acc
        mlp_copy(l).start()
        mlp_copy(l).wait_recv()
        hbuf[l + 1, 0, my_rows, :] = (ybuf[my_rows, :].astype(F32) + (mlp_s[l, my_rows, :] + mlp_r[l])).astype(BF16)
        return carry

    lax.fori_loop(0, layers, layer, 0)
    out_cp = pltpu.make_async_copy(hbuf.at[layers, 0, my_rows], out, l_sem.at[2])
    out_cp.start()

    mem_send.wait_send()

    def drain(l, carry):
        for k in range(9):
            h_copy(l, k).wait_send()
        for k in range(2):
            att_copy(l, k).wait_send()
        for k in range(1, 4):
            q_copy(l, k).wait_send()
            r_copy(l, k).wait_send()
            st_copy(l, k).wait_send()
        mlp_copy(l).wait_send()
        return carry

    lax.fori_loop(0, layers, drain, 0)
    out_cp.wait()


def solution(mesh):
    group = mesh.shape["sp"]
    n_chips = group // 2
    row_spec = P(("dp", "sp"), None)

    def local_step(hidden, memory, mem_len, norm_self, norm_cross, norm_mlp, self_q, self_k, self_v, self_o, cross_q, cross_k, cross_v, cross_o, mlp_gate, mlp_up, mlp_down):
        rows, width = hidden.shape
        mem_rows = memory.shape[0]
        layers, heads, head_dim = self_o.shape[:3]
        ffl = mlp_gate.shape[2] // 2
        half_w = width // 2
        hl = heads // 2
        pairs = hl // 2
        T = 2 * rows
        mem_all = 2 * mem_rows
        wso = self_o.reshape(layers, heads * head_dim, width)
        wco = cross_o.reshape(layers, heads * head_dim, width)
        dims = (n_chips, layers, rows, width, heads, head_dim, mem_rows, ffl)
        dma = pltpu.SemaphoreType.DMA
        anyspace = pl.BlockSpec(memory_space=pl.ANY)
        vmem = pl.BlockSpec(memory_space=pltpu.VMEM)
        call = pl.pallas_call(
            functools.partial(decoder_kernel, dims),
            out_shape=jax.ShapeDtypeStruct(hidden.shape, BF16),
            in_specs=[anyspace, anyspace, pl.BlockSpec(memory_space=pltpu.SMEM)] + [vmem] * 3 + [anyspace] * 11,
            out_specs=anyspace,
            scratch_shapes=[
                pltpu.VMEM((layers, width, half_w), BF16),
                pltpu.VMEM((layers, width, half_w), BF16),
                pltpu.VMEM((layers, width, half_w), BF16),
                pltpu.VMEM((layers, width, width), BF16),
                pltpu.VMEM((layers, width, half_w), BF16),
                pltpu.VMEM((layers, width, half_w), BF16),
                pltpu.VMEM((layers, width, half_w), BF16),
                pltpu.VMEM((layers, width, width), BF16),
                pltpu.VMEM((layers, width, ffl), BF16),
                pltpu.VMEM((layers, width, ffl), BF16),
                pltpu.VMEM((layers, ffl, width), BF16),
                pltpu.VMEM((layers + 1, n_chips, T, width), BF16),
                pltpu.VMEM((2, mem_rows, width), BF16),
                pltpu.VMEM((T, width), BF16),
                pltpu.VMEM((half_w, width), BF16),
                pltpu.VMEM((half_w, T), BF16),
                pltpu.VMEM((pairs, n_chips * T, 128), BF16),
                pltpu.VMEM((hl, head_dim, n_chips * T), BF16),
                pltpu.VMEM((pairs, mem_all, 128), BF16),
                pltpu.VMEM((hl, head_dim, mem_all), BF16),
                pltpu.VMEM((layers, 4, half_w, T), BF16),
                pltpu.VMEM((mem_all, T), F32),
                pltpu.VMEM((mem_all, T), F32),
                pltpu.VMEM((half_w, T), F32),
                pltpu.VMEM((16, T), F32),
                pltpu.VMEM((layers, 4, half_w, T), BF16),
                pltpu.VMEM((layers, 4, 16, T), F32),
                pltpu.VMEM((layers, 4, half_w, T), BF16),
                pltpu.VMEM((layers, 4, 16, T), F32),
                pltpu.VMEM((layers, 2, width, T), BF16),
                pltpu.VMEM((layers, T, width), F32),
                pltpu.VMEM((layers, rows, width), F32),
                dma((layers, 11)),
                dma((3,)),
                dma((layers, 9)), dma((layers, 9)),
                dma, dma,
                dma((layers, 2)), dma((layers, 2)),
                dma((layers, 4)), dma((layers, 4)),
                dma((layers, 2, 4)), dma((layers, 2, 4)),
                dma((layers,)), dma((layers,)),
            ],
            compiler_params=pltpu.CompilerParams(collective_id=0, has_side_effects=True, vmem_limit_bytes=67043328),
            name="decoder",
        )
        return call(hidden, memory, mem_len, norm_self, norm_cross, norm_mlp, self_q, self_k, self_v, wso, cross_q, cross_k, cross_v, wco, mlp_gate, mlp_up, mlp_down)

    return jax.shard_map(local_step, mesh=mesh, in_specs=(row_spec, row_spec, P("dp")) + (P(),) * 14, out_specs=row_spec, check_vma=False)
```

```python
import functools

import jax
import jax.numpy as jnp
from jax import lax
from jax.experimental import pallas as pl
from jax.experimental.pallas import tpu as pltpu
from jax.sharding import PartitionSpec as P

EPS = 1e-6
NEG_BIG = -1e30
LOG2E = 1.4426950408889634
F32 = jnp.float32
BF16 = jnp.bfloat16
MESH = pl.DeviceIdType.MESH
BIG = 512
SMALL = 256


def rms_norm(hidden, gain_vec):
    hidden32 = hidden.astype(F32)
    inv_rms = lax.rsqrt(jnp.mean(hidden32 * hidden32, axis=-1, keepdims=True) + EPS)
    return (hidden32 * inv_rms * gain_vec.astype(F32)).astype(BF16)


def mm(a, b):
    return jnp.dot(a, b, preferred_element_type=F32)


def mm_nt(a, b):
    return lax.dot_general(a, b, (((1,), (1,)), ((), ())), preferred_element_type=F32)


def decoder_kernel(dims, *refs):
    (n_chips, layers, rows, width, heads, head_dim, mem_rows, ffl) = dims
    (hid_in, mem_in, len_in, ns_in, nc_in, nm_in,
     w_sq, w_sk, w_sv, w_so, w_cq, w_ck, w_cv, w_co, w_g, w_u, w_d, out,
     wsq, wsk, wsv, wso, wcq, wck, wcv, wco, wg, wu, wd, norm_self, norm_cross, norm_mlp, mem_len,
     hbuf, mbuf, ybuf, wvt, qself, kself, vself, kc, vc, qc, s_even, s_odd,
     res_s, st_s, res_r, st_r, att, act, mlp_s, mlp_r,
     w_sem, l_sem, h_ss, h_rs, m_ss, m_rs, a_ss, a_rs, q_ss, q_rs, r_ss, r_rs, f_ss, f_rs) = refs
    T = 2 * rows
    half_w = width // 2
    hl = heads // 2
    pairs = hl // 2
    half = rows // 2
    pw = 2 * head_dim
    mem_all = 2 * mem_rows
    exp_c = head_dim ** -0.5 * LOG2E
    neg = NEG_BIG * LOG2E

    me = lax.axis_index("sp")
    c = me // 2
    h = me % 2
    sib = c * 2 + (1 - h)

    def peer(step):
        return lax.rem(c + step, n_chips) * 2 + h

    right, left, across = peer(1), peer(n_chips - 1), peer(2)
    chip_of = (c, lax.rem(c + n_chips - 1, n_chips), lax.rem(c + 1, n_chips), lax.rem(c + 2, n_chips))

    def remote(src, dst, ss, rs, dev):
        return pltpu.make_async_remote_copy(src_ref=src, dst_ref=dst, send_sem=ss, recv_sem=rs,
                                            device_id={"sp": dev}, device_id_type=MESH)

    def piece(core, part):
        return pl.ds(pl.multiple_of(core * rows + part * half, half), half)

    my_rows = pl.ds(pl.multiple_of(h * rows, rows), rows)
    sib_rows = pl.ds(pl.multiple_of((1 - h) * rows, rows), rows)
    my_cols = pl.ds(pl.multiple_of(h * half_w, 128), half_w)
    my_ff = pl.ds(pl.multiple_of(h * ffl, 128), ffl)

    plans = (
        (w_ck, wck, "c"), (w_cv, wcv, "c"), (w_sk, wsk, "c"), (w_sv, wsv, "c"), (w_sq, wsq, "c"), (w_so, wso, "f"),
        (w_cq, wcq, "c"), (w_co, wco, "f"), (w_g, wg, "m"), (w_u, wu, "m"), (w_d, wd, "r"),
    )
    CK, CV, SK, SV, SQ, SO, CQ, CO, G, U, DN = range(11)

    def w_copy(k, l):
        src, dst, kind = plans[k]
        if kind == "c":
            s = src.at[l, :, my_cols]
        elif kind == "m":
            s = src.at[l, :, my_ff]
        elif kind == "r":
            s = src.at[l, my_ff]
        else:
            s = src.at[l]
        return pltpu.make_async_copy(s, dst.at[l], w_sem.at[l, k])

    hid_cp = pltpu.make_async_copy(hid_in, hbuf.at[0, 0, my_rows], l_sem.at[0])
    mem_cp = pltpu.make_async_copy(mem_in, mbuf.at[0], l_sem.at[1])
    small = [pltpu.make_async_copy(s, d, l_sem.at[3 + i]) for i, (s, d) in enumerate(
        ((ns_in, norm_self), (nc_in, norm_cross), (nm_in, norm_mlp), (len_in, mem_len)))]
    hid_cp.start()
    mem_cp.start()
    w_copy(CK, 0).start()
    w_copy(CV, 0).start()
    for cp in small:
        cp.start()

    barrier = pltpu.get_barrier_semaphore()
    for dev in (sib, right, left, across):
        pl.semaphore_signal(barrier, inc=1, device_id={"sp": dev}, device_id_type=MESH)
    pl.semaphore_wait(barrier, 4)

    h_plan = (
        (0, 0, None, sib),
        (0, 1, 0, right), (0, 2, 1, left), (0, 1, 1, right), (0, 2, 0, left),
        (1, 3, 0, right), (2, 3, 1, left),
        (1, 1, None, sib), (2, 2, None, sib), (3, 3, 0, sib), (3, 3, 1, sib),
    )
    n_h = len(h_plan)

    def h_copy(l, k):
        s, d, part, dev = h_plan[k]
        rr = my_rows if part is None else piece(h, part)
        return remote(hbuf.at[l, s, rr], hbuf.at[l, d, rr], h_ss.at[l, k], h_rs.at[l, k], dev)

    def h_wait(l, k):
        s, d, part, dev = h_plan[k]
        core = 1 - h if k in (0, 7, 8, 9, 10) else h
        rr = pl.ds(pl.multiple_of(core * rows, rows), rows) if part is None else piece(core, part)
        ref = hbuf.at[l, d, rr]
        remote(ref, ref, h_ss.at[l, k], h_rs.at[l, k], sib).wait_recv()

    mem_send = remote(mbuf.at[0], mbuf.at[1], m_ss, m_rs, sib)

    def att_copy(l, k, p):
        ref = att.at[l, k, pl.ds(pl.multiple_of(h * half_w + p * pw, pw), pw)]
        return remote(ref, ref, a_ss.at[l, k, p], a_rs.at[l, k, p], sib)

    def att_wait(l, k, p):
        ref = att.at[l, k, pl.ds(pl.multiple_of((1 - h) * half_w + p * pw, pw), pw)]
        remote(ref, ref, a_ss.at[l, k, p], a_rs.at[l, k, p], sib).wait_recv()

    def pair_rows(p):
        return pl.ds(pl.multiple_of(p * pw, pw), pw)

    def q_copy(l, k, p):
        dev = (None, right, left, across)[k]
        return remote(qc.at[l, 0, pair_rows(p)], qc.at[l, k, pair_rows(p)], q_ss.at[l, k, p], q_rs.at[l, k, p], dev)

    def q_wait(l, k, p):
        ref = qc.at[l, k, pair_rows(p)]
        remote(ref, ref, q_ss.at[l, k, p], q_rs.at[l, k, p], sib).wait_recv()

    def r_copies(l, k, p):
        k = jnp.int32(k)
        step = jnp.where(k == 1, n_chips - 1, jnp.where(k == 2, 1, 2))
        slot = jnp.where(k == 1, 2, jnp.where(k == 2, 1, 3))
        dev = peer(step)
        return (remote(res_s.at[l, k, pair_rows(p)], res_r.at[l, slot, pair_rows(p)], r_ss.at[l, 0, k, p], r_rs.at[l, 0, slot, p], dev),
                remote(st_s.at[l, k, p], st_r.at[l, slot, p], r_ss.at[l, 1, k, p], r_rs.at[l, 1, slot, p], dev))

    def r_wait(l, k, p):
        a, b = res_r.at[l, k, pair_rows(p)], st_r.at[l, k, p]
        remote(a, a, r_ss.at[l, 0, k, p], r_rs.at[l, 0, k, p], sib).wait_recv()
        remote(b, b, r_ss.at[l, 1, k, p], r_rs.at[l, 1, k, p], sib).wait_recv()

    def mlp_copy(l):
        return remote(mlp_s.at[l], mlp_r.at[l], f_ss.at[l], f_rs.at[l], sib)

    def attend(items, item, qref, kref, vref, nk, allowed, before, put, after):
        def rhs_of(t, odd):
            block, pair = item(t)
            start = pl.multiple_of(pair * pw + odd * head_dim, head_dim)
            q = qref[block, pl.ds(start, head_dim), :].astype(F32) * exp_c
            hi = q.astype(BF16)
            lo = (q - hi.astype(F32)).astype(BF16)
            z = jnp.zeros_like(hi)
            return jnp.concatenate([z, hi, z, lo] if odd else [hi, z, lo, z], axis=0)

        def score(pair, rhs, s_ref, j, top):
            k = kref[pair, j * BIG:(j + 1) * BIG, :]
            s = mm(jnp.concatenate([k, k], axis=1), rhs)
            s = jnp.where(allowed(j * BIG, BIG), s, neg)
            s_ref[j * BIG:(j + 1) * BIG, :] = s
            t = jnp.max(s.reshape(BIG // 8, 8, T), axis=0)
            return t if top is None else jnp.maximum(top, t)

        def accumulate(head, s_ref, j, top, total, o):
            p = jnp.exp2(s_ref[j * SMALL:(j + 1) * SMALL, :] - top)
            t = jnp.sum(p.reshape(SMALL // 8, 8, T), axis=0)
            vt = jnp.concatenate([vref[head, j * (SMALL // 128) + i] for i in range(SMALL // 128)], axis=1)
            v = mm(vt, p.astype(BF16))
            return (t, v) if total is None else (total + t, o + v)

        def step(nxt, nxt_odd, nxt_ref, cur, cur_odd, cur_ref, cur_top):
            rhs = rhs_of(nxt, nxt_odd)
            nxt_pair = item(nxt)[1]
            head = item(cur)[1] * 2 + cur_odd
            top = total = o = None
            for j in range(nk // BIG):
                top = score(nxt_pair, rhs, nxt_ref, j, top)
                for i in range(BIG // SMALL):
                    total, o = accumulate(head, cur_ref, j * (BIG // SMALL) + i, cur_top, total, o)
            put(cur, cur_odd, o, cur_top, jnp.sum(total, axis=0, keepdims=True))
            return jnp.max(top, axis=0, keepdims=True)

        before(0)
        rhs0 = rhs_of(0, 0)
        top = None
        for j in range(nk // BIG):
            top = score(item(0)[1], rhs0, s_even, j, top)
        top = jnp.max(top, axis=0, keepdims=True)

        def body(t, top_even):
            last = t == items - 1
            nxt = jnp.where(last, t, t + 1)

            @pl.when(jnp.logical_not(last))
            def _():
                before(t + 1)

            top_odd = step(t, 1, s_odd, t, 0, s_even, top_even)
            top_next = step(nxt, 0, s_even, t, 1, s_odd, top_odd)
            after(t)
            return top_next

        lax.fori_loop(0, items, body, top)

    def gain(ref, l):
        g = ref[0:1, :].astype(F32)
        for i in range(1, layers):
            g = jnp.where(l == i, ref[i:i + 1, :].astype(F32), g)
        return g

    def store_kv(kref, vref, row0, tile0, k, v, n):
        for p in range(pairs):
            kref[p, pl.ds(row0, n), :] = k[:, p * pw:(p + 1) * pw]
        v = v.reshape(hl, head_dim, n)
        for i in range(n // 128):
            vref[:, pl.ds(tile0 + i, 1)] = v[:, None, :, i * 128:(i + 1) * 128]

    def layer(l, carry):
        first = l == 0
        with jax.named_scope("gather_send"):
            @pl.when(first)
            def _():
                hid_cp.wait()

            for k in range(5):
                h_copy(l, k).start()

            @pl.when(first)
            def _():
                mem_cp.wait()
                mem_send.start()
                for l0 in range(layers):
                    for k in range(len(plans)):
                        if l0 > 0 or k > CV:
                            w_copy(k, l0).start()

        with jax.named_scope("w_wait"):
            w_copy(CK, l).wait()
            w_copy(CV, l).wait()
            wvt[...] = wcv[l].T

        blk = 512

        def mem_proj(part):
            def body(b, cc):
                r0 = pl.multiple_of(b * blk, blk)
                m = mbuf[part, pl.ds(r0, blk), :]
                k = mm(m, wck[l]).astype(BF16)
                v = mm_nt(wvt[...], m).astype(BF16)
                d0 = pl.multiple_of(part * mem_rows + b * blk, blk)
                store_kv(kc, vc, d0, (part * mem_rows + b * blk) // 128, k, v, blk)
                return cc

            lax.fori_loop(0, mem_rows // blk, body, 0)

        with jax.named_scope("mem_proj0"):
            mem_proj(0)

            @pl.when(first)
            def _():
                mem_send.wait_recv()
                for cp in small:
                    cp.wait()

        with jax.named_scope("mem_proj1"):
            mem_proj(1)

        def self_proj(r, with_q):
            x = rms_norm(hbuf[l, r], gain(norm_self, l))
            k = mm(x, wsk[l]).astype(BF16)
            v = mm_nt(wvt[...], x).astype(BF16)
            store_kv(kself, vself, r * T, r * (T // 128), k, v, T)
            if with_q:
                qself[0] = mm(x, wsq[l]).astype(BF16).T

        with jax.named_scope("gather_wait1"):
            for k in (SK, SV, SQ):
                w_copy(k, l).wait()
            wvt[...] = wsv[l].T
            h_wait(l, 1)
            h_copy(l, 5).start()
            h_wait(l, 2)
            h_copy(l, 6).start()
            h_wait(l, 0)
        with jax.named_scope("self_proj0"):
            self_proj(0, True)
        with jax.named_scope("gather_wait2"):
            h_wait(l, 3)
            h_copy(l, 7).start()
            h_wait(l, 4)
            h_copy(l, 8).start()
            h_wait(l, 7)
        with jax.named_scope("self_proj1"):
            self_proj(1, False)
            h_wait(l, 8)
            self_proj(2, False)
        with jax.named_scope("gather_wait3"):
            h_wait(l, 5)
            h_copy(l, 9).start()
            h_wait(l, 6)
            h_copy(l, 10).start()
            h_wait(l, 9)
            h_wait(l, 10)
        with jax.named_scope("self_proj3"):
            self_proj(3, False)

        def causal(start, size):
            parts = []
            kio = lax.broadcasted_iota(jnp.int32, (T, T), 0)
            qio = lax.broadcasted_iota(jnp.int32, (T, T), 1)
            for r in range(start // T, (start + size) // T):
                parts.append(kio + (chip_of[r] - c) * T <= qio)
            return jnp.concatenate(parts, axis=0)

        def att_rows(t, odd):
            return pl.ds(pl.multiple_of(h * half_w + t * pw + odd * head_dim, head_dim), head_dim)

        def put_self(t, odd, o, top, total):
            att[l, 0, att_rows(t, odd), :] = (o / total).astype(BF16)

        with jax.named_scope("self_attend"):
            attend(pairs, lambda t: (0, t), qself, kself, vself, n_chips * T, causal, lambda t: None, put_self,
                   lambda t: att_copy(l, 0, t).start())
        with jax.named_scope("att0_exchange"):
            w_copy(SO, l).wait()
            w_copy(CQ, l).wait()
            for p in range(pairs):
                att_wait(l, 0, p)
        with jax.named_scope("self_o_q"):
            y = (hbuf[l, 0].astype(F32) + mm(att[l, 0].T, wso[l])).astype(BF16)
            ybuf[...] = y
            x = rms_norm(y, gain(norm_cross, l))
            qc[l, 0] = mm(x, wcq[l]).astype(BF16).T
            for p in range(pairs):
                for k in (1, 2):
                    q_copy(l, k, p).start()
            for p in range(pairs):
                q_copy(l, 3, p).start()

        limit = mem_len[0]

        def valid(start, size):
            core = h if start < mem_rows else 1 - h
            base = (2 * c + core) * mem_rows + start % mem_rows
            return lax.broadcasted_iota(jnp.int32, (size, T), 0) < limit - base

        n_items = 4 * pairs
        lead = pairs - 1

        def item(t):
            t = jnp.int32(t)
            u = t - lead
            far = jnp.logical_and(t >= lead, t < n_items - 1)
            block = jnp.where(far, 1 + u // pairs, 0)
            pair = jnp.where(far, u % pairs, jnp.where(t == n_items - 1, pairs - 1, t))
            return block, pair

        def before(t):
            block, pair = item(t)
            for k in (1, 2, 3):
                @pl.when(block == k)
                def _():
                    q_wait(l, k, pair)

        def put_cross(t, odd, o, top, total):
            block, pair = item(t)
            res_s[l, block, pl.ds(pl.multiple_of(pair * pw + odd * head_dim, head_dim), head_dim), :] = o.astype(BF16)
            st_s[l, block, pair, odd:odd + 1, :] = top
            st_s[l, block, pair, 2 + odd:3 + odd, :] = total

        def after(t):
            block, pair = item(t)

            @pl.when(block > 0)
            def _():
                for cp in r_copies(l, block, pair):
                    cp.start()

        with jax.named_scope("cross"):
            attend(n_items, item, qc.at[l], kc, vc, mem_all, valid, before, put_cross, after)

        for p in range(pairs):
            with jax.named_scope(f"res_wait{p}"):
                for r in (1, 2, 3):
                    r_wait(l, r, p)
            with jax.named_scope(f"combine{p}"):
                for odd in (0, 1):
                    hs = slice(p * pw + odd * head_dim, p * pw + (odd + 1) * head_dim)
                    tops = [st_s[l, 0, p, odd:odd + 1, :]] + [st_r[l, r, p, odd:odd + 1, :] for r in (1, 2, 3)]
                    sums = [st_s[l, 0, p, 2 + odd:3 + odd, :]] + [st_r[l, r, p, 2 + odd:3 + odd, :] for r in (1, 2, 3)]
                    nums = [res_s[l, 0, hs, :].astype(F32)] + [res_r[l, r, hs, :].astype(F32) for r in (1, 2, 3)]
                    top = functools.reduce(jnp.maximum, tops)
                    scale = [jnp.exp2(t - top) for t in tops]
                    den = sum(s * t for s, t in zip(scale, sums))
                    num = sum(s * t for s, t in zip(scale, nums))
                    att[l, 1, att_rows(p, odd), :] = (num / den).astype(BF16)
                att_copy(l, 1, p).start()
        with jax.named_scope("att1_exchange"):
            w_copy(CO, l).wait()
            w_copy(G, l).wait()
            w_copy(U, l).wait()
            w_copy(DN, l).wait()
            for p in range(pairs):
                att_wait(l, 1, p)
        with jax.named_scope("mlp"):
            y = (ybuf[...].astype(F32) + mm(att[l, 1].T, wco[l])).astype(BF16)
            ybuf[...] = y
            x = rms_norm(y, gain(norm_mlp, l))
            step = 512
            for s in range(ffl // step):
                sl = slice(s * step, (s + 1) * step)
                gate = mm(x, wg[l, :, sl])
                act[:, sl] = (jax.nn.silu(gate) * mm(x, wu[l, :, sl])).astype(BF16)
            mlp_s[l] = mm(act[sib_rows, :], wd[l])
            mlp_copy(l).start()
            mine = mm(act[my_rows, :], wd[l])
        with jax.named_scope("mlp_exchange"):
            remote(mlp_s.at[l], mlp_r.at[l], f_ss.at[l], f_rs.at[l], sib).wait_recv()
            hbuf[l + 1, 0, my_rows, :] = (ybuf[my_rows, :].astype(F32) + (mine + mlp_r[l])).astype(BF16)
        return carry

    lax.fori_loop(0, layers, layer, 0)
    out_cp = pltpu.make_async_copy(hbuf.at[layers, 0, my_rows], out, l_sem.at[2])
    out_cp.start()

    mem_send.wait_send()

    def drain(l, carry):
        for k in range(n_h):
            h_copy(l, k).wait_send()
        for p in range(pairs):
            for k in range(2):
                att_copy(l, k, p).wait_send()
            for k in range(1, 4):
                q_copy(l, k, p).wait_send()
                for cp in r_copies(l, k, p):
                    cp.wait_send()
        mlp_copy(l).wait_send()
        return carry

    lax.fori_loop(0, layers, drain, 0)
    out_cp.wait()


def solution(mesh):
    group = mesh.shape["sp"]
    n_chips = group // 2
    row_spec = P(("dp", "sp"), None)

    def local_step(hidden, memory, mem_len, norm_self, norm_cross, norm_mlp, self_q, self_k, self_v, self_o, cross_q, cross_k, cross_v, cross_o, mlp_gate, mlp_up, mlp_down):
        rows, width = hidden.shape
        mem_rows = memory.shape[0]
        layers, heads, head_dim = self_o.shape[:3]
        ffl = mlp_gate.shape[2] // 2
        half_w = width // 2
        hl = heads // 2
        pairs = hl // 2
        T = 2 * rows
        mem_all = 2 * mem_rows
        wso = self_o.reshape(layers, heads * head_dim, width)
        wco = cross_o.reshape(layers, heads * head_dim, width)
        dims = (n_chips, layers, rows, width, heads, head_dim, mem_rows, ffl)
        dma = pltpu.SemaphoreType.DMA
        anyspace = pl.BlockSpec(memory_space=pl.ANY)
        call = pl.pallas_call(
            functools.partial(decoder_kernel, dims),
            out_shape=jax.ShapeDtypeStruct(hidden.shape, BF16),
            in_specs=[anyspace] * 17,
            out_specs=anyspace,
            scratch_shapes=[
                pltpu.VMEM((layers, width, half_w), BF16),
                pltpu.VMEM((layers, width, half_w), BF16),
                pltpu.VMEM((layers, width, half_w), BF16),
                pltpu.VMEM((layers, width, width), BF16),
                pltpu.VMEM((layers, width, half_w), BF16),
                pltpu.VMEM((layers, width, half_w), BF16),
                pltpu.VMEM((layers, width, half_w), BF16),
                pltpu.VMEM((layers, width, width), BF16),
                pltpu.VMEM((layers, width, ffl), BF16),
                pltpu.VMEM((layers, width, ffl), BF16),
                pltpu.VMEM((layers, ffl, width), BF16),
                pltpu.VMEM((layers, width), BF16),
                pltpu.VMEM((layers, width), BF16),
                pltpu.VMEM((layers, width), BF16),
                pltpu.SMEM((1,), jnp.int32),
                pltpu.VMEM((layers + 1, n_chips, T, width), BF16),
                pltpu.VMEM((2, mem_rows, width), BF16),
                pltpu.VMEM((T, width), BF16),
                pltpu.VMEM((half_w, width), BF16),
                pltpu.VMEM((1, half_w, T), BF16),
                pltpu.VMEM((pairs, n_chips * T, 128), BF16),
                pltpu.VMEM((hl, n_chips * T // 128, head_dim, 128), BF16),
                pltpu.VMEM((pairs, mem_all, 128), BF16),
                pltpu.VMEM((hl, mem_all // 128, head_dim, 128), BF16),
                pltpu.VMEM((layers, 4, half_w, T), BF16),
                pltpu.VMEM((mem_all, T), F32),
                pltpu.VMEM((mem_all, T), F32),
                pltpu.VMEM((layers, 4, half_w, T), BF16),
                pltpu.VMEM((layers, 4, pairs, 8, T), F32),
                pltpu.VMEM((layers, 4, half_w, T), BF16),
                pltpu.VMEM((layers, 4, pairs, 8, T), F32),
                pltpu.VMEM((layers, 2, width, T), BF16),
                pltpu.VMEM((T, ffl), BF16),
                pltpu.VMEM((layers, rows, width), F32),
                pltpu.VMEM((layers, rows, width), F32),
                dma((layers, 11)),
                dma((7,)),
                dma((layers, 11)), dma((layers, 11)),
                dma, dma,
                dma((layers, 2, pairs)), dma((layers, 2, pairs)),
                dma((layers, 4, pairs)), dma((layers, 4, pairs)),
                dma((layers, 2, 4, pairs)), dma((layers, 2, 4, pairs)),
                dma((layers,)), dma((layers,)),
            ],
            compiler_params=pltpu.CompilerParams(collective_id=0, has_side_effects=True, vmem_limit_bytes=67043328),
            name="decoder",
        )
        return call(hidden, memory, mem_len, norm_self, norm_cross, norm_mlp, self_q, self_k, self_v, wso, cross_q, cross_k, cross_v, wco, mlp_gate, mlp_up, mlp_down)

    return jax.shard_map(local_step, mesh=mesh, in_specs=(row_spec, row_spec, P("dp")) + (P(),) * 14, out_specs=row_spec, check_vma=False)
```

```python
import functools

import jax
import jax.numpy as jnp
from jax import lax
from jax.experimental import pallas as pl
from jax.experimental.pallas import tpu as pltpu
from jax.sharding import PartitionSpec as P

EPS = 1e-6
NEG_BIG = -1e30
LOG2E = 1.4426950408889634
F32 = jnp.float32
BF16 = jnp.bfloat16
CB, CS = 1024, 256
MESH = pl.DeviceIdType.MESH


def rms_norm(hidden, gain_vec):
    hidden32 = hidden.astype(F32)
    inv_rms = lax.rsqrt(jnp.mean(hidden32 * hidden32, axis=-1, keepdims=True) + EPS)
    return (hidden32 * inv_rms * gain_vec.astype(F32)).astype(BF16)


def mm(a, b):
    return jnp.dot(a, b, preferred_element_type=F32)


def mm_nt(a, b):
    return lax.dot_general(a, b, (((1,), (1,)), ((), ())), preferred_element_type=F32)


def decoder_kernel(dims, *refs):
    (n_chips, layers, rows, width, heads, head_dim, mem_rows, ffl) = dims
    (hid_in, mem_in, len_in, ns_in, nc_in, nm_in,
     w_sq, w_sk, w_sv, w_so, w_cq, w_ck, w_cv, w_co, w_g, w_u, w_d, out,
     wsq, wsk, wsv, wso, wcq, wck, wcv, wco, wg, wu, wd, norm_self, norm_cross, norm_mlp, mem_len,
     hbuf, mbuf, ybuf, wvt, qself, kself, vself, kc, vc, qc, s_even, s_odd,
     res_s, st_s, res_r, st_r, att, act, mlp_s, mlp_r,
     w_sem, l_sem, h_ss, h_rs, m_ss, m_rs, a_ss, a_rs, q_ss, q_rs, r_ss, r_rs, f_ss, f_rs) = refs
    T = 2 * rows
    half_w = width // 2
    hl = heads // 2
    pairs = hl // 2
    half = rows // 2
    pw = 2 * head_dim
    mem_all = 2 * mem_rows
    exp_c = head_dim ** -0.5 * LOG2E
    neg = NEG_BIG * LOG2E

    me = lax.axis_index("sp")
    c = me // 2
    h = me % 2
    sib = c * 2 + (1 - h)

    def peer(step):
        return lax.rem(c + step, n_chips) * 2 + h

    right, left, across = peer(1), peer(n_chips - 1), peer(2)
    chip_of = (c, lax.rem(c + n_chips - 1, n_chips), lax.rem(c + 1, n_chips), lax.rem(c + 2, n_chips))

    def remote(src, dst, ss, rs, dev):
        return pltpu.make_async_remote_copy(src_ref=src, dst_ref=dst, send_sem=ss, recv_sem=rs,
                                            device_id={"sp": dev}, device_id_type=MESH)

    def piece(core, part):
        return pl.ds(pl.multiple_of(core * rows + part * half, half), half)

    my_rows = pl.ds(pl.multiple_of(h * rows, rows), rows)
    sib_rows = pl.ds(pl.multiple_of((1 - h) * rows, rows), rows)
    my_cols = pl.ds(pl.multiple_of(h * half_w, 128), half_w)
    my_ff = pl.ds(pl.multiple_of(h * ffl, 128), ffl)

    plans = (
        (w_ck, wck, "c"), (w_cv, wcv, "c"), (w_sk, wsk, "c"), (w_sv, wsv, "c"), (w_sq, wsq, "c"), (w_so, wso, "f"),
        (w_cq, wcq, "c"), (w_co, wco, "f"), (w_g, wg, "m"), (w_u, wu, "m"), (w_d, wd, "r"),
    )
    CK, CV, SK, SV, SQ, SO, CQ, CO, G, U, DN = range(11)

    def w_copy(k, l):
        src, dst, kind = plans[k]
        if kind == "c":
            s = src.at[l, :, my_cols]
        elif kind == "m":
            s = src.at[l, :, my_ff]
        elif kind == "r":
            s = src.at[l, my_ff]
        else:
            s = src.at[l]
        return pltpu.make_async_copy(s, dst.at[l], w_sem.at[l, k])

    hid_cp = pltpu.make_async_copy(hid_in, hbuf.at[0, 0, my_rows], l_sem.at[0])
    mem_cp = pltpu.make_async_copy(mem_in, mbuf.at[0], l_sem.at[1])
    small = [pltpu.make_async_copy(s, d, l_sem.at[3 + i]) for i, (s, d) in enumerate(
        ((ns_in, norm_self), (nc_in, norm_cross), (nm_in, norm_mlp), (len_in, mem_len)))]
    hid_cp.start()
    mem_cp.start()
    w_copy(CK, 0).start()
    w_copy(CV, 0).start()
    for cp in small:
        cp.start()

    barrier = pltpu.get_barrier_semaphore()
    for dev in (sib, right, left, across):
        pl.semaphore_signal(barrier, inc=1, device_id={"sp": dev}, device_id_type=MESH)
    pl.semaphore_wait(barrier, 4)

    h_plan = (
        (0, 0, None, sib),
        (0, 1, 0, right), (0, 2, 1, left), (0, 1, 1, right), (0, 2, 0, left),
        (1, 3, 0, right), (2, 3, 1, left),
        (1, 1, None, sib), (2, 2, None, sib), (3, 3, 0, sib), (3, 3, 1, sib),
    )
    n_h = len(h_plan)

    def h_copy(l, k):
        s, d, part, dev = h_plan[k]
        rr = my_rows if part is None else piece(h, part)
        return remote(hbuf.at[l, s, rr], hbuf.at[l, d, rr], h_ss.at[l, k], h_rs.at[l, k], dev)

    def h_wait(l, k):
        s, d, part, dev = h_plan[k]
        core = 1 - h if k in (0, 7, 8, 9, 10) else h
        rr = pl.ds(pl.multiple_of(core * rows, rows), rows) if part is None else piece(core, part)
        ref = hbuf.at[l, d, rr]
        remote(ref, ref, h_ss.at[l, k], h_rs.at[l, k], sib).wait_recv()

    mem_send = remote(mbuf.at[0], mbuf.at[1], m_ss, m_rs, sib)

    def att_copy(l, k, p):
        ref = att.at[l, k, pl.ds(pl.multiple_of(h * half_w + p * pw, pw), pw)]
        return remote(ref, ref, a_ss.at[l, k, p], a_rs.at[l, k, p], sib)

    def att_wait(l, k, p):
        ref = att.at[l, k, pl.ds(pl.multiple_of((1 - h) * half_w + p * pw, pw), pw)]
        remote(ref, ref, a_ss.at[l, k, p], a_rs.at[l, k, p], sib).wait_recv()

    def pair_rows(p):
        return pl.ds(pl.multiple_of(p * pw, pw), pw)

    def q_copy(l, k, p):
        dev = (None, right, left, across)[k]
        return remote(qc.at[l, 0, pair_rows(p)], qc.at[l, k, pair_rows(p)], q_ss.at[l, k, p], q_rs.at[l, k, p], dev)

    def q_wait(l, k, p):
        ref = qc.at[l, k, pair_rows(p)]
        remote(ref, ref, q_ss.at[l, k, p], q_rs.at[l, k, p], sib).wait_recv()

    def r_copies(l, k, p):
        k = jnp.int32(k)
        step = jnp.where(k == 1, n_chips - 1, jnp.where(k == 2, 1, 2))
        slot = jnp.where(k == 1, 2, jnp.where(k == 2, 1, 3))
        dev = peer(step)
        return (remote(res_s.at[l, k, pair_rows(p)], res_r.at[l, slot, pair_rows(p)], r_ss.at[l, 0, k, p], r_rs.at[l, 0, slot, p], dev),
                remote(st_s.at[l, k, p], st_r.at[l, slot, p], r_ss.at[l, 1, k, p], r_rs.at[l, 1, slot, p], dev))

    def r_wait(l, k, p):
        a, b = res_r.at[l, k, pair_rows(p)], st_r.at[l, k, p]
        remote(a, a, r_ss.at[l, 0, k, p], r_rs.at[l, 0, k, p], sib).wait_recv()
        remote(b, b, r_ss.at[l, 1, k, p], r_rs.at[l, 1, k, p], sib).wait_recv()

    def mlp_copy(l):
        return remote(mlp_s.at[l], mlp_r.at[l], f_ss.at[l], f_rs.at[l], sib)

    def attend(BIG, SMALL, items, item, qref, kref, vref, nk, allowed, keep, finish, before, put, after):
        def rhs_of(t, odd):
            block, pair = item(t)
            start = pl.multiple_of(pair * pw + odd * head_dim, head_dim)
            q = qref[block, pl.ds(start, head_dim), :].astype(F32) * exp_c
            hi = q.astype(BF16)
            lo = (q - hi.astype(F32)).astype(BF16)
            z = jnp.zeros_like(hi)
            return jnp.concatenate([z, hi, z, lo] if odd else [hi, z, lo, z], axis=0)

        def score(pair, rhs, s_ref, j, top):
            k = kref[pair, j * BIG:(j + 1) * BIG, :]
            s = mm(jnp.concatenate([k, k], axis=1), rhs)
            if allowed is not None:
                s = jnp.where(allowed(j * BIG, BIG), s, neg)
            s_ref[j * BIG:(j + 1) * BIG, :] = s
            t = jnp.max(s.reshape(BIG // 8, 8, T), axis=0)
            return t if top is None else jnp.maximum(top, t)

        def accumulate(head, s_ref, j, top, total, o):
            p = jnp.exp2(s_ref[j * SMALL:(j + 1) * SMALL, :] - top)
            t = jnp.sum(p.reshape(SMALL // 8, 8, T), axis=0)
            if keep is not None:
                t = t * keep(j * SMALL, SMALL)
            vt = jnp.concatenate([vref[head, j * (SMALL // 128) + i] for i in range(SMALL // 128)], axis=1)
            v = mm(vt, p.astype(BF16))
            return (t, v) if total is None else (total + t, o + v)

        def step(nxt, nxt_odd, nxt_ref, cur, cur_odd, cur_ref, cur_top):
            rhs = rhs_of(nxt, nxt_odd)
            nxt_pair = item(nxt)[1]
            head = item(cur)[1] * 2 + cur_odd
            top = total = o = None
            for j in range(nk // BIG):
                top = score(nxt_pair, rhs, nxt_ref, j, top)
                for i in range(BIG // SMALL):
                    total, o = accumulate(head, cur_ref, j * (BIG // SMALL) + i, cur_top, total, o)
            total = jnp.sum(total, axis=0, keepdims=True)
            if finish is not None:
                cur_top, total = finish(cur_ref, cur_top, total)
            put(cur, cur_odd, o, cur_top, total)
            return jnp.max(top, axis=0, keepdims=True)

        before(0)
        rhs0 = rhs_of(0, 0)
        top = None
        for j in range(nk // BIG):
            top = score(item(0)[1], rhs0, s_even, j, top)
        top = jnp.max(top, axis=0, keepdims=True)

        def body(t, top_even):
            last = t == items - 1
            nxt = jnp.where(last, t, t + 1)

            @pl.when(jnp.logical_not(last))
            def _():
                before(t + 1)

            top_odd = step(t, 1, s_odd, t, 0, s_even, top_even)
            top_next = step(nxt, 0, s_even, t, 1, s_odd, top_odd)
            after(t)
            return top_next

        lax.fori_loop(0, items, body, top)

    def gain(ref, l):
        g = ref[0:1, :].astype(F32)
        for i in range(1, layers):
            g = jnp.where(l == i, ref[i:i + 1, :].astype(F32), g)
        return g

    def store_kv(kref, vref, row0, tile0, k, v, n):
        for p in range(pairs):
            kref[p, pl.ds(row0, n), :] = k[:, p * pw:(p + 1) * pw]
        v = v.reshape(hl, head_dim, n)
        for i in range(n // 128):
            vref[:, pl.ds(tile0 + i, 1)] = v[:, None, :, i * 128:(i + 1) * 128]

    def layer(l, carry):
        first = l == 0
        with jax.named_scope("gather_send"):
            @pl.when(first)
            def _():
                hid_cp.wait()

            for k in range(5):
                h_copy(l, k).start()

            @pl.when(first)
            def _():
                mem_cp.wait()
                mem_send.start()
                for l0 in range(layers):
                    for k in range(len(plans)):
                        if l0 > 0 or k > CV:
                            w_copy(k, l0).start()

        with jax.named_scope("w_wait"):
            w_copy(CK, l).wait()
            w_copy(CV, l).wait()
            wvt[...] = wcv[l].T

        blk = 512

        def mem_proj(part):
            core = h if part == 0 else 1 - h

            def body(b, cc):
                r0 = pl.multiple_of(b * blk, blk)
                m = mbuf[part, pl.ds(r0, blk), :]
                left_valid = limit - ((2 * c + core) * mem_rows + b * blk)
                m = jnp.where(lax.broadcasted_iota(jnp.int32, (blk, width), 0) < left_valid, m, mbuf[h, 0:1, :])
                k = mm(m, wck[l]).astype(BF16)
                v = mm_nt(wvt[...], m)
                v = jnp.where(lax.broadcasted_iota(jnp.int32, (half_w, blk), 1) < left_valid, v, 0.0).astype(BF16)
                d0 = pl.multiple_of(part * mem_rows + b * blk, blk)
                store_kv(kc, vc, d0, (part * mem_rows + b * blk) // 128, k, v, blk)
                return cc

            lax.fori_loop(0, mem_rows // blk, body, 0)

        with jax.named_scope("mem_wait"):
            @pl.when(first)
            def _():
                mem_send.wait_recv()
                for cp in small:
                    cp.wait()

        limit = mem_len[0]
        with jax.named_scope("mem_proj0"):
            mem_proj(0)

        with jax.named_scope("mem_proj1"):
            mem_proj(1)

        def self_proj(r, with_q):
            x = rms_norm(hbuf[l, r], gain(norm_self, l))
            k = mm(x, wsk[l]).astype(BF16)
            v = mm_nt(wvt[...], x).astype(BF16)
            store_kv(kself, vself, r * T, r * (T // 128), k, v, T)
            if with_q:
                qself[0] = mm(x, wsq[l]).astype(BF16).T

        with jax.named_scope("gather_wait1"):
            for k in (SK, SV, SQ):
                w_copy(k, l).wait()
            wvt[...] = wsv[l].T
            h_wait(l, 1)
            h_copy(l, 5).start()
            h_wait(l, 2)
            h_copy(l, 6).start()
            h_wait(l, 0)
        with jax.named_scope("self_proj0"):
            self_proj(0, True)
        with jax.named_scope("gather_wait2"):
            h_wait(l, 3)
            h_copy(l, 7).start()
            h_wait(l, 4)
            h_copy(l, 8).start()
            h_wait(l, 7)
        with jax.named_scope("self_proj1"):
            self_proj(1, False)
            h_wait(l, 8)
            self_proj(2, False)
        with jax.named_scope("gather_wait3"):
            h_wait(l, 5)
            h_copy(l, 9).start()
            h_wait(l, 6)
            h_copy(l, 10).start()
            h_wait(l, 9)
            h_wait(l, 10)
        with jax.named_scope("self_proj3"):
            self_proj(3, False)

        def causal(start, size):
            parts = []
            kio = lax.broadcasted_iota(jnp.int32, (T, T), 0)
            qio = lax.broadcasted_iota(jnp.int32, (T, T), 1)
            for r in range(start // T, (start + size) // T):
                parts.append(kio + (chip_of[r] - c) * T <= qio)
            return jnp.concatenate(parts, axis=0)

        def att_rows(t, odd):
            return pl.ds(pl.multiple_of(h * half_w + t * pw + odd * head_dim, head_dim), head_dim)

        def put_self(t, odd, o, top, total):
            att[l, 0, att_rows(t, odd), :] = (o / total).astype(BF16)

        with jax.named_scope("self_attend"):
            attend(512, 512, pairs, lambda t: (0, t), qself, kself, vself, n_chips * T, causal, None, None, lambda t: None, put_self,
                   lambda t: att_copy(l, 0, t).start())
        with jax.named_scope("att0_exchange"):
            w_copy(SO, l).wait()
            w_copy(CQ, l).wait()
            for p in range(pairs):
                att_wait(l, 0, p)
        with jax.named_scope("self_o_q"):
            y = (hbuf[l, 0].astype(F32) + mm(att[l, 0].T, wso[l])).astype(BF16)
            ybuf[...] = y
            x = rms_norm(y, gain(norm_cross, l))
            qc[l, 0] = mm(x, wcq[l]).astype(BF16).T
            for p in range(pairs):
                for k in (1, 2):
                    q_copy(l, k, p).start()
            for p in range(pairs):
                q_copy(l, 3, p).start()

        def invalid_in(start, size):
            core = h if start < mem_rows else 1 - h
            end = (2 * c + core) * mem_rows + start % mem_rows + size
            return jnp.clip(end - limit, 0, size)

        def keep(start, size):
            return jnp.where(invalid_in(start, size) < size, 1.0, 0.0).astype(F32)

        extra = jnp.int32(0)
        for start in range(0, mem_all, CS):
            bad = invalid_in(start, CS)
            extra = extra + jnp.where(bad < CS, bad, 0)
        extra = extra.astype(F32)
        any_valid = 2 * c * mem_rows < limit

        def finish(s_ref, top, total):
            first_row = s_ref[pl.ds(pl.multiple_of(h * mem_rows, 8), 1), :]
            total = total - extra * jnp.exp2(first_row - top)
            return jnp.where(any_valid, top, neg), jnp.where(any_valid, total, 0.0)

        n_items = 4 * pairs
        lead = pairs - 1

        def item(t):
            t = jnp.int32(t)
            u = t - lead
            far = jnp.logical_and(t >= lead, t < n_items - 1)
            block = jnp.where(far, 1 + u // pairs, 0)
            pair = jnp.where(far, u % pairs, jnp.where(t == n_items - 1, pairs - 1, t))
            return block, pair

        def before(t):
            block, pair = item(t)
            for k in (1, 2, 3):
                @pl.when(block == k)
                def _():
                    q_wait(l, k, pair)

        def put_cross(t, odd, o, top, total):
            block, pair = item(t)
            res_s[l, block, pl.ds(pl.multiple_of(pair * pw + odd * head_dim, head_dim), head_dim), :] = o.astype(BF16)
            st_s[l, block, pair, odd:odd + 1, :] = top
            st_s[l, block, pair, 2 + odd:3 + odd, :] = total

        def after(t):
            block, pair = item(t)

            @pl.when(block > 0)
            def _():
                for cp in r_copies(l, block, pair):
                    cp.start()

        with jax.named_scope("cross"):
            attend(CB, CS, n_items, item, qc.at[l], kc, vc, mem_all, None, keep, finish, before, put_cross, after)

        for p in range(pairs):
            with jax.named_scope(f"res_wait{p}"):
                for r in (1, 2, 3):
                    r_wait(l, r, p)
            with jax.named_scope(f"combine{p}"):
                for odd in (0, 1):
                    hs = slice(p * pw + odd * head_dim, p * pw + (odd + 1) * head_dim)
                    tops = [st_s[l, 0, p, odd:odd + 1, :]] + [st_r[l, r, p, odd:odd + 1, :] for r in (1, 2, 3)]
                    sums = [st_s[l, 0, p, 2 + odd:3 + odd, :]] + [st_r[l, r, p, 2 + odd:3 + odd, :] for r in (1, 2, 3)]
                    nums = [res_s[l, 0, hs, :].astype(F32)] + [res_r[l, r, hs, :].astype(F32) for r in (1, 2, 3)]
                    top = functools.reduce(jnp.maximum, tops)
                    scale = [jnp.exp2(t - top) for t in tops]
                    den = sum(s * t for s, t in zip(scale, sums))
                    num = sum(s * t for s, t in zip(scale, nums))
                    att[l, 1, att_rows(p, odd), :] = (num / den).astype(BF16)
                att_copy(l, 1, p).start()
        with jax.named_scope("att1_exchange"):
            w_copy(CO, l).wait()
            w_copy(G, l).wait()
            w_copy(U, l).wait()
            w_copy(DN, l).wait()
            for p in range(pairs):
                att_wait(l, 1, p)
        with jax.named_scope("mlp"):
            y = (ybuf[...].astype(F32) + mm(att[l, 1].T, wco[l])).astype(BF16)
            ybuf[...] = y
            x = rms_norm(y, gain(norm_mlp, l))
            step = 512
            for s in range(ffl // step):
                sl = slice(s * step, (s + 1) * step)
                gate = mm(x, wg[l, :, sl])
                act[:, sl] = (jax.nn.silu(gate) * mm(x, wu[l, :, sl])).astype(BF16)
            mlp_s[l] = mm(act[sib_rows, :], wd[l])
            mlp_copy(l).start()
            mine = mm(act[my_rows, :], wd[l])
        with jax.named_scope("mlp_exchange"):
            remote(mlp_s.at[l], mlp_r.at[l], f_ss.at[l], f_rs.at[l], sib).wait_recv()
            hbuf[l + 1, 0, my_rows, :] = (ybuf[my_rows, :].astype(F32) + (mine + mlp_r[l])).astype(BF16)
        return carry

    lax.fori_loop(0, layers, layer, 0)
    out_cp = pltpu.make_async_copy(hbuf.at[layers, 0, my_rows], out, l_sem.at[2])
    out_cp.start()

    mem_send.wait_send()

    def drain(l, carry):
        for k in range(n_h):
            h_copy(l, k).wait_send()
        for p in range(pairs):
            for k in range(2):
                att_copy(l, k, p).wait_send()
            for k in range(1, 4):
                q_copy(l, k, p).wait_send()
                for cp in r_copies(l, k, p):
                    cp.wait_send()
        mlp_copy(l).wait_send()
        return carry

    lax.fori_loop(0, layers, drain, 0)
    out_cp.wait()


def solution(mesh):
    group = mesh.shape["sp"]
    n_chips = group // 2
    row_spec = P(("dp", "sp"), None)

    def local_step(hidden, memory, mem_len, norm_self, norm_cross, norm_mlp, self_q, self_k, self_v, self_o, cross_q, cross_k, cross_v, cross_o, mlp_gate, mlp_up, mlp_down):
        rows, width = hidden.shape
        mem_rows = memory.shape[0]
        layers, heads, head_dim = self_o.shape[:3]
        ffl = mlp_gate.shape[2] // 2
        half_w = width // 2
        hl = heads // 2
        pairs = hl // 2
        T = 2 * rows
        mem_all = 2 * mem_rows
        wso = self_o.reshape(layers, heads * head_dim, width)
        wco = cross_o.reshape(layers, heads * head_dim, width)
        dims = (n_chips, layers, rows, width, heads, head_dim, mem_rows, ffl)
        dma = pltpu.SemaphoreType.DMA
        anyspace = pl.BlockSpec(memory_space=pl.ANY)
        call = pl.pallas_call(
            functools.partial(decoder_kernel, dims),
            out_shape=jax.ShapeDtypeStruct(hidden.shape, BF16),
            in_specs=[anyspace] * 17,
            out_specs=anyspace,
            scratch_shapes=[
                pltpu.VMEM((layers, width, half_w), BF16),
                pltpu.VMEM((layers, width, half_w), BF16),
                pltpu.VMEM((layers, width, half_w), BF16),
                pltpu.VMEM((layers, width, width), BF16),
                pltpu.VMEM((layers, width, half_w), BF16),
                pltpu.VMEM((layers, width, half_w), BF16),
                pltpu.VMEM((layers, width, half_w), BF16),
                pltpu.VMEM((layers, width, width), BF16),
                pltpu.VMEM((layers, width, ffl), BF16),
                pltpu.VMEM((layers, width, ffl), BF16),
                pltpu.VMEM((layers, ffl, width), BF16),
                pltpu.VMEM((layers, width), BF16),
                pltpu.VMEM((layers, width), BF16),
                pltpu.VMEM((layers, width), BF16),
                pltpu.SMEM((1,), jnp.int32),
                pltpu.VMEM((layers + 1, n_chips, T, width), BF16),
                pltpu.VMEM((2, mem_rows, width), BF16),
                pltpu.VMEM((T, width), BF16),
                pltpu.VMEM((half_w, width), BF16),
                pltpu.VMEM((1, half_w, T), BF16),
                pltpu.VMEM((pairs, n_chips * T, 128), BF16),
                pltpu.VMEM((hl, n_chips * T // 128, head_dim, 128), BF16),
                pltpu.VMEM((pairs, mem_all, 128), BF16),
                pltpu.VMEM((hl, mem_all // 128, head_dim, 128), BF16),
                pltpu.VMEM((layers, 4, half_w, T), BF16),
                pltpu.VMEM((mem_all, T), F32),
                pltpu.VMEM((mem_all, T), F32),
                pltpu.VMEM((layers, 4, half_w, T), BF16),
                pltpu.VMEM((layers, 4, pairs, 8, T), F32),
                pltpu.VMEM((layers, 4, half_w, T), BF16),
                pltpu.VMEM((layers, 4, pairs, 8, T), F32),
                pltpu.VMEM((layers, 2, width, T), BF16),
                pltpu.VMEM((T, ffl), BF16),
                pltpu.VMEM((layers, rows, width), F32),
                pltpu.VMEM((layers, rows, width), F32),
                dma((layers, 11)),
                dma((7,)),
                dma((layers, 11)), dma((layers, 11)),
                dma, dma,
                dma((layers, 2, pairs)), dma((layers, 2, pairs)),
                dma((layers, 4, pairs)), dma((layers, 4, pairs)),
                dma((layers, 2, 4, pairs)), dma((layers, 2, 4, pairs)),
                dma((layers,)), dma((layers,)),
            ],
            compiler_params=pltpu.CompilerParams(collective_id=0, has_side_effects=True, vmem_limit_bytes=67043328),
            name="decoder",
        )
        return call(hidden, memory, mem_len, norm_self, norm_cross, norm_mlp, self_q, self_k, self_v, wso, cross_q, cross_k, cross_v, wco, mlp_gate, mlp_up, mlp_down)

    return jax.shard_map(local_step, mesh=mesh, in_specs=(row_spec, row_spec, P("dp")) + (P(),) * 14, out_specs=row_spec, check_vma=False)
```

```python
import functools

import jax
import jax.numpy as jnp
from jax import lax
from jax.experimental import pallas as pl
from jax.experimental.pallas import tpu as pltpu
from jax.sharding import PartitionSpec as P

EPS = 1e-6
NEG_BIG = -1e30
LOG2E = 1.4426950408889634
F32 = jnp.float32
BF16 = jnp.bfloat16
CB, CS = 1024, 256
MESH = pl.DeviceIdType.MESH


def rms_norm(hidden, gain_vec):
    hidden32 = hidden.astype(F32)
    inv_rms = lax.rsqrt(jnp.mean(hidden32 * hidden32, axis=-1, keepdims=True) + EPS)
    return (hidden32 * inv_rms * gain_vec.astype(F32)).astype(BF16)


def mm(a, b):
    return jnp.dot(a, b, preferred_element_type=F32)


def mm_nt(a, b):
    return lax.dot_general(a, b, (((1,), (1,)), ((), ())), preferred_element_type=F32)


def decoder_kernel(dims, *refs):
    (n_chips, layers, rows, width, heads, head_dim, mem_rows, ffl) = dims
    (hid_in, mem_in, len_in, ns_in, nc_in, nm_in,
     w_sq, w_sk, w_sv, w_so, w_cq, w_ck, w_cv, w_co, w_g, w_u, w_d, out,
     wsq, wsk, wsv, wso, wcq, wck, wcv, wco, wg, wu, wd, norm_self, norm_cross, norm_mlp, mem_len,
     hbuf, mbuf, ybuf, wvt, qself, kself, vself, kc, vc, qc, s_even, s_odd,
     res_s, st_s, res_r, st_r, att, act, mlp_s, mlp_r,
     w_sem, l_sem, h_ss, h_rs, m_ss, m_rs, a_ss, a_rs, q_ss, q_rs, r_ss, r_rs, f_ss, f_rs) = refs
    T = 2 * rows
    half_w = width // 2
    hl = heads // 2
    pairs = hl // 2
    half = rows // 2
    pw = 2 * head_dim
    mem_all = 2 * mem_rows
    exp_c = head_dim ** -0.5 * LOG2E
    neg = NEG_BIG * LOG2E

    me = lax.axis_index("sp")
    c = me // 2
    h = me % 2
    sib = c * 2 + (1 - h)

    def peer(step):
        return lax.rem(c + step, n_chips) * 2 + h

    right, left, across = peer(1), peer(n_chips - 1), peer(2)
    chip_of = (c, lax.rem(c + n_chips - 1, n_chips), lax.rem(c + 1, n_chips), lax.rem(c + 2, n_chips))

    def remote(src, dst, ss, rs, dev):
        return pltpu.make_async_remote_copy(src_ref=src, dst_ref=dst, send_sem=ss, recv_sem=rs,
                                            device_id={"sp": dev}, device_id_type=MESH)

    def piece(core, part):
        return pl.ds(pl.multiple_of(core * rows + part * half, half), half)

    my_rows = pl.ds(pl.multiple_of(h * rows, rows), rows)
    sib_rows = pl.ds(pl.multiple_of((1 - h) * rows, rows), rows)
    my_cols = pl.ds(pl.multiple_of(h * half_w, 128), half_w)
    my_ff = pl.ds(pl.multiple_of(h * ffl, 128), ffl)

    plans = (
        (w_ck, wck, "c"), (w_cv, wcv, "c"), (w_sk, wsk, "c"), (w_sv, wsv, "c"), (w_sq, wsq, "c"), (w_so, wso, "f"),
        (w_cq, wcq, "c"), (w_co, wco, "f"), (w_g, wg, "m"), (w_u, wu, "m"), (w_d, wd, "r"),
    )
    CK, CV, SK, SV, SQ, SO, CQ, CO, G, U, DN = range(11)

    def w_copy(k, l):
        src, dst, kind = plans[k]
        if kind == "c":
            s = src.at[l, :, my_cols]
        elif kind == "m":
            s = src.at[l, :, my_ff]
        elif kind == "r":
            s = src.at[l, my_ff]
        else:
            s = src.at[l]
        return pltpu.make_async_copy(s, dst.at[l], w_sem.at[l, k])

    hid_cp = pltpu.make_async_copy(hid_in, hbuf.at[0, 0, my_rows], l_sem.at[0])
    mem_cp = pltpu.make_async_copy(mem_in, mbuf.at[0], l_sem.at[1])
    small = [pltpu.make_async_copy(s, d, l_sem.at[3 + i]) for i, (s, d) in enumerate(
        ((ns_in, norm_self), (nc_in, norm_cross), (nm_in, norm_mlp), (len_in, mem_len)))]
    hid_cp.start()
    mem_cp.start()
    w_copy(CK, 0).start()
    w_copy(CV, 0).start()
    for cp in small:
        cp.start()

    barrier = pltpu.get_barrier_semaphore()
    for dev in (sib, right, left, across):
        pl.semaphore_signal(barrier, inc=1, device_id={"sp": dev}, device_id_type=MESH)
    pl.semaphore_wait(barrier, 4)

    h_plan = (
        (0, 0, None, sib),
        (0, 1, 0, right), (0, 2, 1, left), (0, 1, 1, right), (0, 2, 0, left),
        (1, 3, 0, right), (2, 3, 1, left),
        (1, 1, None, sib), (2, 2, None, sib), (3, 3, 0, sib), (3, 3, 1, sib),
    )
    n_h = len(h_plan)

    def h_copy(l, k):
        s, d, part, dev = h_plan[k]
        rr = my_rows if part is None else piece(h, part)
        return remote(hbuf.at[l, s, rr], hbuf.at[l, d, rr], h_ss.at[l, k], h_rs.at[l, k], dev)

    def h_wait(l, k):
        s, d, part, dev = h_plan[k]
        core = 1 - h if k in (0, 7, 8, 9, 10) else h
        rr = pl.ds(pl.multiple_of(core * rows, rows), rows) if part is None else piece(core, part)
        ref = hbuf.at[l, d, rr]
        remote(ref, ref, h_ss.at[l, k], h_rs.at[l, k], sib).wait_recv()

    mem_send = remote(mbuf.at[0], mbuf.at[1], m_ss, m_rs, sib)

    def att_copy(l, k, p):
        ref = att.at[l, k, pl.ds(pl.multiple_of(h * half_w + p * pw, pw), pw)]
        return remote(ref, ref, a_ss.at[l, k, p], a_rs.at[l, k, p], sib)

    def att_wait(l, k, p):
        ref = att.at[l, k, pl.ds(pl.multiple_of((1 - h) * half_w + p * pw, pw), pw)]
        remote(ref, ref, a_ss.at[l, k, p], a_rs.at[l, k, p], sib).wait_recv()

    def pair_rows(p):
        return pl.ds(pl.multiple_of(p * pw, pw), pw)

    def q_copy(l, k, p):
        dev = (None, right, left)[k]
        return remote(qc.at[l, 0, pair_rows(p)], qc.at[l, k, pair_rows(p)], q_ss.at[l, k, p], q_rs.at[l, k, p], dev)

    def q_relay(l, k, p):
        rr = pl.ds(pl.multiple_of(p * pw + (k - 1) * head_dim, head_dim), head_dim)
        dev = (None, right, left)[k]
        return remote(qc.at[l, k, rr], qc.at[l, 3, rr], q_ss.at[l, 2 + k, p], q_rs.at[l, 2 + k, p], dev)

    def q_relay_wait(l, p):
        for k in (1, 2):
            rr = pl.ds(pl.multiple_of(p * pw + (k - 1) * head_dim, head_dim), head_dim)
            ref = qc.at[l, 3, rr]
            remote(ref, ref, q_ss.at[l, 2 + k, p], q_rs.at[l, 2 + k, p], sib).wait_recv()

    def q_wait(l, k, p):
        ref = qc.at[l, k, pair_rows(p)]
        remote(ref, ref, q_ss.at[l, k, p], q_rs.at[l, k, p], sib).wait_recv()

    def r_copies(l, k, p):
        k = jnp.int32(k)
        step = jnp.where(k == 1, n_chips - 1, jnp.where(k == 2, 1, 2))
        slot = jnp.where(k == 1, 2, jnp.where(k == 2, 1, 3))
        dev = peer(step)
        return (remote(res_s.at[l, k, pair_rows(p)], res_r.at[l, slot, pair_rows(p)], r_ss.at[l, 0, k, p], r_rs.at[l, 0, slot, p], dev),
                remote(st_s.at[l, k, p], st_r.at[l, slot, p], r_ss.at[l, 1, k, p], r_rs.at[l, 1, slot, p], dev))

    def r_wait(l, k, p):
        a, b = res_r.at[l, k, pair_rows(p)], st_r.at[l, k, p]
        remote(a, a, r_ss.at[l, 0, k, p], r_rs.at[l, 0, k, p], sib).wait_recv()
        remote(b, b, r_ss.at[l, 1, k, p], r_rs.at[l, 1, k, p], sib).wait_recv()

    def mlp_copy(l):
        return remote(mlp_s.at[l], mlp_r.at[l], f_ss.at[l], f_rs.at[l], sib)

    def attend(BIG, SMALL, items, item, qref, kref, vref, nk, allowed, keep, finish, before, put, after):
        def rhs_of(t, odd):
            block, pair = item(t)
            start = pl.multiple_of(pair * pw + odd * head_dim, head_dim)
            q = qref[block, pl.ds(start, head_dim), :].astype(F32) * exp_c
            hi = q.astype(BF16)
            lo = (q - hi.astype(F32)).astype(BF16)
            z = jnp.zeros_like(hi)
            return jnp.concatenate([z, hi, z, lo] if odd else [hi, z, lo, z], axis=0)

        def score(pair, rhs, s_ref, j, top):
            k = kref[pair, j * BIG:(j + 1) * BIG, :]
            s = mm(jnp.concatenate([k, k], axis=1), rhs)
            if allowed is not None:
                s = jnp.where(allowed(j * BIG, BIG), s, neg)
            s_ref[j * BIG:(j + 1) * BIG, :] = s
            t = jnp.max(s.reshape(BIG // 8, 8, T), axis=0)
            return t if top is None else jnp.maximum(top, t)

        def accumulate(head, s_ref, j, top, total, o):
            p = jnp.exp2(s_ref[j * SMALL:(j + 1) * SMALL, :] - top)
            t = jnp.sum(p.reshape(SMALL // 8, 8, T), axis=0)
            if keep is not None:
                t = t * keep(j * SMALL, SMALL)
            vt = jnp.concatenate([vref[head, j * (SMALL // 128) + i] for i in range(SMALL // 128)], axis=1)
            v = mm(vt, p.astype(BF16))
            return (t, v) if total is None else (total + t, o + v)

        def step(nxt, nxt_odd, nxt_ref, cur, cur_odd, cur_ref, cur_top):
            rhs = rhs_of(nxt, nxt_odd)
            nxt_pair = item(nxt)[1]
            head = item(cur)[1] * 2 + cur_odd
            top = total = o = None
            for j in range(nk // BIG):
                top = score(nxt_pair, rhs, nxt_ref, j, top)
                for i in range(BIG // SMALL):
                    total, o = accumulate(head, cur_ref, j * (BIG // SMALL) + i, cur_top, total, o)
            total = jnp.sum(total, axis=0, keepdims=True)
            if finish is not None:
                cur_top, total = finish(cur_ref, cur_top, total)
            put(cur, cur_odd, o, cur_top, total)
            return jnp.max(top, axis=0, keepdims=True)

        before(0)
        rhs0 = rhs_of(0, 0)
        top = None
        for j in range(nk // BIG):
            top = score(item(0)[1], rhs0, s_even, j, top)
        top = jnp.max(top, axis=0, keepdims=True)

        def body(t, top_even):
            last = t == items - 1
            nxt = jnp.where(last, t, t + 1)

            @pl.when(jnp.logical_not(last))
            def _():
                before(t + 1)

            top_odd = step(t, 1, s_odd, t, 0, s_even, top_even)
            top_next = step(nxt, 0, s_even, t, 1, s_odd, top_odd)
            after(t)
            return top_next

        lax.fori_loop(0, items, body, top)

    def gain(ref, l):
        g = ref[0:1, :].astype(F32)
        for i in range(1, layers):
            g = jnp.where(l == i, ref[i:i + 1, :].astype(F32), g)
        return g

    def store_kv(kref, vref, row0, tile0, k, v, n):
        for p in range(pairs):
            kref[p, pl.ds(row0, n), :] = k[:, p * pw:(p + 1) * pw]
        v = v.reshape(hl, head_dim, n)
        for i in range(n // 128):
            vref[:, pl.ds(tile0 + i, 1)] = v[:, None, :, i * 128:(i + 1) * 128]

    def layer(l, carry):
        first = l == 0
        with jax.named_scope("gather_send"):
            @pl.when(first)
            def _():
                hid_cp.wait()

            for k in range(5):
                h_copy(l, k).start()

            @pl.when(first)
            def _():
                mem_cp.wait()
                mem_send.start()
                for l0 in range(layers):
                    for k in range(len(plans)):
                        if l0 > 0 or k > CV:
                            w_copy(k, l0).start()

        with jax.named_scope("w_wait"):
            w_copy(CK, l).wait()
            w_copy(CV, l).wait()
            wvt[...] = wcv[l].T

        blk = 512

        def mem_proj(part):
            core = h if part == 0 else 1 - h

            def body(b, cc):
                r0 = pl.multiple_of(b * blk, blk)
                m = mbuf[part, pl.ds(r0, blk), :]
                left_valid = limit - ((2 * c + core) * mem_rows + b * blk)
                m = jnp.where(lax.broadcasted_iota(jnp.int32, (blk, width), 0) < left_valid, m, mbuf[h, 0:1, :])
                k = mm(m, wck[l]).astype(BF16)
                v = mm_nt(wvt[...], m)
                v = jnp.where(lax.broadcasted_iota(jnp.int32, (half_w, blk), 1) < left_valid, v, 0.0).astype(BF16)
                d0 = pl.multiple_of(part * mem_rows + b * blk, blk)
                store_kv(kc, vc, d0, (part * mem_rows + b * blk) // 128, k, v, blk)
                return cc

            lax.fori_loop(0, mem_rows // blk, body, 0)

        with jax.named_scope("mem_wait"):
            @pl.when(first)
            def _():
                mem_send.wait_recv()
                for cp in small:
                    cp.wait()

        limit = mem_len[0]
        with jax.named_scope("mem_proj0"):
            mem_proj(0)

        with jax.named_scope("mem_proj1"):
            mem_proj(1)

        def self_proj(r, with_q):
            x = rms_norm(hbuf[l, r], gain(norm_self, l))
            k = mm(x, wsk[l]).astype(BF16)
            v = mm_nt(wvt[...], x).astype(BF16)
            store_kv(kself, vself, r * T, r * (T // 128), k, v, T)
            if with_q:
                qself[0] = mm(x, wsq[l]).astype(BF16).T

        with jax.named_scope("gather_wait1"):
            for k in (SK, SV, SQ):
                w_copy(k, l).wait()
            wvt[...] = wsv[l].T
            h_wait(l, 1)
            h_copy(l, 5).start()
            h_wait(l, 2)
            h_copy(l, 6).start()
            h_wait(l, 0)
        with jax.named_scope("self_proj0"):
            self_proj(0, True)
        with jax.named_scope("gather_wait2"):
            h_wait(l, 3)
            h_copy(l, 7).start()
            h_wait(l, 4)
            h_copy(l, 8).start()
            h_wait(l, 7)
        with jax.named_scope("self_proj1"):
            self_proj(1, False)
            h_wait(l, 8)
            self_proj(2, False)
        with jax.named_scope("gather_wait3"):
            h_wait(l, 5)
            h_copy(l, 9).start()
            h_wait(l, 6)
            h_copy(l, 10).start()
            h_wait(l, 9)
            h_wait(l, 10)
        with jax.named_scope("self_proj3"):
            self_proj(3, False)

        def causal(start, size):
            parts = []
            kio = lax.broadcasted_iota(jnp.int32, (T, T), 0)
            qio = lax.broadcasted_iota(jnp.int32, (T, T), 1)
            for r in range(start // T, (start + size) // T):
                parts.append(kio + (chip_of[r] - c) * T <= qio)
            return jnp.concatenate(parts, axis=0)

        def att_rows(t, odd):
            return pl.ds(pl.multiple_of(h * half_w + t * pw + odd * head_dim, head_dim), head_dim)

        def put_self(t, odd, o, top, total):
            att[l, 0, att_rows(t, odd), :] = (o / total).astype(BF16)

        with jax.named_scope("self_attend"):
            attend(512, 512, pairs, lambda t: (0, t), qself, kself, vself, n_chips * T, causal, None, None, lambda t: None, put_self,
                   lambda t: att_copy(l, 0, t).start())
        with jax.named_scope("att0_exchange"):
            w_copy(SO, l).wait()
            w_copy(CQ, l).wait()
            for p in range(pairs):
                att_wait(l, 0, p)
        with jax.named_scope("self_o_q"):
            y = (hbuf[l, 0].astype(F32) + mm(att[l, 0].T, wso[l])).astype(BF16)
            ybuf[...] = y
            x = rms_norm(y, gain(norm_cross, l))
            qc[l, 0] = mm(x, wcq[l]).astype(BF16).T
            for p in range(pairs):
                for k in (1, 2):
                    q_copy(l, k, p).start()

        def invalid_in(start, size):
            core = h if start < mem_rows else 1 - h
            end = (2 * c + core) * mem_rows + start % mem_rows + size
            return jnp.clip(end - limit, 0, size)

        def keep(start, size):
            return jnp.where(invalid_in(start, size) < size, 1.0, 0.0).astype(F32)

        extra = jnp.int32(0)
        for start in range(0, mem_all, CS):
            bad = invalid_in(start, CS)
            extra = extra + jnp.where(bad < CS, bad, 0)
        extra = extra.astype(F32)
        any_valid = 2 * c * mem_rows < limit

        def finish(s_ref, top, total):
            first_row = s_ref[pl.ds(pl.multiple_of(h * mem_rows, 8), 1), :]
            total = total - extra * jnp.exp2(first_row - top)
            return jnp.where(any_valid, top, neg), jnp.where(any_valid, total, 0.0)

        n_items = 4 * pairs
        lead = pairs - 1

        def item(t):
            t = jnp.int32(t)
            u = t - lead
            far = jnp.logical_and(t >= lead, t < n_items - 1)
            turn = u // pairs
            block = jnp.where(far, jnp.where(turn == 0, 1, jnp.where(turn == 1, 3, 2)), 0)
            pair = jnp.where(far, u % pairs, jnp.where(t == n_items - 1, pairs - 1, t))
            return block, pair

        def before(t):
            block, pair = item(t)
            @pl.when(block == 1)
            def _():
                for k in (1, 2):
                    q_wait(l, k, pair)
                    q_relay(l, k, pair).start()

            @pl.when(block == 3)
            def _():
                q_relay_wait(l, pair)

        def put_cross(t, odd, o, top, total):
            block, pair = item(t)
            res_s[l, block, pl.ds(pl.multiple_of(pair * pw + odd * head_dim, head_dim), head_dim), :] = o.astype(BF16)
            st_s[l, block, pair, odd:odd + 1, :] = top
            st_s[l, block, pair, 2 + odd:3 + odd, :] = total

        def after(t):
            block, pair = item(t)

            @pl.when(block > 0)
            def _():
                for cp in r_copies(l, block, pair):
                    cp.start()

        with jax.named_scope("cross"):
            attend(CB, CS, n_items, item, qc.at[l], kc, vc, mem_all, None, keep, finish, before, put_cross, after)

        for k in range(n_h):
            h_copy(l, k).wait_send()
        for p in range(pairs):
            att_copy(l, 0, p).wait_send()
            for k in (1, 2):
                q_copy(l, k, p).wait_send()
                q_relay(l, k, p).wait_send()
        for p in range(pairs):
            with jax.named_scope(f"res_wait{p}"):
                for r in (1, 2, 3):
                    r_wait(l, r, p)
            with jax.named_scope(f"combine{p}"):
                for odd in (0, 1):
                    hs = slice(p * pw + odd * head_dim, p * pw + (odd + 1) * head_dim)
                    tops = [st_s[l, 0, p, odd:odd + 1, :]] + [st_r[l, r, p, odd:odd + 1, :] for r in (1, 2, 3)]
                    sums = [st_s[l, 0, p, 2 + odd:3 + odd, :]] + [st_r[l, r, p, 2 + odd:3 + odd, :] for r in (1, 2, 3)]
                    nums = [res_s[l, 0, hs, :].astype(F32)] + [res_r[l, r, hs, :].astype(F32) for r in (1, 2, 3)]
                    top = functools.reduce(jnp.maximum, tops)
                    scale = [jnp.exp2(t - top) for t in tops]
                    den = sum(s * t for s, t in zip(scale, sums))
                    num = sum(s * t for s, t in zip(scale, nums))
                    att[l, 1, att_rows(p, odd), :] = (num / den).astype(BF16)
                att_copy(l, 1, p).start()
        with jax.named_scope("att1_exchange"):
            w_copy(CO, l).wait()
            w_copy(G, l).wait()
            w_copy(U, l).wait()
            w_copy(DN, l).wait()
            for p in range(pairs):
                att_wait(l, 1, p)
        with jax.named_scope("mlp"):
            y = (ybuf[...].astype(F32) + mm(att[l, 1].T, wco[l])).astype(BF16)
            ybuf[...] = y
            x = rms_norm(y, gain(norm_mlp, l))
            step = 512
            for s in range(ffl // step):
                sl = slice(s * step, (s + 1) * step)
                gate = mm(x, wg[l, :, sl])
                act[:, sl] = (jax.nn.silu(gate) * mm(x, wu[l, :, sl])).astype(BF16)
            mlp_s[l] = mm(act[sib_rows, :], wd[l])
            mlp_copy(l).start()
            mine = mm(act[my_rows, :], wd[l])
        for p in range(pairs):
            att_copy(l, 1, p).wait_send()
            for k in range(1, 4):
                for cp in r_copies(l, k, p):
                    cp.wait_send()
        with jax.named_scope("mlp_exchange"):
            remote(mlp_s.at[l], mlp_r.at[l], f_ss.at[l], f_rs.at[l], sib).wait_recv()
            hbuf[l + 1, 0, my_rows, :] = (ybuf[my_rows, :].astype(F32) + (mine + mlp_r[l])).astype(BF16)
        return carry

    lax.fori_loop(0, layers, layer, 0)
    out_cp = pltpu.make_async_copy(hbuf.at[layers, 0, my_rows], out, l_sem.at[2])
    out_cp.start()

    mem_send.wait_send()

    for l in range(layers):
        mlp_copy(l).wait_send()
    out_cp.wait()


def solution(mesh):
    group = mesh.shape["sp"]
    n_chips = group // 2
    row_spec = P(("dp", "sp"), None)

    def local_step(hidden, memory, mem_len, norm_self, norm_cross, norm_mlp, self_q, self_k, self_v, self_o, cross_q, cross_k, cross_v, cross_o, mlp_gate, mlp_up, mlp_down):
        rows, width = hidden.shape
        mem_rows = memory.shape[0]
        layers, heads, head_dim = self_o.shape[:3]
        ffl = mlp_gate.shape[2] // 2
        half_w = width // 2
        hl = heads // 2
        pairs = hl // 2
        T = 2 * rows
        mem_all = 2 * mem_rows
        wso = self_o.reshape(layers, heads * head_dim, width)
        wco = cross_o.reshape(layers, heads * head_dim, width)
        dims = (n_chips, layers, rows, width, heads, head_dim, mem_rows, ffl)
        dma = pltpu.SemaphoreType.DMA
        anyspace = pl.BlockSpec(memory_space=pl.ANY)
        call = pl.pallas_call(
            functools.partial(decoder_kernel, dims),
            out_shape=jax.ShapeDtypeStruct(hidden.shape, BF16),
            in_specs=[anyspace] * 17,
            out_specs=anyspace,
            scratch_shapes=[
                pltpu.VMEM((layers, width, half_w), BF16),
                pltpu.VMEM((layers, width, half_w), BF16),
                pltpu.VMEM((layers, width, half_w), BF16),
                pltpu.VMEM((layers, width, width), BF16),
                pltpu.VMEM((layers, width, half_w), BF16),
                pltpu.VMEM((layers, width, half_w), BF16),
                pltpu.VMEM((layers, width, half_w), BF16),
                pltpu.VMEM((layers, width, width), BF16),
                pltpu.VMEM((layers, width, ffl), BF16),
                pltpu.VMEM((layers, width, ffl), BF16),
                pltpu.VMEM((layers, ffl, width), BF16),
                pltpu.VMEM((layers, width), BF16),
                pltpu.VMEM((layers, width), BF16),
                pltpu.VMEM((layers, width), BF16),
                pltpu.SMEM((1,), jnp.int32),
                pltpu.VMEM((layers + 1, n_chips, T, width), BF16),
                pltpu.VMEM((2, mem_rows, width), BF16),
                pltpu.VMEM((T, width), BF16),
                pltpu.VMEM((half_w, width), BF16),
                pltpu.VMEM((1, half_w, T), BF16),
                pltpu.VMEM((pairs, n_chips * T, 128), BF16),
                pltpu.VMEM((hl, n_chips * T // 128, head_dim, 128), BF16),
                pltpu.VMEM((pairs, mem_all, 128), BF16),
                pltpu.VMEM((hl, mem_all // 128, head_dim, 128), BF16),
                pltpu.VMEM((layers, 4, half_w, T), BF16),
                pltpu.VMEM((mem_all, T), F32),
                pltpu.VMEM((mem_all, T), F32),
                pltpu.VMEM((layers, 4, half_w, T), BF16),
                pltpu.VMEM((layers, 4, pairs, 8, T), F32),
                pltpu.VMEM((layers, 4, half_w, T), BF16),
                pltpu.VMEM((layers, 4, pairs, 8, T), F32),
                pltpu.VMEM((layers, 2, width, T), BF16),
                pltpu.VMEM((T, ffl), BF16),
                pltpu.VMEM((layers, rows, width), F32),
                pltpu.VMEM((layers, rows, width), F32),
                dma((layers, 11)),
                dma((7,)),
                dma((layers, 11)), dma((layers, 11)),
                dma, dma,
                dma((layers, 2, pairs)), dma((layers, 2, pairs)),
                dma((layers, 5, pairs)), dma((layers, 5, pairs)),
                dma((layers, 2, 4, pairs)), dma((layers, 2, 4, pairs)),
                dma((layers,)), dma((layers,)),
            ],
            compiler_params=pltpu.CompilerParams(collective_id=0, has_side_effects=True, vmem_limit_bytes=67043328),
            name="decoder",
        )
        return call(hidden, memory, mem_len, norm_self, norm_cross, norm_mlp, self_q, self_k, self_v, wso, cross_q, cross_k, cross_v, wco, mlp_gate, mlp_up, mlp_down)

    return jax.shard_map(local_step, mesh=mesh, in_specs=(row_spec, row_spec, P("dp")) + (P(),) * 14, out_specs=row_spec, check_vma=False)
```

```python
import functools

import jax
import jax.numpy as jnp
from jax import lax
from jax.experimental import pallas as pl
from jax.experimental.pallas import tpu as pltpu
from jax.sharding import PartitionSpec as P

EPS = 1e-6
NEG_BIG = -1e30
LOG2E = 1.4426950408889634
F32 = jnp.float32
BF16 = jnp.bfloat16
CB, CS = 1024, 256
MESH = pl.DeviceIdType.MESH


def rms_norm(hidden, gain_vec):
    hidden32 = hidden.astype(F32)
    inv_rms = lax.rsqrt(jnp.mean(hidden32 * hidden32, axis=-1, keepdims=True) + EPS)
    return (hidden32 * inv_rms * gain_vec.astype(F32)).astype(BF16)


def mm(a, b):
    return jnp.dot(a, b, preferred_element_type=F32)


def mm_nt(a, b):
    return lax.dot_general(a, b, (((1,), (1,)), ((), ())), preferred_element_type=F32)


def decoder_kernel(dims, *refs):
    (n_chips, layers, rows, width, heads, head_dim, mem_rows, ffl) = dims
    (hid_in, mem_in, len_in, ns_in, nc_in, nm_in,
     w_sq, w_sk, w_sv, w_so, w_cq, w_ck, w_cv, w_co, w_g, w_u, w_d, out,
     wsq, wsk, wsv, wso, wcq, wck, wcv, wco, wg, wu, wd, norm_self, norm_cross, norm_mlp, mem_len,
     hbuf, mbuf, ybuf, wvt, qself, kself, vself, kc, vc, qc, s_even, s_odd,
     part_o, part_st, res_s, st_s, res_r, st_r, rx_o, rx_st, att, act, mlp_s, mlp_r,
     w_sem, l_sem, h_ss, h_rs, m_ss, m_rs, a_ss, a_rs, q_ss, q_rs, r_ss, r_rs, x_ss, x_rs, f_ss, f_rs) = refs
    T = 2 * rows
    half_w = width // 2
    hl = heads // 2
    pairs = hl // 2
    half = rows // 2
    pw = 2 * head_dim
    mem_all = 2 * mem_rows
    exp_c = head_dim ** -0.5 * LOG2E
    neg = NEG_BIG * LOG2E

    me = lax.axis_index("sp")
    c = me // 2
    h = me % 2
    sib = c * 2 + (1 - h)

    def peer(step):
        return lax.rem(c + step, n_chips) * 2 + h

    right, left, across = peer(1), peer(n_chips - 1), peer(2)
    chip_of = (c, lax.rem(c + n_chips - 1, n_chips), lax.rem(c + 1, n_chips), lax.rem(c + 2, n_chips))

    def remote(src, dst, ss, rs, dev):
        return pltpu.make_async_remote_copy(src_ref=src, dst_ref=dst, send_sem=ss, recv_sem=rs,
                                            device_id={"sp": dev}, device_id_type=MESH)

    def piece(core, part):
        return pl.ds(pl.multiple_of(core * rows + part * half, half), half)

    my_rows = pl.ds(pl.multiple_of(h * rows, rows), rows)
    sib_rows = pl.ds(pl.multiple_of((1 - h) * rows, rows), rows)
    my_cols = pl.ds(pl.multiple_of(h * half_w, 128), half_w)
    my_ff = pl.ds(pl.multiple_of(h * ffl, 128), ffl)

    plans = (
        (w_ck, wck, "c"), (w_cv, wcv, "c"), (w_sk, wsk, "c"), (w_sv, wsv, "c"), (w_sq, wsq, "c"), (w_so, wso, "f"),
        (w_cq, wcq, "c"), (w_co, wco, "f"), (w_g, wg, "m"), (w_u, wu, "m"), (w_d, wd, "r"),
    )
    CK, CV, SK, SV, SQ, SO, CQ, CO, G, U, DN = range(11)

    def w_copy(k, l):
        src, dst, kind = plans[k]
        if kind == "c":
            s = src.at[l, :, my_cols]
        elif kind == "m":
            s = src.at[l, :, my_ff]
        elif kind == "r":
            s = src.at[l, my_ff]
        else:
            s = src.at[l]
        return pltpu.make_async_copy(s, dst.at[l], w_sem.at[l, k])

    hid_cp = pltpu.make_async_copy(hid_in, hbuf.at[0, 0, my_rows], l_sem.at[0])
    mem_cp = pltpu.make_async_copy(mem_in, mbuf.at[0], l_sem.at[1])
    small = [pltpu.make_async_copy(s, d, l_sem.at[3 + i]) for i, (s, d) in enumerate(
        ((ns_in, norm_self), (nc_in, norm_cross), (nm_in, norm_mlp), (len_in, mem_len)))]
    hid_cp.start()
    mem_cp.start()
    w_copy(CK, 0).start()
    w_copy(CV, 0).start()
    for cp in small:
        cp.start()

    barrier = pltpu.get_barrier_semaphore()
    for dev in (sib, right, left, across):
        pl.semaphore_signal(barrier, inc=1, device_id={"sp": dev}, device_id_type=MESH)
    pl.semaphore_wait(barrier, 4)

    h_plan = (
        (0, 0, None, sib),
        (0, 1, 0, right), (0, 2, 1, left), (0, 1, 1, right), (0, 2, 0, left),
        (1, 3, 0, right), (2, 3, 1, left),
        (1, 1, None, sib), (2, 2, None, sib), (3, 3, 0, sib), (3, 3, 1, sib),
    )
    n_h = len(h_plan)

    def h_copy(l, k):
        s, d, part, dev = h_plan[k]
        rr = my_rows if part is None else piece(h, part)
        return remote(hbuf.at[l, s, rr], hbuf.at[l, d, rr], h_ss.at[l, k], h_rs.at[l, k], dev)

    def h_wait(l, k):
        s, d, part, dev = h_plan[k]
        core = 1 - h if k in (0, 7, 8, 9, 10) else h
        rr = pl.ds(pl.multiple_of(core * rows, rows), rows) if part is None else piece(core, part)
        ref = hbuf.at[l, d, rr]
        remote(ref, ref, h_ss.at[l, k], h_rs.at[l, k], sib).wait_recv()

    mem_send = remote(mbuf.at[0], mbuf.at[1], m_ss, m_rs, sib)

    def att_copy(l, k, p):
        ref = att.at[l, k, pl.ds(pl.multiple_of(h * half_w + p * pw, pw), pw)]
        return remote(ref, ref, a_ss.at[l, k, p], a_rs.at[l, k, p], sib)

    def att_wait(l, k, p):
        ref = att.at[l, k, pl.ds(pl.multiple_of((1 - h) * half_w + p * pw, pw), pw)]
        remote(ref, ref, a_ss.at[l, k, p], a_rs.at[l, k, p], sib).wait_recv()

    def pair_rows(p):
        return pl.ds(pl.multiple_of(p * pw, pw), pw)

    def q_copy(l, k, p):
        dev = (None, right, left)[k]
        return remote(qc.at[l, 0, pair_rows(p)], qc.at[l, k, pair_rows(p)], q_ss.at[l, k, p], q_rs.at[l, k, p], dev)

    def q_relay(l, k, p):
        rr = pl.ds(pl.multiple_of(p * pw + (k - 1) * head_dim, head_dim), head_dim)
        dev = (None, right, left)[k]
        return remote(qc.at[l, k, rr], qc.at[l, 3, rr], q_ss.at[l, 2 + k, p], q_rs.at[l, 2 + k, p], dev)

    def q_relay_wait(l, p):
        for k in (1, 2):
            rr = pl.ds(pl.multiple_of(p * pw + (k - 1) * head_dim, head_dim), head_dim)
            ref = qc.at[l, 3, rr]
            remote(ref, ref, q_ss.at[l, 2 + k, p], q_rs.at[l, 2 + k, p], sib).wait_recv()

    def q_wait(l, k, p):
        ref = qc.at[l, k, pair_rows(p)]
        remote(ref, ref, q_ss.at[l, k, p], q_rs.at[l, k, p], sib).wait_recv()

    def head_rows(p, odd):
        return pl.ds(pl.multiple_of(p * pw + odd * head_dim, head_dim), head_dim)

    def r_copies(l, k, p, odd):
        slot, dev = ((2, left), (1, right))[k - 1]
        rr, hd = head_rows(p, odd), p * 2 + odd
        a, b = (k - 1) * 2 + odd, (slot - 1) * 2 + odd
        return (remote(res_s.at[l, k, rr], res_r.at[l, slot, rr], r_ss.at[l, a, p], r_rs.at[l, b, p], dev),
                remote(st_s.at[l, k, hd], st_r.at[l, slot, hd], r_ss.at[l, 4 + a, p], r_rs.at[l, 4 + b, p], dev))

    def r_wait(l, slot, p, odd):
        a, b = res_r.at[l, slot, head_rows(p, odd)], st_r.at[l, slot, p * 2 + odd]
        i = (slot - 1) * 2 + odd
        remote(a, a, r_ss.at[l, i, p], r_rs.at[l, i, p], sib).wait_recv()
        remote(b, b, r_ss.at[l, 4 + i, p], r_rs.at[l, 4 + i, p], sib).wait_recv()

    def x_copies(l, odd, p):
        dev = (right, left)[odd]
        return (remote(res_s.at[l, 3, head_rows(p, odd)], rx_o.at[l, odd, p], x_ss.at[l, odd, p], x_rs.at[l, odd, p], dev),
                remote(st_s.at[l, 3, p * 2 + odd], rx_st.at[l, odd, p], x_ss.at[l, 2 + odd, p], x_rs.at[l, 2 + odd, p], dev))

    def x_wait(l, odd, p):
        a, b = rx_o.at[l, odd, p], rx_st.at[l, odd, p]
        remote(a, a, x_ss.at[l, odd, p], x_rs.at[l, odd, p], sib).wait_recv()
        remote(b, b, x_ss.at[l, 2 + odd, p], x_rs.at[l, 2 + odd, p], sib).wait_recv()

    def mlp_copy(l):
        return remote(mlp_s.at[l], mlp_r.at[l], f_ss.at[l], f_rs.at[l], sib)

    def attend(BIG, SMALL, items, item, qref, kref, vref, nk, allowed, keep, finish, before, put, after):
        def rhs_of(t, odd):
            block, pair = item(t)
            start = pl.multiple_of(pair * pw + odd * head_dim, head_dim)
            q = qref[block, pl.ds(start, head_dim), :].astype(F32) * exp_c
            hi = q.astype(BF16)
            lo = (q - hi.astype(F32)).astype(BF16)
            z = jnp.zeros_like(hi)
            return jnp.concatenate([z, hi, z, lo] if odd else [hi, z, lo, z], axis=0)

        def score(pair, rhs, s_ref, j, top):
            k = kref[pair, j * BIG:(j + 1) * BIG, :]
            s = mm(jnp.concatenate([k, k], axis=1), rhs)
            if allowed is not None:
                s = jnp.where(allowed(j * BIG, BIG), s, neg)
            s_ref[j * BIG:(j + 1) * BIG, :] = s
            t = jnp.max(s.reshape(BIG // 8, 8, T), axis=0)
            return t if top is None else jnp.maximum(top, t)

        def accumulate(head, s_ref, j, top, total, o):
            p = jnp.exp2(s_ref[j * SMALL:(j + 1) * SMALL, :] - top)
            t = jnp.sum(p.reshape(SMALL // 8, 8, T), axis=0)
            if keep is not None:
                t = t * keep(j * SMALL, SMALL)
            vt = jnp.concatenate([vref[head, j * (SMALL // 128) + i] for i in range(SMALL // 128)], axis=1)
            v = mm(vt, p.astype(BF16))
            return (t, v) if total is None else (total + t, o + v)

        def step(nxt, nxt_odd, nxt_ref, cur, cur_odd, cur_ref, cur_top):
            rhs = rhs_of(nxt, nxt_odd)
            nxt_pair = item(nxt)[1]
            head = item(cur)[1] * 2 + cur_odd
            top = total = o = None
            for j in range(nk // BIG):
                top = score(nxt_pair, rhs, nxt_ref, j, top)
                for i in range(BIG // SMALL):
                    total, o = accumulate(head, cur_ref, j * (BIG // SMALL) + i, cur_top, total, o)
            total = jnp.sum(total, axis=0, keepdims=True)
            if finish is not None:
                cur_top, total = finish(cur_ref, cur_top, total)
            put(cur, cur_odd, o, cur_top, total)
            return jnp.max(top, axis=0, keepdims=True)

        before(0)
        rhs0 = rhs_of(0, 0)
        top = None
        for j in range(nk // BIG):
            top = score(item(0)[1], rhs0, s_even, j, top)
        top = jnp.max(top, axis=0, keepdims=True)

        def body(t, top_even):
            last = t == items - 1
            nxt = jnp.where(last, t, t + 1)

            @pl.when(jnp.logical_not(last))
            def _():
                before(t + 1)

            top_odd = step(t, 1, s_odd, t, 0, s_even, top_even)
            top_next = step(nxt, 0, s_even, t, 1, s_odd, top_odd)
            after(t)
            return top_next

        lax.fori_loop(0, items, body, top)

    def gain(ref, l):
        g = ref[0:1, :].astype(F32)
        for i in range(1, layers):
            g = jnp.where(l == i, ref[i:i + 1, :].astype(F32), g)
        return g

    def store_kv(kref, vref, row0, tile0, k, v, n):
        for p in range(pairs):
            kref[p, pl.ds(row0, n), :] = k[:, p * pw:(p + 1) * pw]
        v = v.reshape(hl, head_dim, n)
        for i in range(n // 128):
            vref[:, pl.ds(tile0 + i, 1)] = v[:, None, :, i * 128:(i + 1) * 128]

    def layer(l, carry):
        first = l == 0
        with jax.named_scope("gather_send"):
            @pl.when(first)
            def _():
                hid_cp.wait()

            for k in range(5):
                h_copy(l, k).start()

            @pl.when(first)
            def _():
                mem_cp.wait()
                mem_send.start()
                for l0 in range(layers):
                    for k in range(len(plans)):
                        if l0 > 0 or k > CV:
                            w_copy(k, l0).start()

        with jax.named_scope("w_wait"):
            w_copy(CK, l).wait()
            w_copy(CV, l).wait()
            wvt[...] = wcv[l].T

        blk = 512

        def mem_proj(part):
            core = h if part == 0 else 1 - h

            def body(b, cc):
                r0 = pl.multiple_of(b * blk, blk)
                m = mbuf[part, pl.ds(r0, blk), :]
                left_valid = limit - ((2 * c + core) * mem_rows + b * blk)
                m = jnp.where(lax.broadcasted_iota(jnp.int32, (blk, width), 0) < left_valid, m, mbuf[h, 0:1, :])
                k = mm(m, wck[l]).astype(BF16)
                v = mm_nt(wvt[...], m)
                v = jnp.where(lax.broadcasted_iota(jnp.int32, (half_w, blk), 1) < left_valid, v, 0.0).astype(BF16)
                d0 = pl.multiple_of(part * mem_rows + b * blk, blk)
                store_kv(kc, vc, d0, (part * mem_rows + b * blk) // 128, k, v, blk)
                return cc

            lax.fori_loop(0, mem_rows // blk, body, 0)

        with jax.named_scope("mem_wait"):
            @pl.when(first)
            def _():
                mem_send.wait_recv()
                for cp in small:
                    cp.wait()

        limit = mem_len[0]
        with jax.named_scope("mem_proj0"):
            mem_proj(0)

        with jax.named_scope("mem_proj1"):
            mem_proj(1)

        def self_proj(r, with_q):
            x = rms_norm(hbuf[l, r], gain(norm_self, l))
            k = mm(x, wsk[l]).astype(BF16)
            v = mm_nt(wvt[...], x).astype(BF16)
            store_kv(kself, vself, r * T, r * (T // 128), k, v, T)
            if with_q:
                qself[0] = mm(x, wsq[l]).astype(BF16).T

        with jax.named_scope("gather_wait1"):
            for k in (SK, SV, SQ):
                w_copy(k, l).wait()
            wvt[...] = wsv[l].T
            h_wait(l, 1)
            h_copy(l, 5).start()
            h_wait(l, 2)
            h_copy(l, 6).start()
            h_wait(l, 0)
        with jax.named_scope("self_proj0"):
            self_proj(0, True)
        with jax.named_scope("gather_wait2"):
            h_wait(l, 3)
            h_copy(l, 7).start()
            h_wait(l, 4)
            h_copy(l, 8).start()
            h_wait(l, 7)
        with jax.named_scope("self_proj1"):
            self_proj(1, False)
            h_wait(l, 8)
            self_proj(2, False)
        with jax.named_scope("gather_wait3"):
            h_wait(l, 5)
            h_copy(l, 9).start()
            h_wait(l, 6)
            h_copy(l, 10).start()
            h_wait(l, 9)
            h_wait(l, 10)
        with jax.named_scope("self_proj3"):
            self_proj(3, False)

        def causal(start, size):
            parts = []
            kio = lax.broadcasted_iota(jnp.int32, (T, T), 0)
            qio = lax.broadcasted_iota(jnp.int32, (T, T), 1)
            for r in range(start // T, (start + size) // T):
                parts.append(kio + (chip_of[r] - c) * T <= qio)
            return jnp.concatenate(parts, axis=0)

        def att_rows(t, odd):
            return pl.ds(pl.multiple_of(h * half_w + t * pw + odd * head_dim, head_dim), head_dim)

        def put_self(t, odd, o, top, total):
            att[l, 0, att_rows(t, odd), :] = (o / total).astype(BF16)

        with jax.named_scope("self_attend"):
            attend(512, 512, pairs, lambda t: (0, t), qself, kself, vself, n_chips * T, causal, None, None, lambda t: None, put_self,
                   lambda t: att_copy(l, 0, t).start())
        with jax.named_scope("att0_exchange"):
            w_copy(SO, l).wait()
            w_copy(CQ, l).wait()
            for p in range(pairs):
                att_wait(l, 0, p)
        with jax.named_scope("self_o_q"):
            y = (hbuf[l, 0].astype(F32) + mm(att[l, 0].T, wso[l])).astype(BF16)
            ybuf[...] = y
            x = rms_norm(y, gain(norm_cross, l))
            qc[l, 0] = mm(x, wcq[l]).astype(BF16).T
            for p in range(pairs):
                for k in (1, 2):
                    q_copy(l, k, p).start()

        def invalid_in(start, size):
            core = h if start < mem_rows else 1 - h
            end = (2 * c + core) * mem_rows + start % mem_rows + size
            return jnp.clip(end - limit, 0, size)

        def keep(start, size):
            return jnp.where(invalid_in(start, size) < size, 1.0, 0.0).astype(F32)

        extra = jnp.int32(0)
        for start in range(0, mem_all, CS):
            bad = invalid_in(start, CS)
            extra = extra + jnp.where(bad < CS, bad, 0)
        extra = extra.astype(F32)
        any_valid = 2 * c * mem_rows < limit

        def finish(s_ref, top, total):
            first_row = s_ref[pl.ds(pl.multiple_of(h * mem_rows, 8), 1), :]
            total = total - extra * jnp.exp2(first_row - top)
            return jnp.where(any_valid, top, neg), jnp.where(any_valid, total, 0.0)

        n_items = 4 * pairs
        lead = pairs - 1

        def item(t):
            t = jnp.int32(t)
            u = t - lead
            far = jnp.logical_and(t >= lead, t < n_items - 1)
            turn = u // pairs
            block = jnp.where(far, jnp.where(turn == 0, 1, jnp.where(turn == 1, 3, 2)), 0)
            pair = jnp.where(far, u % pairs, jnp.where(t == n_items - 1, pairs - 1, t))
            return block, pair

        def before(t):
            block, pair = item(t)
            @pl.when(block == 1)
            def _():
                for k in (1, 2):
                    q_wait(l, k, pair)
                    q_relay(l, k, pair).start()

            @pl.when(block == 3)
            def _():
                q_relay_wait(l, pair)

        def put_cross(t, odd, o, top, total):
            block, pair = item(t)
            part_o[block, head_rows(pair, odd), :] = o
            part_st[block, pair * 2 + odd, 0:1, :] = top
            part_st[block, pair * 2 + odd, 1:2, :] = total

        def stage(k, p, odd):
            res_s[l, k, head_rows(p, odd), :] = part_o[k, head_rows(p, odd), :].astype(BF16)
            st_s[l, k, p * 2 + odd] = part_st[k, p * 2 + odd]

        def join(k, p, odd):
            hd = p * 2 + odd
            m1, m2 = part_st[k, hd, 0:1, :], rx_st[l, odd, p, 0:1, :]
            top = jnp.maximum(m1, m2)
            a, b = jnp.exp2(m1 - top), jnp.exp2(m2 - top)
            num = part_o[k, head_rows(p, odd), :] * a + rx_o[l, odd, p].astype(F32) * b
            res_s[l, k, head_rows(p, odd), :] = num.astype(BF16)
            st_s[l, k, hd, 0:1, :] = top
            st_s[l, k, hd, 1:2, :] = part_st[k, hd, 1:2, :] * a + rx_st[l, odd, p, 1:2, :] * b

        def start(copies):
            for cp in copies:
                cp.start()

        def after(t):
            block, pair = item(t)

            @pl.when(block == 1)
            def _():
                stage(1, pair, 0)
                start(r_copies(l, 1, pair, 0))

            @pl.when(block == 3)
            def _():
                for odd in (0, 1):
                    stage(3, pair, odd)
                    start(x_copies(l, odd, pair))

            @pl.when(block == 2)
            def _():
                stage(2, pair, 1)
                start(r_copies(l, 2, pair, 1))
                x_wait(l, 0, pair)
                join(2, pair, 0)
                start(r_copies(l, 2, pair, 0))
                x_wait(l, 1, pair)
                join(1, pair, 1)
                start(r_copies(l, 1, pair, 1))

        with jax.named_scope("cross"):
            attend(CB, CS, n_items, item, qc.at[l], kc, vc, mem_all, None, keep, finish, before, put_cross, after)

        for k in range(n_h):
            h_copy(l, k).wait_send()
        for p in range(pairs):
            att_copy(l, 0, p).wait_send()
            for k in (1, 2):
                q_copy(l, k, p).wait_send()
                q_relay(l, k, p).wait_send()
        for p in range(pairs):
            with jax.named_scope(f"res_wait{p}"):
                for slot in (1, 2):
                    for odd in (0, 1):
                        r_wait(l, slot, p, odd)
            with jax.named_scope(f"combine{p}"):
                for odd in (0, 1):
                    hs, hd = slice(p * pw + odd * head_dim, p * pw + (odd + 1) * head_dim), p * 2 + odd
                    tops = [part_st[0, hd, 0:1, :]] + [st_r[l, slot, hd, 0:1, :] for slot in (1, 2)]
                    sums = [part_st[0, hd, 1:2, :]] + [st_r[l, slot, hd, 1:2, :] for slot in (1, 2)]
                    nums = [part_o[0, hs, :]] + [res_r[l, slot, hs, :].astype(F32) for slot in (1, 2)]
                    top = functools.reduce(jnp.maximum, tops)
                    scale = [jnp.exp2(t - top) for t in tops]
                    den = sum(s * t for s, t in zip(scale, sums))
                    num = sum(s * t for s, t in zip(scale, nums))
                    att[l, 1, att_rows(p, odd), :] = (num / den).astype(BF16)
                att_copy(l, 1, p).start()
        with jax.named_scope("att1_exchange"):
            w_copy(CO, l).wait()
            w_copy(G, l).wait()
            w_copy(U, l).wait()
            w_copy(DN, l).wait()
            for p in range(pairs):
                att_wait(l, 1, p)
        with jax.named_scope("mlp"):
            y = (ybuf[...].astype(F32) + mm(att[l, 1].T, wco[l])).astype(BF16)
            ybuf[...] = y
            x = rms_norm(y, gain(norm_mlp, l))
            step = 512
            for s in range(ffl // step):
                sl = slice(s * step, (s + 1) * step)
                gate = mm(x, wg[l, :, sl])
                act[:, sl] = (jax.nn.silu(gate) * mm(x, wu[l, :, sl])).astype(BF16)
            mlp_s[l] = mm(act[sib_rows, :], wd[l])
            mlp_copy(l).start()
            mine = mm(act[my_rows, :], wd[l])
        for p in range(pairs):
            att_copy(l, 1, p).wait_send()
            for odd in (0, 1):
                for cp in r_copies(l, 1, p, odd) + r_copies(l, 2, p, odd) + x_copies(l, odd, p):
                    cp.wait_send()
        with jax.named_scope("mlp_exchange"):
            remote(mlp_s.at[l], mlp_r.at[l], f_ss.at[l], f_rs.at[l], sib).wait_recv()
            hbuf[l + 1, 0, my_rows, :] = (ybuf[my_rows, :].astype(F32) + (mine + mlp_r[l])).astype(BF16)
        return carry

    lax.fori_loop(0, layers, layer, 0)
    out_cp = pltpu.make_async_copy(hbuf.at[layers, 0, my_rows], out, l_sem.at[2])
    out_cp.start()

    mem_send.wait_send()

    for l in range(layers):
        mlp_copy(l).wait_send()
    out_cp.wait()


def solution(mesh):
    group = mesh.shape["sp"]
    n_chips = group // 2
    row_spec = P(("dp", "sp"), None)

    def local_step(hidden, memory, mem_len, norm_self, norm_cross, norm_mlp, self_q, self_k, self_v, self_o, cross_q, cross_k, cross_v, cross_o, mlp_gate, mlp_up, mlp_down):
        rows, width = hidden.shape
        mem_rows = memory.shape[0]
        layers, heads, head_dim = self_o.shape[:3]
        ffl = mlp_gate.shape[2] // 2
        half_w = width // 2
        hl = heads // 2
        pairs = hl // 2
        T = 2 * rows
        mem_all = 2 * mem_rows
        wso = self_o.reshape(layers, heads * head_dim, width)
        wco = cross_o.reshape(layers, heads * head_dim, width)
        dims = (n_chips, layers, rows, width, heads, head_dim, mem_rows, ffl)
        dma = pltpu.SemaphoreType.DMA
        anyspace = pl.BlockSpec(memory_space=pl.ANY)
        call = pl.pallas_call(
            functools.partial(decoder_kernel, dims),
            out_shape=jax.ShapeDtypeStruct(hidden.shape, BF16),
            in_specs=[anyspace] * 17,
            out_specs=anyspace,
            scratch_shapes=[
                pltpu.VMEM((layers, width, half_w), BF16),
                pltpu.VMEM((layers, width, half_w), BF16),
                pltpu.VMEM((layers, width, half_w), BF16),
                pltpu.VMEM((layers, width, width), BF16),
                pltpu.VMEM((layers, width, half_w), BF16),
                pltpu.VMEM((layers, width, half_w), BF16),
                pltpu.VMEM((layers, width, half_w), BF16),
                pltpu.VMEM((layers, width, width), BF16),
                pltpu.VMEM((layers, width, ffl), BF16),
                pltpu.VMEM((layers, width, ffl), BF16),
                pltpu.VMEM((layers, ffl, width), BF16),
                pltpu.VMEM((layers, width), BF16),
                pltpu.VMEM((layers, width), BF16),
                pltpu.VMEM((layers, width), BF16),
                pltpu.SMEM((1,), jnp.int32),
                pltpu.VMEM((layers + 1, n_chips, T, width), BF16),
                pltpu.VMEM((2, mem_rows, width), BF16),
                pltpu.VMEM((T, width), BF16),
                pltpu.VMEM((half_w, width), BF16),
                pltpu.VMEM((1, half_w, T), BF16),
                pltpu.VMEM((pairs, n_chips * T, 128), BF16),
                pltpu.VMEM((hl, n_chips * T // 128, head_dim, 128), BF16),
                pltpu.VMEM((pairs, mem_all, 128), BF16),
                pltpu.VMEM((hl, mem_all // 128, head_dim, 128), BF16),
                pltpu.VMEM((layers, 4, half_w, T), BF16),
                pltpu.VMEM((mem_all, T), F32),
                pltpu.VMEM((mem_all, T), F32),
                pltpu.VMEM((4, half_w, T), F32),
                pltpu.VMEM((4, hl, 2, T), F32),
                pltpu.VMEM((layers, 4, half_w, T), BF16),
                pltpu.VMEM((layers, 4, hl, 2, T), F32),
                pltpu.VMEM((layers, 3, half_w, T), BF16),
                pltpu.VMEM((layers, 3, hl, 2, T), F32),
                pltpu.VMEM((layers, 2, pairs, head_dim, T), BF16),
                pltpu.VMEM((layers, 2, pairs, 2, T), F32),
                pltpu.VMEM((layers, 2, width, T), BF16),
                pltpu.VMEM((T, ffl), BF16),
                pltpu.VMEM((layers, rows, width), F32),
                pltpu.VMEM((layers, rows, width), F32),
                dma((layers, 11)),
                dma((7,)),
                dma((layers, 11)), dma((layers, 11)),
                dma, dma,
                dma((layers, 2, pairs)), dma((layers, 2, pairs)),
                dma((layers, 5, pairs)), dma((layers, 5, pairs)),
                dma((layers, 8, pairs)), dma((layers, 8, pairs)),
                dma((layers, 4, pairs)), dma((layers, 4, pairs)),
                dma((layers,)), dma((layers,)),
            ],
            compiler_params=pltpu.CompilerParams(collective_id=0, has_side_effects=True, vmem_limit_bytes=67043328),
            name="decoder",
        )
        return call(hidden, memory, mem_len, norm_self, norm_cross, norm_mlp, self_q, self_k, self_v, wso, cross_q, cross_k, cross_v, wco, mlp_gate, mlp_up, mlp_down)

    return jax.shard_map(local_step, mesh=mesh, in_specs=(row_spec, row_spec, P("dp")) + (P(),) * 14, out_specs=row_spec, check_vma=False)
```

```python
import functools

import jax
import jax.numpy as jnp
from jax import lax
from jax.experimental import pallas as pl
from jax.experimental.pallas import tpu as pltpu
from jax.sharding import PartitionSpec as P

EPS = 1e-6
NEG_BIG = -1e30
LOG2E = 1.4426950408889634
F32 = jnp.float32
BF16 = jnp.bfloat16
CB, CS = 1024, 256
MESH = pl.DeviceIdType.MESH


def rms_norm(hidden, gain_vec):
    hidden32 = hidden.astype(F32)
    inv_rms = lax.rsqrt(jnp.mean(hidden32 * hidden32, axis=-1, keepdims=True) + EPS)
    return (hidden32 * inv_rms * gain_vec.astype(F32)).astype(BF16)


def mm(a, b):
    return jnp.dot(a, b, preferred_element_type=F32)


def mm_nt(a, b):
    return lax.dot_general(a, b, (((1,), (1,)), ((), ())), preferred_element_type=F32)


def decoder_kernel(dims, *refs):
    (n_chips, layers, rows, width, heads, head_dim, mem_rows, ffl) = dims
    (hid_in, mem_in, len_in, ns_in, nc_in, nm_in,
     w_sq, w_sk, w_sv, w_so, w_cq, w_ck, w_cv, w_co, w_g, w_u, w_d, out,
     wsq, wsk, wsv, wso, wcq, wck, wcv, wco, wg, wu, wd, norm_self, norm_cross, norm_mlp, mem_len,
     hbuf, mbuf, ybuf, wvt, qself, kself, vself, kc, vc, qc, s_even, s_odd, s_self, t_self,
     part_o, part_st, res_s, st_s, res_r, st_r, rx_o, rx_st, att, act, mlp_s, mlp_r,
     w_sem, l_sem, h_ss, h_rs, m_ss, m_rs, a_ss, a_rs, q_ss, q_rs, r_ss, r_rs, x_ss, x_rs, f_ss, f_rs) = refs
    T = 2 * rows
    half_w = width // 2
    hl = heads // 2
    pairs = hl // 2
    half = rows // 2
    pw = 2 * head_dim
    mem_all = 2 * mem_rows
    exp_c = head_dim ** -0.5 * LOG2E
    neg = NEG_BIG * LOG2E

    me = lax.axis_index("sp")
    c = me // 2
    h = me % 2
    sib = c * 2 + (1 - h)

    def peer(step):
        return lax.rem(c + step, n_chips) * 2 + h

    right, left, across = peer(1), peer(n_chips - 1), peer(2)
    chip_of = (c, lax.rem(c + n_chips - 1, n_chips), lax.rem(c + 1, n_chips), lax.rem(c + 2, n_chips))

    def remote(src, dst, ss, rs, dev):
        return pltpu.make_async_remote_copy(src_ref=src, dst_ref=dst, send_sem=ss, recv_sem=rs,
                                            device_id={"sp": dev}, device_id_type=MESH)

    def piece(core, part):
        return pl.ds(pl.multiple_of(core * rows + part * half, half), half)

    my_rows = pl.ds(pl.multiple_of(h * rows, rows), rows)
    sib_rows = pl.ds(pl.multiple_of((1 - h) * rows, rows), rows)
    my_cols = pl.ds(pl.multiple_of(h * half_w, 128), half_w)
    my_ff = pl.ds(pl.multiple_of(h * ffl, 128), ffl)

    plans = (
        (w_ck, wck, "c"), (w_cv, wcv, "c"), (w_sk, wsk, "c"), (w_sv, wsv, "c"), (w_sq, wsq, "c"), (w_so, wso, "f"),
        (w_cq, wcq, "c"), (w_co, wco, "f"), (w_g, wg, "m"), (w_u, wu, "m"), (w_d, wd, "r"),
    )
    CK, CV, SK, SV, SQ, SO, CQ, CO, G, U, DN = range(11)

    def w_copy(k, l):
        src, dst, kind = plans[k]
        if kind == "c":
            s = src.at[l, :, my_cols]
        elif kind == "m":
            s = src.at[l, :, my_ff]
        elif kind == "r":
            s = src.at[l, my_ff]
        else:
            s = src.at[l]
        return pltpu.make_async_copy(s, dst.at[l], w_sem.at[l, k])

    hid_cp = pltpu.make_async_copy(hid_in, hbuf.at[0, 0, my_rows], l_sem.at[0])
    mem_cp = pltpu.make_async_copy(mem_in, mbuf.at[0], l_sem.at[1])
    small = [pltpu.make_async_copy(s, d, l_sem.at[3 + i]) for i, (s, d) in enumerate(
        ((ns_in, norm_self), (nc_in, norm_cross), (nm_in, norm_mlp), (len_in, mem_len)))]
    hid_cp.start()
    mem_cp.start()
    w_copy(CK, 0).start()
    w_copy(CV, 0).start()
    for cp in small:
        cp.start()

    barrier = pltpu.get_barrier_semaphore()
    for dev in (sib, right, left, across):
        pl.semaphore_signal(barrier, inc=1, device_id={"sp": dev}, device_id_type=MESH)
    pl.semaphore_wait(barrier, 4)

    h_plan = (
        (0, 0, None, sib),
        (0, 1, 0, right), (0, 2, 1, left), (0, 1, 1, right), (0, 2, 0, left),
        (1, 3, 0, right), (2, 3, 1, left),
        (1, 1, None, sib), (2, 2, None, sib), (3, 3, 0, sib), (3, 3, 1, sib),
    )
    n_h = len(h_plan)

    def h_copy(l, k):
        s, d, part, dev = h_plan[k]
        rr = my_rows if part is None else piece(h, part)
        return remote(hbuf.at[l, s, rr], hbuf.at[l, d, rr], h_ss.at[l, k], h_rs.at[l, k], dev)

    def h_wait(l, k):
        s, d, part, dev = h_plan[k]
        core = 1 - h if k in (0, 7, 8, 9, 10) else h
        rr = pl.ds(pl.multiple_of(core * rows, rows), rows) if part is None else piece(core, part)
        ref = hbuf.at[l, d, rr]
        remote(ref, ref, h_ss.at[l, k], h_rs.at[l, k], sib).wait_recv()

    mem_cut = (pl.ds(0, 16), pl.ds(16, mem_rows - 16))
    mem_send = [remote(mbuf.at[0, rr], mbuf.at[1, rr], m_ss.at[i], m_rs.at[i], sib) for i, rr in enumerate(mem_cut)]

    def att_copy(l, k, p):
        ref = att.at[l, k, pl.ds(pl.multiple_of(h * half_w + p * pw, pw), pw)]
        return remote(ref, ref, a_ss.at[l, k, p], a_rs.at[l, k, p], sib)

    def att_wait(l, k, p):
        ref = att.at[l, k, pl.ds(pl.multiple_of((1 - h) * half_w + p * pw, pw), pw)]
        remote(ref, ref, a_ss.at[l, k, p], a_rs.at[l, k, p], sib).wait_recv()

    def pair_rows(p):
        return pl.ds(pl.multiple_of(p * pw, pw), pw)

    def q_copy(l, k, p):
        dev = (None, right, left)[k]
        return remote(qc.at[l, 0, pair_rows(p)], qc.at[l, k, pair_rows(p)], q_ss.at[l, k, p], q_rs.at[l, k, p], dev)

    def q_relay(l, k, p):
        rr = pl.ds(pl.multiple_of(p * pw + (k - 1) * head_dim, head_dim), head_dim)
        dev = (None, right, left)[k]
        return remote(qc.at[l, k, rr], qc.at[l, 3, rr], q_ss.at[l, 2 + k, p], q_rs.at[l, 2 + k, p], dev)

    def q_relay_wait(l, p):
        for k in (1, 2):
            rr = pl.ds(pl.multiple_of(p * pw + (k - 1) * head_dim, head_dim), head_dim)
            ref = qc.at[l, 3, rr]
            remote(ref, ref, q_ss.at[l, 2 + k, p], q_rs.at[l, 2 + k, p], sib).wait_recv()

    def q_wait(l, k, p):
        ref = qc.at[l, k, pair_rows(p)]
        remote(ref, ref, q_ss.at[l, k, p], q_rs.at[l, k, p], sib).wait_recv()

    def head_rows(p, odd):
        return pl.ds(pl.multiple_of(p * pw + odd * head_dim, head_dim), head_dim)

    def r_copies(l, k, p, odd):
        slot, dev = ((2, left), (1, right))[k - 1]
        rr, hd = head_rows(p, odd), p * 2 + odd
        a, b = (k - 1) * 2 + odd, (slot - 1) * 2 + odd
        return (remote(res_s.at[l, k, rr], res_r.at[l, slot, rr], r_ss.at[l, a, p], r_rs.at[l, b, p], dev),
                remote(st_s.at[l, k, hd], st_r.at[l, slot, hd], r_ss.at[l, 4 + a, p], r_rs.at[l, 4 + b, p], dev))

    def r_wait(l, slot, p, odd):
        a, b = res_r.at[l, slot, head_rows(p, odd)], st_r.at[l, slot, p * 2 + odd]
        i = (slot - 1) * 2 + odd
        remote(a, a, r_ss.at[l, i, p], r_rs.at[l, i, p], sib).wait_recv()
        remote(b, b, r_ss.at[l, 4 + i, p], r_rs.at[l, 4 + i, p], sib).wait_recv()

    def x_copies(l, odd, p):
        dev = (right, left)[odd]
        return (remote(res_s.at[l, 3, head_rows(p, odd)], rx_o.at[l, odd, p], x_ss.at[l, odd, p], x_rs.at[l, odd, p], dev),
                remote(st_s.at[l, 3, p * 2 + odd], rx_st.at[l, odd, p], x_ss.at[l, 2 + odd, p], x_rs.at[l, 2 + odd, p], dev))

    def x_wait(l, odd, p):
        a, b = rx_o.at[l, odd, p], rx_st.at[l, odd, p]
        remote(a, a, x_ss.at[l, odd, p], x_rs.at[l, odd, p], sib).wait_recv()
        remote(b, b, x_ss.at[l, 2 + odd, p], x_rs.at[l, 2 + odd, p], sib).wait_recv()

    def mlp_copy(l):
        return remote(mlp_s.at[l], mlp_r.at[l], f_ss.at[l], f_rs.at[l], sib)

    def split_rhs(q, odd):
        q = q.astype(F32) * exp_c
        hi = q.astype(BF16)
        lo = (q - hi.astype(F32)).astype(BF16)
        z = jnp.zeros_like(hi)
        return jnp.concatenate([z, hi, z, lo] if odd else [hi, z, lo, z], axis=0)

    def attend(BIG, SMALL, items, item, qref, kref, vref, nk, allowed, keep, finish, before, put, after):
        def rhs_of(t, odd):
            block, pair = item(t)
            start = pl.multiple_of(pair * pw + odd * head_dim, head_dim)
            return split_rhs(qref[block, pl.ds(start, head_dim), :], odd)

        def score(pair, rhs, s_ref, j, top):
            k = kref[pair, j * BIG:(j + 1) * BIG, :]
            s = mm(jnp.concatenate([k, k], axis=1), rhs)
            if allowed is not None:
                s = jnp.where(allowed(j * BIG, BIG), s, neg)
            s_ref[j * BIG:(j + 1) * BIG, :] = s
            t = jnp.max(s.reshape(BIG // 8, 8, T), axis=0)
            return t if top is None else jnp.maximum(top, t)

        def accumulate(head, s_ref, j, top, total, o):
            p = jnp.exp2(s_ref[j * SMALL:(j + 1) * SMALL, :] - top)
            t = jnp.sum(p.reshape(SMALL // 8, 8, T), axis=0)
            if keep is not None:
                t = t * keep(j * SMALL, SMALL)
            vt = jnp.concatenate([vref[head, j * (SMALL // 128) + i] for i in range(SMALL // 128)], axis=1)
            v = mm(vt, p.astype(BF16))
            return (t, v) if total is None else (total + t, o + v)

        def step(nxt, nxt_odd, nxt_ref, cur, cur_odd, cur_ref, cur_top):
            rhs = rhs_of(nxt, nxt_odd)
            nxt_pair = item(nxt)[1]
            head = item(cur)[1] * 2 + cur_odd
            top = total = o = None
            for j in range(nk // BIG):
                top = score(nxt_pair, rhs, nxt_ref, j, top)
                for i in range(BIG // SMALL):
                    total, o = accumulate(head, cur_ref, j * (BIG // SMALL) + i, cur_top, total, o)
            total = jnp.sum(total, axis=0, keepdims=True)
            if finish is not None:
                cur_top, total = finish(cur_ref, cur_top, total)
            put(cur, cur_odd, o, cur_top, total)
            return jnp.max(top, axis=0, keepdims=True)

        before(0)
        rhs0 = rhs_of(0, 0)
        top = None
        for j in range(nk // BIG):
            top = score(item(0)[1], rhs0, s_even, j, top)
        top = jnp.max(top, axis=0, keepdims=True)

        def body(t, top_even):
            last = t == items - 1
            nxt = jnp.where(last, t, t + 1)

            @pl.when(jnp.logical_not(last))
            def _():
                before(t + 1)

            top_odd = step(t, 1, s_odd, t, 0, s_even, top_even)
            top_next = step(nxt, 0, s_even, t, 1, s_odd, top_odd)
            after(t)
            return top_next

        lax.fori_loop(0, items, body, top)

    def gain(ref, l):
        g = ref[0:1, :].astype(F32)
        for i in range(1, layers):
            g = jnp.where(l == i, ref[i:i + 1, :].astype(F32), g)
        return g

    def store_kv(kref, vref, row0, tile0, k, v, n):
        for p in range(pairs):
            kref[p, pl.ds(row0, n), :] = k[:, p * pw:(p + 1) * pw]
        v = v.reshape(hl, head_dim, n)
        for i in range(n // 128):
            vref[:, pl.ds(tile0 + i, 1)] = v[:, None, :, i * 128:(i + 1) * 128]

    def layer(l, carry):
        first = l == 0
        with jax.named_scope("gather_send"):
            @pl.when(first)
            def _():
                hid_cp.wait()

            for k in range(5):
                h_copy(l, k).start()

            @pl.when(first)
            def _():
                mem_cp.wait()
                for cp in mem_send:
                    cp.start()
                for l0 in range(layers):
                    for k in range(len(plans)):
                        if l0 > 0 or k > CV:
                            w_copy(k, l0).start()

        with jax.named_scope("w_wait"):
            w_copy(CK, l).wait()
            w_copy(CV, l).wait()
            wvt[...] = wcv[l].T

        blk = 512

        def mem_proj(part):
            core = h if part == 0 else 1 - h

            def body(b, cc):
                r0 = pl.multiple_of(b * blk, blk)
                m = mbuf[part, pl.ds(r0, blk), :]
                left_valid = limit - ((2 * c + core) * mem_rows + b * blk)
                m = jnp.where(lax.broadcasted_iota(jnp.int32, (blk, width), 0) < left_valid, m, mbuf[h, 0:1, :])
                k = mm(m, wck[l]).astype(BF16)
                v = mm_nt(wvt[...], m)
                v = jnp.where(lax.broadcasted_iota(jnp.int32, (half_w, blk), 1) < left_valid, v, 0.0).astype(BF16)
                d0 = pl.multiple_of(part * mem_rows + b * blk, blk)
                store_kv(kc, vc, d0, (part * mem_rows + b * blk) // 128, k, v, blk)
                return cc

            lax.fori_loop(0, mem_rows // blk, body, 0)

        with jax.named_scope("mem_wait"):
            @pl.when(first)
            def _():
                mem_send[0].wait_recv()
                for cp in small:
                    cp.wait()

        limit = mem_len[0]
        with jax.named_scope("mem_proj0"):
            mem_proj(0)

        with jax.named_scope("mem_wait1"):
            @pl.when(first)
            def _():
                mem_send[1].wait_recv()

        with jax.named_scope("mem_proj1"):
            mem_proj(1)

        def self_proj(r, with_q):
            x = rms_norm(hbuf[l, r], gain(norm_self, l))
            if r > 0:
                x = jnp.where(chip_of[r] > c, rms_norm(hbuf[l, 0, 0:1, :], gain(norm_self, l)), x)
            k = mm(x, wsk[l]).astype(BF16)
            v = mm_nt(wvt[...], x)
            if r > 0:
                v = jnp.where(chip_of[r] > c, 0.0, v)
            v = v.astype(BF16)
            store_kv(kself, vself, r * T, r * (T // 128), k, v, T)
            if with_q:
                qself[0] = mm(x, wsq[l]).astype(BF16).T

        with jax.named_scope("gather_wait1"):
            for k in (SK, SV, SQ):
                w_copy(k, l).wait()
            wvt[...] = wsv[l].T
            h_wait(l, 1)
            h_copy(l, 5).start()
            h_wait(l, 2)
            h_copy(l, 6).start()
            h_wait(l, 0)
        with jax.named_scope("self_proj0"):
            self_proj(0, True)
        with jax.named_scope("gather_wait2"):
            h_wait(l, 3)
            h_copy(l, 7).start()
            h_wait(l, 4)
            h_copy(l, 8).start()
            h_wait(l, 7)
        with jax.named_scope("self_proj1"):
            self_proj(1, False)
            h_wait(l, 8)
            self_proj(2, False)
        def self_rhs(hd):
            return split_rhs(qself[0, hd * head_dim:(hd + 1) * head_dim, :], hd % 2)

        def self_score(hd, rhs, r):
            k = kself[hd // 2, r * T:(r + 1) * T, :]
            sc = mm(jnp.concatenate([k, k], axis=1), rhs)
            if r == 0:
                kio = lax.broadcasted_iota(jnp.int32, (T, T), 0)
                qio = lax.broadcasted_iota(jnp.int32, (T, T), 1)
                sc = jnp.where(kio <= qio, sc, neg)
            s_self[hd, r * T:(r + 1) * T, :] = sc
            return jnp.max(sc.reshape(T // 8, 8, T), axis=0)

        with jax.named_scope("self_score"):
            for hd in range(hl):
                rhs = self_rhs(hd)
                t_self[hd] = functools.reduce(jnp.maximum, [self_score(hd, rhs, r) for r in (0, 1, 2)])
        with jax.named_scope("gather_wait3"):
            h_wait(l, 5)
            h_copy(l, 9).start()
            h_wait(l, 6)
            h_copy(l, 10).start()
            h_wait(l, 9)
            h_wait(l, 10)
        with jax.named_scope("self_proj3"):
            self_proj(3, False)

        def att_rows(t, odd):
            return pl.ds(pl.multiple_of(h * half_w + t * pw + odd * head_dim, head_dim), head_dim)

        with jax.named_scope("self_attend"):
            seen = [None] + [jnp.where(chip_of[r] > c, 0.0, 1.0).astype(F32) for r in (1, 2, 3)]

            def self_top(hd):
                top = jnp.maximum(t_self[hd], self_score(hd, self_rhs(hd), 3))
                return jnp.max(top, axis=0, keepdims=True)

            top = self_top(0)
            for hd in range(hl):
                ahead = self_top(hd + 1) if hd + 1 < hl else None
                total = o = None
                for r in range(n_chips):
                    p = jnp.exp2(s_self[hd, r * T:(r + 1) * T, :] - top)
                    t = jnp.sum(p.reshape(T // 8, 8, T), axis=0)
                    if r > 0:
                        t = t * seen[r]
                    v = mm(jnp.concatenate([vself[hd, r * (T // 128) + i] for i in range(T // 128)], axis=1), p.astype(BF16))
                    total, o = (t, v) if total is None else (total + t, o + v)
                total = jnp.sum(total, axis=0, keepdims=True)
                att[l, 0, att_rows(hd // 2, hd % 2), :] = (o / total).astype(BF16)
                top = ahead
            for p in range(pairs):
                att_copy(l, 0, p).start()
        with jax.named_scope("att0_exchange"):
            w_copy(SO, l).wait()
            w_copy(CQ, l).wait()
            for p in range(pairs):
                att_wait(l, 0, p)
        with jax.named_scope("self_o_q"):
            y = (hbuf[l, 0].astype(F32) + mm(att[l, 0].T, wso[l])).astype(BF16)
            ybuf[...] = y
            x = rms_norm(y, gain(norm_cross, l))
            qc[l, 0] = mm(x, wcq[l]).astype(BF16).T
            for p in range(pairs):
                for k in (1, 2):
                    q_copy(l, k, p).start()

        def invalid_in(start, size):
            core = h if start < mem_rows else 1 - h
            end = (2 * c + core) * mem_rows + start % mem_rows + size
            return jnp.clip(end - limit, 0, size)

        def keep(start, size):
            return jnp.where(invalid_in(start, size) < size, 1.0, 0.0).astype(F32)

        extra = jnp.int32(0)
        for start in range(0, mem_all, CS):
            bad = invalid_in(start, CS)
            extra = extra + jnp.where(bad < CS, bad, 0)
        extra = extra.astype(F32)
        any_valid = 2 * c * mem_rows < limit

        def finish(s_ref, top, total):
            first_row = s_ref[pl.ds(pl.multiple_of(h * mem_rows, 8), 1), :]
            total = total - extra * jnp.exp2(first_row - top)
            return jnp.where(any_valid, top, neg), jnp.where(any_valid, total, 0.0)

        n_items = 4 * pairs
        lead = pairs - 1

        def item(t):
            t = jnp.int32(t)
            u = t - lead
            far = jnp.logical_and(t >= lead, t < n_items - 1)
            turn = u // pairs
            block = jnp.where(far, jnp.where(turn == 0, 1, jnp.where(turn == 1, 3, 2)), 0)
            pair = jnp.where(far, u % pairs, jnp.where(t == n_items - 1, pairs - 1, t))
            return block, pair

        def before(t):
            block, pair = item(t)
            @pl.when(block == 1)
            def _():
                for k in (1, 2):
                    q_wait(l, k, pair)
                    q_relay(l, k, pair).start()

            @pl.when(block == 3)
            def _():
                q_relay_wait(l, pair)

        def put_cross(t, odd, o, top, total):
            block, pair = item(t)
            part_o[block, head_rows(pair, odd), :] = o
            part_st[block, pair * 2 + odd, 0:1, :] = top
            part_st[block, pair * 2 + odd, 1:2, :] = total

        def stage(k, p, odd):
            res_s[l, k, head_rows(p, odd), :] = part_o[k, head_rows(p, odd), :].astype(BF16)
            st_s[l, k, p * 2 + odd] = part_st[k, p * 2 + odd]

        def join(k, p, odd):
            hd = p * 2 + odd
            m1, m2 = part_st[k, hd, 0:1, :], rx_st[l, odd, p, 0:1, :]
            top = jnp.maximum(m1, m2)
            a, b = jnp.exp2(m1 - top), jnp.exp2(m2 - top)
            num = part_o[k, head_rows(p, odd), :] * a + rx_o[l, odd, p].astype(F32) * b
            res_s[l, k, head_rows(p, odd), :] = num.astype(BF16)
            st_s[l, k, hd, 0:1, :] = top
            st_s[l, k, hd, 1:2, :] = part_st[k, hd, 1:2, :] * a + rx_st[l, odd, p, 1:2, :] * b

        def start(copies):
            for cp in copies:
                cp.start()

        def after(t):
            block, pair = item(t)

            @pl.when(block == 1)
            def _():
                stage(1, pair, 0)
                start(r_copies(l, 1, pair, 0))

            @pl.when(block == 3)
            def _():
                for odd in (0, 1):
                    stage(3, pair, odd)
                    start(x_copies(l, odd, pair))

            @pl.when(block == 2)
            def _():
                stage(2, pair, 1)
                start(r_copies(l, 2, pair, 1))
                x_wait(l, 0, pair)
                join(2, pair, 0)
                start(r_copies(l, 2, pair, 0))
                x_wait(l, 1, pair)
                join(1, pair, 1)
                start(r_copies(l, 1, pair, 1))

        with jax.named_scope("cross"):
            attend(CB, CS, n_items, item, qc.at[l], kc, vc, mem_all, None, keep, finish, before, put_cross, after)

        for k in range(n_h):
            h_copy(l, k).wait_send()
        for p in range(pairs):
            att_copy(l, 0, p).wait_send()
            for k in (1, 2):
                q_copy(l, k, p).wait_send()
                q_relay(l, k, p).wait_send()
        for p in range(pairs):
            with jax.named_scope(f"res_wait{p}"):
                for slot in (1, 2):
                    for odd in (0, 1):
                        r_wait(l, slot, p, odd)
            with jax.named_scope(f"combine{p}"):
                for odd in (0, 1):
                    hs, hd = slice(p * pw + odd * head_dim, p * pw + (odd + 1) * head_dim), p * 2 + odd
                    tops = [part_st[0, hd, 0:1, :]] + [st_r[l, slot, hd, 0:1, :] for slot in (1, 2)]
                    sums = [part_st[0, hd, 1:2, :]] + [st_r[l, slot, hd, 1:2, :] for slot in (1, 2)]
                    nums = [part_o[0, hs, :]] + [res_r[l, slot, hs, :].astype(F32) for slot in (1, 2)]
                    top = functools.reduce(jnp.maximum, tops)
                    scale = [jnp.exp2(t - top) for t in tops]
                    den = sum(s * t for s, t in zip(scale, sums))
                    num = sum(s * t for s, t in zip(scale, nums))
                    att[l, 1, att_rows(p, odd), :] = (num / den).astype(BF16)
                att_copy(l, 1, p).start()
        with jax.named_scope("att1_exchange"):
            w_copy(CO, l).wait()
            w_copy(G, l).wait()
            w_copy(U, l).wait()
            w_copy(DN, l).wait()
            for p in range(pairs):
                att_wait(l, 1, p)
        with jax.named_scope("mlp"):
            y = (ybuf[...].astype(F32) + mm(att[l, 1].T, wco[l])).astype(BF16)
            ybuf[...] = y
            x = rms_norm(y, gain(norm_mlp, l))
            step = 512
            for s in range(ffl // step):
                sl = slice(s * step, (s + 1) * step)
                gate = mm(x, wg[l, :, sl])
                act[:, sl] = (jax.nn.silu(gate) * mm(x, wu[l, :, sl])).astype(BF16)
            mlp_s[l] = mm(act[sib_rows, :], wd[l])
            mlp_copy(l).start()
            mine = mm(act[my_rows, :], wd[l])
        for p in range(pairs):
            att_copy(l, 1, p).wait_send()
            for odd in (0, 1):
                for cp in r_copies(l, 1, p, odd) + r_copies(l, 2, p, odd) + x_copies(l, odd, p):
                    cp.wait_send()
        with jax.named_scope("mlp_exchange"):
            remote(mlp_s.at[l], mlp_r.at[l], f_ss.at[l], f_rs.at[l], sib).wait_recv()
            hbuf[l + 1, 0, my_rows, :] = (ybuf[my_rows, :].astype(F32) + (mine + mlp_r[l])).astype(BF16)
        return carry

    lax.fori_loop(0, layers, layer, 0)
    out_cp = pltpu.make_async_copy(hbuf.at[layers, 0, my_rows], out, l_sem.at[2])
    out_cp.start()

    for cp in mem_send:
        cp.wait_send()

    for l in range(layers):
        mlp_copy(l).wait_send()
    out_cp.wait()


def solution(mesh):
    group = mesh.shape["sp"]
    n_chips = group // 2
    row_spec = P(("dp", "sp"), None)

    def local_step(hidden, memory, mem_len, norm_self, norm_cross, norm_mlp, self_q, self_k, self_v, self_o, cross_q, cross_k, cross_v, cross_o, mlp_gate, mlp_up, mlp_down):
        rows, width = hidden.shape
        mem_rows = memory.shape[0]
        layers, heads, head_dim = self_o.shape[:3]
        ffl = mlp_gate.shape[2] // 2
        half_w = width // 2
        hl = heads // 2
        pairs = hl // 2
        T = 2 * rows
        mem_all = 2 * mem_rows
        wso = self_o.reshape(layers, heads * head_dim, width)
        wco = cross_o.reshape(layers, heads * head_dim, width)
        dims = (n_chips, layers, rows, width, heads, head_dim, mem_rows, ffl)
        dma = pltpu.SemaphoreType.DMA
        anyspace = pl.BlockSpec(memory_space=pl.ANY)
        call = pl.pallas_call(
            functools.partial(decoder_kernel, dims),
            out_shape=jax.ShapeDtypeStruct(hidden.shape, BF16),
            in_specs=[anyspace] * 17,
            out_specs=anyspace,
            scratch_shapes=[
                pltpu.VMEM((layers, width, half_w), BF16),
                pltpu.VMEM((layers, width, half_w), BF16),
                pltpu.VMEM((layers, width, half_w), BF16),
                pltpu.VMEM((layers, width, width), BF16),
                pltpu.VMEM((layers, width, half_w), BF16),
                pltpu.VMEM((layers, width, half_w), BF16),
                pltpu.VMEM((layers, width, half_w), BF16),
                pltpu.VMEM((layers, width, width), BF16),
                pltpu.VMEM((layers, width, ffl), BF16),
                pltpu.VMEM((layers, width, ffl), BF16),
                pltpu.VMEM((layers, ffl, width), BF16),
                pltpu.VMEM((layers, width), BF16),
                pltpu.VMEM((layers, width), BF16),
                pltpu.VMEM((layers, width), BF16),
                pltpu.SMEM((1,), jnp.int32),
                pltpu.VMEM((layers + 1, n_chips, T, width), BF16),
                pltpu.VMEM((2, mem_rows, width), BF16),
                pltpu.VMEM((T, width), BF16),
                pltpu.VMEM((half_w, width), BF16),
                pltpu.VMEM((1, half_w, T), BF16),
                pltpu.VMEM((pairs, n_chips * T, 128), BF16),
                pltpu.VMEM((hl, n_chips * T // 128, head_dim, 128), BF16),
                pltpu.VMEM((pairs, mem_all, 128), BF16),
                pltpu.VMEM((hl, mem_all // 128, head_dim, 128), BF16),
                pltpu.VMEM((layers, 4, half_w, T), BF16),
                pltpu.VMEM((mem_all, T), F32),
                pltpu.VMEM((mem_all, T), F32),
                pltpu.VMEM((hl, n_chips * T, T), F32),
                pltpu.VMEM((hl, 8, T), F32),
                pltpu.VMEM((4, half_w, T), F32),
                pltpu.VMEM((4, hl, 2, T), F32),
                pltpu.VMEM((layers, 4, half_w, T), BF16),
                pltpu.VMEM((layers, 4, hl, 2, T), F32),
                pltpu.VMEM((layers, 3, half_w, T), BF16),
                pltpu.VMEM((layers, 3, hl, 2, T), F32),
                pltpu.VMEM((layers, 2, pairs, head_dim, T), BF16),
                pltpu.VMEM((layers, 2, pairs, 2, T), F32),
                pltpu.VMEM((layers, 2, width, T), BF16),
                pltpu.VMEM((T, ffl), BF16),
                pltpu.VMEM((layers, rows, width), F32),
                pltpu.VMEM((layers, rows, width), F32),
                dma((layers, 11)),
                dma((7,)),
                dma((layers, 11)), dma((layers, 11)),
                dma((2,)), dma((2,)),
                dma((layers, 2, pairs)), dma((layers, 2, pairs)),
                dma((layers, 5, pairs)), dma((layers, 5, pairs)),
                dma((layers, 8, pairs)), dma((layers, 8, pairs)),
                dma((layers, 4, pairs)), dma((layers, 4, pairs)),
                dma((layers,)), dma((layers,)),
            ],
            compiler_params=pltpu.CompilerParams(collective_id=0, has_side_effects=True, vmem_limit_bytes=67043328),
            name="decoder",
        )
        return call(hidden, memory, mem_len, norm_self, norm_cross, norm_mlp, self_q, self_k, self_v, wso, cross_q, cross_k, cross_v, wco, mlp_gate, mlp_up, mlp_down)

    return jax.shard_map(local_step, mesh=mesh, in_specs=(row_spec, row_spec, P("dp")) + (P(),) * 14, out_specs=row_spec, check_vma=False)
```

```python
import functools

import jax
import jax.numpy as jnp
from jax import lax
from jax.experimental import pallas as pl
from jax.experimental.pallas import tpu as pltpu
from jax.sharding import PartitionSpec as P

EPS = 1e-6
NEG_BIG = -1e30
LOG2E = 1.4426950408889634
F32 = jnp.float32
BF16 = jnp.bfloat16
CB, CS = 1024, 256
MESH = pl.DeviceIdType.MESH


def rms_norm(hidden, gain_vec):
    hidden32 = hidden.astype(F32)
    inv_rms = lax.rsqrt(jnp.mean(hidden32 * hidden32, axis=-1, keepdims=True) + EPS)
    return (hidden32 * inv_rms * gain_vec.astype(F32)).astype(BF16)


def mm(a, b):
    return jnp.dot(a, b, preferred_element_type=F32)


def mm_nt(a, b):
    return lax.dot_general(a, b, (((1,), (1,)), ((), ())), preferred_element_type=F32)


def decoder_kernel(dims, *refs):
    (n_chips, layers, rows, width, heads, head_dim, mem_rows, ffl) = dims
    (hid_in, mem_in, len_in, ns_in, nc_in, nm_in,
     w_sq, w_sk, w_sv, w_so, w_cq, w_ck, w_cv, w_co, w_g, w_u, w_d, out,
     wsq, wsk, wsv, wso, wcq, wck, wcv, wco, wg, wu, wd, norm_self, norm_cross, norm_mlp, mem_len,
     hbuf, mbuf, ybuf, wvt, qself, kself, vself, kc, vc, qc, s_even, s_odd, s_self, t_self,
     part_o, part_st, res_s, st_s, res_r, st_r, rx_o, rx_st, att, act, mlp_s, mlp_r,
     w_sem, l_sem, h_ss, h_rs, m_ss, m_rs, a_ss, a_rs, q_ss, q_rs, r_ss, r_rs, x_ss, x_rs, f_ss, f_rs) = refs
    T = 2 * rows
    half_w = width // 2
    hl = heads // 2
    pairs = hl // 2
    half = rows // 2
    pw = 2 * head_dim
    mem_all = 2 * mem_rows
    exp_c = head_dim ** -0.5 * LOG2E
    neg = NEG_BIG * LOG2E

    me = lax.axis_index("sp")
    c = me // 2
    h = me % 2
    sib = c * 2 + (1 - h)

    def peer(step):
        return lax.rem(c + step, n_chips) * 2 + h

    right, left, across = peer(1), peer(n_chips - 1), peer(2)
    chip_of = (c, lax.rem(c + n_chips - 1, n_chips), lax.rem(c + 1, n_chips), lax.rem(c + 2, n_chips))

    def remote(src, dst, ss, rs, dev):
        return pltpu.make_async_remote_copy(src_ref=src, dst_ref=dst, send_sem=ss, recv_sem=rs,
                                            device_id={"sp": dev}, device_id_type=MESH)

    def piece(core, part):
        return pl.ds(pl.multiple_of(core * rows + part * half, half), half)

    my_rows = pl.ds(pl.multiple_of(h * rows, rows), rows)
    sib_rows = pl.ds(pl.multiple_of((1 - h) * rows, rows), rows)
    my_cols = pl.ds(pl.multiple_of(h * half_w, 128), half_w)
    my_ff = pl.ds(pl.multiple_of(h * ffl, 128), ffl)

    plans = (
        (w_ck, wck, "c"), (w_cv, wcv, "c"), (w_sk, wsk, "c"), (w_sv, wsv, "c"), (w_sq, wsq, "c"), (w_so, wso, "f"),
        (w_cq, wcq, "c"), (w_co, wco, "f"), (w_g, wg, "m"), (w_u, wu, "m"), (w_d, wd, "r"),
    )
    CK, CV, SK, SV, SQ, SO, CQ, CO, G, U, DN = range(11)

    def w_copy(k, l):
        src, dst, kind = plans[k]
        if kind == "c":
            s = src.at[l, :, my_cols]
        elif kind == "m":
            s = src.at[l, :, my_ff]
        elif kind == "r":
            s = src.at[l, my_ff]
        else:
            s = src.at[l]
        return pltpu.make_async_copy(s, dst.at[l], w_sem.at[l, k])

    hid_cp = pltpu.make_async_copy(hid_in, hbuf.at[0, 0, my_rows], l_sem.at[0])
    mem_cp = pltpu.make_async_copy(mem_in, mbuf.at[0], l_sem.at[1])
    small = [pltpu.make_async_copy(s, d, l_sem.at[3 + i]) for i, (s, d) in enumerate(
        ((ns_in, norm_self), (nc_in, norm_cross), (nm_in, norm_mlp), (len_in, mem_len)))]
    hid_cp.start()
    mem_cp.start()
    w_copy(CK, 0).start()
    w_copy(CV, 0).start()
    for cp in small:
        cp.start()

    barrier = pltpu.get_barrier_semaphore()
    for dev in (sib, right, left, across):
        pl.semaphore_signal(barrier, inc=1, device_id={"sp": dev}, device_id_type=MESH)
    pl.semaphore_wait(barrier, 4)

    h_plan = (
        (0, 0, None, sib),
        (0, 1, 0, right), (0, 2, 1, left), (0, 1, 1, right), (0, 2, 0, left),
        (1, 3, 0, right), (2, 3, 1, left),
        (1, 1, None, sib), (2, 2, None, sib), (3, 3, 0, sib), (3, 3, 1, sib),
    )
    n_h = len(h_plan)

    def h_copy(l, k):
        s, d, part, dev = h_plan[k]
        rr = my_rows if part is None else piece(h, part)
        return remote(hbuf.at[l, s, rr], hbuf.at[l, d, rr], h_ss.at[k], h_rs.at[l, k], dev)

    def h_wait(l, k):
        s, d, part, dev = h_plan[k]
        core = 1 - h if k in (0, 7, 8, 9, 10) else h
        rr = pl.ds(pl.multiple_of(core * rows, rows), rows) if part is None else piece(core, part)
        ref = hbuf.at[l, d, rr]
        remote(ref, ref, h_ss.at[k], h_rs.at[l, k], sib).wait_recv()

    mem_cut = (pl.ds(0, 16), pl.ds(16, mem_rows - 16))
    mem_send = [remote(mbuf.at[0, rr], mbuf.at[1, rr], m_ss.at[i], m_rs.at[i], sib) for i, rr in enumerate(mem_cut)]

    def att_copy(l, k, p):
        ref = att.at[l, k, pl.ds(pl.multiple_of(h * half_w + p * pw, pw), pw)]
        return remote(ref, ref, a_ss.at[k, p], a_rs.at[l, k, p], sib)

    def att_wait(l, k, p):
        ref = att.at[l, k, pl.ds(pl.multiple_of((1 - h) * half_w + p * pw, pw), pw)]
        remote(ref, ref, a_ss.at[k, p], a_rs.at[l, k, p], sib).wait_recv()

    def pair_rows(p):
        return pl.ds(pl.multiple_of(p * pw, pw), pw)

    def q_copy(l, k, p):
        dev = (None, right, left)[k]
        return remote(qc.at[l, 0, pair_rows(p)], qc.at[l, k, pair_rows(p)], q_ss.at[k, p], q_rs.at[l, k, p], dev)

    def q_relay(l, k, p):
        rr = pl.ds(pl.multiple_of(p * pw + (k - 1) * head_dim, head_dim), head_dim)
        dev = (None, right, left)[k]
        return remote(qc.at[l, k, rr], qc.at[l, 3, rr], q_ss.at[2 + k, p], q_rs.at[l, 2 + k, p], dev)

    def q_relay_wait(l, p):
        for k in (1, 2):
            rr = pl.ds(pl.multiple_of(p * pw + (k - 1) * head_dim, head_dim), head_dim)
            ref = qc.at[l, 3, rr]
            remote(ref, ref, q_ss.at[2 + k, p], q_rs.at[l, 2 + k, p], sib).wait_recv()

    def q_wait(l, k, p):
        ref = qc.at[l, k, pair_rows(p)]
        remote(ref, ref, q_ss.at[k, p], q_rs.at[l, k, p], sib).wait_recv()

    def head_rows(p, odd):
        return pl.ds(pl.multiple_of(p * pw + odd * head_dim, head_dim), head_dim)

    def r_copies(l, k, p, odd):
        slot, dev = ((2, left), (1, right))[k - 1]
        rr, hd = head_rows(p, odd), p * 2 + odd
        a, b = (k - 1) * 2 + odd, (slot - 1) * 2 + odd
        return (remote(res_s.at[l, k, rr], res_r.at[l, slot, rr], r_ss.at[a, p], r_rs.at[l, b, p], dev),
                remote(st_s.at[l, k, hd], st_r.at[l, slot, hd], r_ss.at[4 + a, p], r_rs.at[l, 4 + b, p], dev))

    def r_wait(l, slot, p, odd):
        a, b = res_r.at[l, slot, head_rows(p, odd)], st_r.at[l, slot, p * 2 + odd]
        i = (slot - 1) * 2 + odd
        remote(a, a, r_ss.at[i, p], r_rs.at[l, i, p], sib).wait_recv()
        remote(b, b, r_ss.at[4 + i, p], r_rs.at[l, 4 + i, p], sib).wait_recv()

    def x_copies(l, odd, p):
        dev = (right, left)[odd]
        return (remote(res_s.at[l, 3, head_rows(p, odd)], rx_o.at[l, odd, p], x_ss.at[odd, p], x_rs.at[l, odd, p], dev),
                remote(st_s.at[l, 3, p * 2 + odd], rx_st.at[l, odd, p], x_ss.at[2 + odd, p], x_rs.at[l, 2 + odd, p], dev))

    def x_wait(l, odd, p):
        a, b = rx_o.at[l, odd, p], rx_st.at[l, odd, p]
        remote(a, a, x_ss.at[odd, p], x_rs.at[l, odd, p], sib).wait_recv()
        remote(b, b, x_ss.at[2 + odd, p], x_rs.at[l, 2 + odd, p], sib).wait_recv()

    def mlp_copy(l):
        return remote(mlp_s.at[l, 0], mlp_r.at[l], f_ss.at[l], f_rs.at[l], sib)

    def split_rhs(q, odd):
        q = q.astype(F32) * exp_c
        hi = q.astype(BF16)
        lo = (q - hi.astype(F32)).astype(BF16)
        z = jnp.zeros_like(hi)
        return jnp.concatenate([z, hi, z, lo] if odd else [hi, z, lo, z], axis=0)

    def attend(BIG, SMALL, items, item, qref, kref, vref, nk, allowed, keep, finish, before, put, after):
        def rhs_of(t, odd):
            block, pair = item(t)
            start = pl.multiple_of(pair * pw + odd * head_dim, head_dim)
            return split_rhs(qref[block, pl.ds(start, head_dim), :], odd)

        def score(pair, rhs, s_ref, j, top):
            k = kref[pair, j * BIG:(j + 1) * BIG, :]
            s = mm(jnp.concatenate([k, k], axis=1), rhs)
            if allowed is not None:
                s = jnp.where(allowed(j * BIG, BIG), s, neg)
            s_ref[j * BIG:(j + 1) * BIG, :] = s
            t = jnp.max(s.reshape(BIG // 8, 8, T), axis=0)
            return t if top is None else jnp.maximum(top, t)

        def accumulate(head, s_ref, j, top, total, o):
            p = jnp.exp2(s_ref[j * SMALL:(j + 1) * SMALL, :] - top)
            t = jnp.sum(p.reshape(SMALL // 8, 8, T), axis=0)
            if keep is not None:
                t = t * keep(j * SMALL, SMALL)
            vt = jnp.concatenate([vref[head, j * (SMALL // 128) + i] for i in range(SMALL // 128)], axis=1)
            v = mm(vt, p.astype(BF16))
            return (t, v) if total is None else (total + t, o + v)

        def step(nxt, nxt_odd, nxt_ref, cur, cur_odd, cur_ref, cur_top):
            rhs = rhs_of(nxt, nxt_odd)
            nxt_pair = item(nxt)[1]
            head = item(cur)[1] * 2 + cur_odd
            top = total = o = None
            for j in range(nk // BIG):
                top = score(nxt_pair, rhs, nxt_ref, j, top)
                for i in range(BIG // SMALL):
                    total, o = accumulate(head, cur_ref, j * (BIG // SMALL) + i, cur_top, total, o)
            total = jnp.sum(total, axis=0, keepdims=True)
            if finish is not None:
                cur_top, total = finish(cur_ref, cur_top, total)
            put(cur, cur_odd, o, cur_top, total)
            return jnp.max(top, axis=0, keepdims=True)

        before(0)
        rhs0 = rhs_of(0, 0)
        top = None
        for j in range(nk // BIG):
            top = score(item(0)[1], rhs0, s_even, j, top)
        top = jnp.max(top, axis=0, keepdims=True)

        def body(t, top_even):
            last = t == items - 1
            nxt = jnp.where(last, t, t + 1)

            @pl.when(jnp.logical_not(last))
            def _():
                before(t + 1)

            top_odd = step(t, 1, s_odd, t, 0, s_even, top_even)
            top_next = step(nxt, 0, s_even, t, 1, s_odd, top_odd)
            after(t)
            return top_next

        lax.fori_loop(0, items, body, top)

    def gain(ref, l):
        g = ref[0:1, :].astype(F32)
        for i in range(1, layers):
            g = jnp.where(l == i, ref[i:i + 1, :].astype(F32), g)
        return g

    def store_kv(kref, vref, row0, tile0, k, v, n):
        for p in range(pairs):
            kref[p, pl.ds(row0, n), :] = k[:, p * pw:(p + 1) * pw]
        v = v.reshape(hl, head_dim, n)
        for i in range(n // 128):
            vref[:, pl.ds(tile0 + i, 1)] = v[:, None, :, i * 128:(i + 1) * 128]

    def layer(l, carry):
        first = l == 0
        with jax.named_scope("gather_send"):
            @pl.when(first)
            def _():
                hid_cp.wait()

            for k in range(5):
                h_copy(l, k).start()

            @pl.when(first)
            def _():
                mem_cp.wait()
                for cp in mem_send:
                    cp.start()
                for l0 in range(layers):
                    for k in range(len(plans)):
                        if l0 > 0 or k > CV:
                            w_copy(k, l0).start()

        with jax.named_scope("w_wait"):
            w_copy(CK, l).wait()
            w_copy(CV, l).wait()
            wvt[...] = wcv[l].T

        blk = 512

        def mem_proj(part):
            core = h if part == 0 else 1 - h

            def body(b, cc):
                r0 = pl.multiple_of(b * blk, blk)
                m = mbuf[part, pl.ds(r0, blk), :]
                left_valid = limit - ((2 * c + core) * mem_rows + b * blk)
                m = jnp.where(lax.broadcasted_iota(jnp.int32, (blk, width), 0) < left_valid, m, mbuf[h, 0:1, :])
                k = mm(m, wck[l]).astype(BF16)
                v = mm_nt(wvt[...], m)
                v = jnp.where(lax.broadcasted_iota(jnp.int32, (half_w, blk), 1) < left_valid, v, 0.0).astype(BF16)
                d0 = pl.multiple_of(part * mem_rows + b * blk, blk)
                store_kv(kc, vc, d0, (part * mem_rows + b * blk) // 128, k, v, blk)
                return cc

            lax.fori_loop(0, mem_rows // blk, body, 0)

        with jax.named_scope("mem_wait"):
            @pl.when(first)
            def _():
                mem_send[0].wait_recv()
                for cp in small:
                    cp.wait()

        limit = mem_len[0]
        with jax.named_scope("mem_proj0"):
            mem_proj(0)

        with jax.named_scope("mem_wait1"):
            @pl.when(first)
            def _():
                mem_send[1].wait_recv()

        with jax.named_scope("mem_proj1"):
            mem_proj(1)

        def self_proj(r, with_q):
            x = rms_norm(hbuf[l, r], gain(norm_self, l))
            if r > 0:
                x = jnp.where(chip_of[r] > c, rms_norm(hbuf[l, 0, 0:1, :], gain(norm_self, l)), x)
            k = mm(x, wsk[l]).astype(BF16)
            v = mm_nt(wvt[...], x)
            if r > 0:
                v = jnp.where(chip_of[r] > c, 0.0, v)
            v = v.astype(BF16)
            store_kv(kself, vself, r * T, r * (T // 128), k, v, T)
            if with_q:
                qself[0] = mm(x, wsq[l]).astype(BF16).T

        with jax.named_scope("gather_wait1"):
            for k in (SK, SV, SQ):
                w_copy(k, l).wait()
            wvt[...] = wsv[l].T
            h_wait(l, 1)
            h_copy(l, 5).start()
            h_wait(l, 2)
            h_copy(l, 6).start()
            h_wait(l, 0)
        with jax.named_scope("self_proj0"):
            self_proj(0, True)
        with jax.named_scope("gather_wait2"):
            h_wait(l, 3)
            h_copy(l, 7).start()
            h_wait(l, 4)
            h_copy(l, 8).start()
            h_wait(l, 7)
        with jax.named_scope("self_proj1"):
            self_proj(1, False)
            h_wait(l, 8)
            self_proj(2, False)
        def self_rhs(hd):
            return split_rhs(qself[0, hd * head_dim:(hd + 1) * head_dim, :], hd % 2)

        def self_score(hd, rhs, r):
            k = kself[hd // 2, r * T:(r + 1) * T, :]
            sc = mm(jnp.concatenate([k, k], axis=1), rhs)
            if r == 0:
                kio = lax.broadcasted_iota(jnp.int32, (T, T), 0)
                qio = lax.broadcasted_iota(jnp.int32, (T, T), 1)
                sc = jnp.where(kio <= qio, sc, neg)
            s_self[hd, r * T:(r + 1) * T, :] = sc
            return jnp.max(sc.reshape(T // 8, 8, T), axis=0)

        with jax.named_scope("self_score"):
            for hd in range(hl):
                rhs = self_rhs(hd)
                t_self[hd] = functools.reduce(jnp.maximum, [self_score(hd, rhs, r) for r in (0, 1, 2)])
        with jax.named_scope("gather_wait3"):
            h_wait(l, 5)
            h_copy(l, 9).start()
            h_wait(l, 6)
            h_copy(l, 10).start()
            h_wait(l, 9)
            h_wait(l, 10)
        with jax.named_scope("self_proj3"):
            self_proj(3, False)

        def att_rows(t, odd):
            return pl.ds(pl.multiple_of(h * half_w + t * pw + odd * head_dim, head_dim), head_dim)

        with jax.named_scope("self_attend"):
            seen = [None] + [jnp.where(chip_of[r] > c, 0.0, 1.0).astype(F32) for r in (1, 2, 3)]

            def self_top(hd):
                top = jnp.maximum(t_self[hd], self_score(hd, self_rhs(hd), 3))
                return jnp.max(top, axis=0, keepdims=True)

            top = self_top(0)
            for hd in range(hl):
                ahead = self_top(hd + 1) if hd + 1 < hl else None
                total = o = None
                for r in range(n_chips):
                    p = jnp.exp2(s_self[hd, r * T:(r + 1) * T, :] - top)
                    t = jnp.sum(p.reshape(T // 8, 8, T), axis=0)
                    if r > 0:
                        t = t * seen[r]
                    v = mm(jnp.concatenate([vself[hd, r * (T // 128) + i] for i in range(T // 128)], axis=1), p.astype(BF16))
                    total, o = (t, v) if total is None else (total + t, o + v)
                total = jnp.sum(total, axis=0, keepdims=True)
                att[l, 0, att_rows(hd // 2, hd % 2), :] = (o / total).astype(BF16)
                top = ahead
            for p in range(pairs):
                att_copy(l, 0, p).start()
        with jax.named_scope("att0_exchange"):
            w_copy(SO, l).wait()
            w_copy(CQ, l).wait()
            for p in range(pairs):
                att_wait(l, 0, p)
        with jax.named_scope("self_o_q"):
            y = (hbuf[l, 0].astype(F32) + mm(att[l, 0].T, wso[l])).astype(BF16)
            ybuf[...] = y
            x = rms_norm(y, gain(norm_cross, l))
            qc[l, 0] = mm(x, wcq[l]).astype(BF16).T
            for p in range(pairs):
                for k in (1, 2):
                    q_copy(l, k, p).start()

        def invalid_in(start, size):
            core = h if start < mem_rows else 1 - h
            end = (2 * c + core) * mem_rows + start % mem_rows + size
            return jnp.clip(end - limit, 0, size)

        def keep(start, size):
            return jnp.where(invalid_in(start, size) < size, 1.0, 0.0).astype(F32)

        extra = jnp.int32(0)
        for start in range(0, mem_all, CS):
            bad = invalid_in(start, CS)
            extra = extra + jnp.where(bad < CS, bad, 0)
        extra = extra.astype(F32)
        any_valid = 2 * c * mem_rows < limit

        def finish(s_ref, top, total):
            first_row = s_ref[pl.ds(pl.multiple_of(h * mem_rows, 8), 1), :]
            total = total - extra * jnp.exp2(first_row - top)
            return jnp.where(any_valid, top, neg), jnp.where(any_valid, total, 0.0)

        n_items = 4 * pairs
        lead = pairs - 1

        def item(t):
            t = jnp.int32(t)
            u = t - lead
            far = jnp.logical_and(t >= lead, t < n_items - 1)
            turn = u // pairs
            block = jnp.where(far, jnp.where(turn == 0, 1, jnp.where(turn == 1, 3, 2)), 0)
            pair = jnp.where(far, u % pairs, jnp.where(t == n_items - 1, pairs - 1, t))
            return block, pair

        def before(t):
            block, pair = item(t)
            @pl.when(block == 1)
            def _():
                for k in (1, 2):
                    q_wait(l, k, pair)
                    q_relay(l, k, pair).start()

            @pl.when(block == 3)
            def _():
                q_relay_wait(l, pair)

        def put_cross(t, odd, o, top, total):
            block, pair = item(t)
            part_o[block, head_rows(pair, odd), :] = o
            part_st[block, pair * 2 + odd, 0:1, :] = top
            part_st[block, pair * 2 + odd, 1:2, :] = total

        def stage(k, p, odd):
            res_s[l, k, head_rows(p, odd), :] = part_o[k, head_rows(p, odd), :].astype(BF16)
            st_s[l, k, p * 2 + odd] = part_st[k, p * 2 + odd]

        def join(k, p, odd):
            hd = p * 2 + odd
            m1, m2 = part_st[k, hd, 0:1, :], rx_st[l, odd, p, 0:1, :]
            top = jnp.maximum(m1, m2)
            a, b = jnp.exp2(m1 - top), jnp.exp2(m2 - top)
            num = part_o[k, head_rows(p, odd), :] * a + rx_o[l, odd, p].astype(F32) * b
            res_s[l, k, head_rows(p, odd), :] = num.astype(BF16)
            st_s[l, k, hd, 0:1, :] = top
            st_s[l, k, hd, 1:2, :] = part_st[k, hd, 1:2, :] * a + rx_st[l, odd, p, 1:2, :] * b

        def start(copies):
            for cp in copies:
                cp.start()

        def after(t):
            block, pair = item(t)

            @pl.when(block == 1)
            def _():
                stage(1, pair, 0)
                start(r_copies(l, 1, pair, 0))

            @pl.when(block == 3)
            def _():
                for odd in (0, 1):
                    stage(3, pair, odd)
                    start(x_copies(l, odd, pair))

            @pl.when(block == 2)
            def _():
                stage(2, pair, 1)
                start(r_copies(l, 2, pair, 1))
                x_wait(l, 0, pair)
                join(2, pair, 0)
                start(r_copies(l, 2, pair, 0))
                x_wait(l, 1, pair)
                join(1, pair, 1)
                start(r_copies(l, 1, pair, 1))

        with jax.named_scope("cross"):
            attend(CB, CS, lead, item, qc.at[l], kc, vc, mem_all, None, keep, finish, lambda t: None, put_cross, lambda t: None)
            attend(CB, CS, n_items - lead, lambda t: item(t + lead), qc.at[l], kc, vc, mem_all, None, keep, finish,
                   lambda t: before(t + lead), lambda t, *rest: put_cross(t + lead, *rest), lambda t: after(t + lead))

        for k in range(n_h):
            h_copy(l, k).wait_send()
        for p in range(pairs):
            att_copy(l, 0, p).wait_send()
            for k in (1, 2):
                q_copy(l, k, p).wait_send()
                q_relay(l, k, p).wait_send()
        for p in range(pairs):
            with jax.named_scope(f"res_wait{p}"):
                for slot in (1, 2):
                    for odd in (0, 1):
                        r_wait(l, slot, p, odd)
            with jax.named_scope(f"combine{p}"):
                for odd in (0, 1):
                    hs, hd = slice(p * pw + odd * head_dim, p * pw + (odd + 1) * head_dim), p * 2 + odd
                    tops = [part_st[0, hd, 0:1, :]] + [st_r[l, slot, hd, 0:1, :] for slot in (1, 2)]
                    sums = [part_st[0, hd, 1:2, :]] + [st_r[l, slot, hd, 1:2, :] for slot in (1, 2)]
                    nums = [part_o[0, hs, :]] + [res_r[l, slot, hs, :].astype(F32) for slot in (1, 2)]
                    top = functools.reduce(jnp.maximum, tops)
                    scale = [jnp.exp2(t - top) for t in tops]
                    den = sum(s * t for s, t in zip(scale, sums))
                    num = sum(s * t for s, t in zip(scale, nums))
                    att[l, 1, att_rows(p, odd), :] = (num / den).astype(BF16)
                att_copy(l, 1, p).start()
        with jax.named_scope("att1_exchange"):
            w_copy(CO, l).wait()
            w_copy(G, l).wait()
            w_copy(U, l).wait()
            w_copy(DN, l).wait()
            for p in range(pairs):
                att_wait(l, 1, p)
        with jax.named_scope("mlp"):
            y = (ybuf[...].astype(F32) + mm(att[l, 1].T, wco[l])).astype(BF16)
            ybuf[...] = y
            x = rms_norm(y, gain(norm_mlp, l))
            step = 512
            for s in range(ffl // step):
                sl = slice(s * step, (s + 1) * step)
                gate = mm(x, wg[l, :, sl])
                act[:, sl] = (jax.nn.silu(gate) * mm(x, wu[l, :, sl])).astype(BF16)

            def down(i, cc):
                core = jnp.where(i == 0, 1 - h, h)
                mlp_s[l, i] = mm(act[pl.ds(pl.multiple_of(core * rows, rows), rows), :], wd[l])

                @pl.when(i == 0)
                def _():
                    mlp_copy(l).start()

                return cc

            lax.fori_loop(0, 2, down, 0)
        for p in range(pairs):
            att_copy(l, 1, p).wait_send()
            for odd in (0, 1):
                for cp in r_copies(l, 1, p, odd) + r_copies(l, 2, p, odd) + x_copies(l, odd, p):
                    cp.wait_send()
        with jax.named_scope("mlp_exchange"):
            mlp_copy(l).wait_recv()
            hbuf[l + 1, 0, my_rows, :] = (ybuf[my_rows, :].astype(F32) + (mlp_s[l, 1] + mlp_r[l])).astype(BF16)
        return carry

    lax.fori_loop(0, layers, layer, 0)
    out_cp = pltpu.make_async_copy(hbuf.at[layers, 0, my_rows], out, l_sem.at[2])
    out_cp.start()

    for cp in mem_send:
        cp.wait_send()

    for l in range(layers):
        mlp_copy(l).wait_send()
    out_cp.wait()


def solution(mesh):
    group = mesh.shape["sp"]
    n_chips = group // 2
    row_spec = P(("dp", "sp"), None)

    def local_step(hidden, memory, mem_len, norm_self, norm_cross, norm_mlp, self_q, self_k, self_v, self_o, cross_q, cross_k, cross_v, cross_o, mlp_gate, mlp_up, mlp_down):
        rows, width = hidden.shape
        mem_rows = memory.shape[0]
        layers, heads, head_dim = self_o.shape[:3]
        ffl = mlp_gate.shape[2] // 2
        half_w = width // 2
        hl = heads // 2
        pairs = hl // 2
        T = 2 * rows
        mem_all = 2 * mem_rows
        wso = self_o.reshape(layers, heads * head_dim, width)
        wco = cross_o.reshape(layers, heads * head_dim, width)
        dims = (n_chips, layers, rows, width, heads, head_dim, mem_rows, ffl)
        dma = pltpu.SemaphoreType.DMA
        anyspace = pl.BlockSpec(memory_space=pl.ANY)
        call = pl.pallas_call(
            functools.partial(decoder_kernel, dims),
            out_shape=jax.ShapeDtypeStruct(hidden.shape, BF16),
            in_specs=[anyspace] * 17,
            out_specs=anyspace,
            scratch_shapes=[
                pltpu.VMEM((layers, width, half_w), BF16),
                pltpu.VMEM((layers, width, half_w), BF16),
                pltpu.VMEM((layers, width, half_w), BF16),
                pltpu.VMEM((layers, width, width), BF16),
                pltpu.VMEM((layers, width, half_w), BF16),
                pltpu.VMEM((layers, width, half_w), BF16),
                pltpu.VMEM((layers, width, half_w), BF16),
                pltpu.VMEM((layers, width, width), BF16),
                pltpu.VMEM((layers, width, ffl), BF16),
                pltpu.VMEM((layers, width, ffl), BF16),
                pltpu.VMEM((layers, ffl, width), BF16),
                pltpu.VMEM((layers, width), BF16),
                pltpu.VMEM((layers, width), BF16),
                pltpu.VMEM((layers, width), BF16),
                pltpu.SMEM((1,), jnp.int32),
                pltpu.VMEM((layers + 1, n_chips, T, width), BF16),
                pltpu.VMEM((2, mem_rows, width), BF16),
                pltpu.VMEM((T, width), BF16),
                pltpu.VMEM((half_w, width), BF16),
                pltpu.VMEM((1, half_w, T), BF16),
                pltpu.VMEM((pairs, n_chips * T, 128), BF16),
                pltpu.VMEM((hl, n_chips * T // 128, head_dim, 128), BF16),
                pltpu.VMEM((pairs, mem_all, 128), BF16),
                pltpu.VMEM((hl, mem_all // 128, head_dim, 128), BF16),
                pltpu.VMEM((layers, 4, half_w, T), BF16),
                pltpu.VMEM((mem_all, T), F32),
                pltpu.VMEM((mem_all, T), F32),
                pltpu.VMEM((hl, n_chips * T, T), F32),
                pltpu.VMEM((hl, 8, T), F32),
                pltpu.VMEM((4, half_w, T), F32),
                pltpu.VMEM((4, hl, 2, T), F32),
                pltpu.VMEM((layers, 4, half_w, T), BF16),
                pltpu.VMEM((layers, 4, hl, 2, T), F32),
                pltpu.VMEM((layers, 3, half_w, T), BF16),
                pltpu.VMEM((layers, 3, hl, 2, T), F32),
                pltpu.VMEM((layers, 2, pairs, head_dim, T), BF16),
                pltpu.VMEM((layers, 2, pairs, 2, T), F32),
                pltpu.VMEM((layers, 2, width, T), BF16),
                pltpu.VMEM((T, ffl), BF16),
                pltpu.VMEM((layers, 2, rows, width), F32),
                pltpu.VMEM((layers, rows, width), F32),
                dma((layers, 11)),
                dma((7,)),
                dma((11,)), dma((layers, 11)),
                dma((2,)), dma((2,)),
                dma((2, pairs)), dma((layers, 2, pairs)),
                dma((5, pairs)), dma((layers, 5, pairs)),
                dma((8, pairs)), dma((layers, 8, pairs)),
                dma((4, pairs)), dma((layers, 4, pairs)),
                dma((layers,)), dma((layers,)),
            ],
            compiler_params=pltpu.CompilerParams(collective_id=0, has_side_effects=True, vmem_limit_bytes=67043328),
            name="decoder",
        )
        return call(hidden, memory, mem_len, norm_self, norm_cross, norm_mlp, self_q, self_k, self_v, wso, cross_q, cross_k, cross_v, wco, mlp_gate, mlp_up, mlp_down)

    return jax.shard_map(local_step, mesh=mesh, in_specs=(row_spec, row_spec, P("dp")) + (P(),) * 14, out_specs=row_spec, check_vma=False)
```

```python
import functools

import jax
import jax.numpy as jnp
from jax import lax
from jax.experimental import pallas as pl
from jax.experimental.pallas import tpu as pltpu
from jax.sharding import PartitionSpec as P

EPS = 1e-6
NEG_BIG = -1e30
LOG2E = 1.4426950408889634
F32 = jnp.float32
BF16 = jnp.bfloat16
CB, CS = 1024, 512
MESH = pl.DeviceIdType.MESH


def rms_norm(hidden, gain_vec):
    hidden32 = hidden.astype(F32)
    inv_rms = lax.rsqrt(jnp.mean(hidden32 * hidden32, axis=-1, keepdims=True) + EPS)
    return (hidden32 * inv_rms * gain_vec.astype(F32)).astype(BF16)


def mm(a, b):
    return jnp.dot(a, b, preferred_element_type=F32)


def mm_nt(a, b):
    return lax.dot_general(a, b, (((1,), (1,)), ((), ())), preferred_element_type=F32)


def decoder_kernel(dims, *refs):
    (n_chips, layers, rows, width, heads, head_dim, mem_rows, ffl) = dims
    (hid_in, mem_in, len_in, ns_in, nc_in, nm_in,
     w_sq, w_sk, w_sv, w_so, w_cq, w_ck, w_cv, w_co, w_g, w_u, w_d, out,
     wsq, wsk, wsv, wso, wcq, wck, wcv, wco, wg, wu, wd, norm_self, norm_cross, norm_mlp, mem_len,
     hbuf, mbuf, ybuf, wvt, qself, kself, vself, kc, vc, qc, s_even, s_odd, s_self, t_self,
     part_o, part_st, res_s, st_s, res_r, st_r, rx_o, rx_st, att, act, mlp_s, mlp_r,
     w_sem, l_sem, h_ss, h_rs, m_ss, m_rs, a_ss, a_rs, q_ss, q_rs, r_ss, r_rs, x_ss, x_rs, f_ss, f_rs) = refs
    T = 2 * rows
    half_w = width // 2
    hl = heads // 2
    pairs = hl // 2
    half = rows // 2
    pw = 2 * head_dim
    mem_all = 2 * mem_rows
    exp_c = head_dim ** -0.5 * LOG2E
    neg = NEG_BIG * LOG2E

    me = lax.axis_index("sp")
    c = me // 2
    h = me % 2
    sib = c * 2 + (1 - h)

    def peer(step):
        return lax.rem(c + step, n_chips) * 2 + h

    right, left, across = peer(1), peer(n_chips - 1), peer(2)
    chip_of = (c, lax.rem(c + n_chips - 1, n_chips), lax.rem(c + 1, n_chips), lax.rem(c + 2, n_chips))

    def remote(src, dst, ss, rs, dev):
        return pltpu.make_async_remote_copy(src_ref=src, dst_ref=dst, send_sem=ss, recv_sem=rs,
                                            device_id={"sp": dev}, device_id_type=MESH)

    def piece(core, part):
        return pl.ds(pl.multiple_of(core * rows + part * half, half), half)

    my_rows = pl.ds(pl.multiple_of(h * rows, rows), rows)
    sib_rows = pl.ds(pl.multiple_of((1 - h) * rows, rows), rows)
    my_cols = pl.ds(pl.multiple_of(h * half_w, 128), half_w)
    my_ff = pl.ds(pl.multiple_of(h * ffl, 128), ffl)

    plans = (
        (w_ck, wck, "c"), (w_cv, wcv, "c"), (w_sk, wsk, "c"), (w_sv, wsv, "c"), (w_sq, wsq, "c"), (w_so, wso, "f"),
        (w_cq, wcq, "c"), (w_co, wco, "f"), (w_g, wg, "m"), (w_u, wu, "m"), (w_d, wd, "r"),
    )
    CK, CV, SK, SV, SQ, SO, CQ, CO, G, U, DN = range(11)

    def w_copy(k, l):
        src, dst, kind = plans[k]
        if kind == "c":
            s = src.at[l, :, my_cols]
        elif kind == "m":
            s = src.at[l, :, my_ff]
        elif kind == "r":
            s = src.at[l, my_ff]
        else:
            s = src.at[l]
        return pltpu.make_async_copy(s, dst.at[l], w_sem.at[l, k])

    hid_cp = pltpu.make_async_copy(hid_in, hbuf.at[0, 0, my_rows], l_sem.at[0])
    mem_cp = pltpu.make_async_copy(mem_in, mbuf.at[0], l_sem.at[1])
    small = [pltpu.make_async_copy(s, d, l_sem.at[3 + i]) for i, (s, d) in enumerate(
        ((ns_in, norm_self), (nc_in, norm_cross), (nm_in, norm_mlp), (len_in, mem_len)))]
    hid_cp.start()
    mem_cp.start()
    w_copy(CK, 0).start()
    w_copy(CV, 0).start()
    for cp in small:
        cp.start()

    barrier = pltpu.get_barrier_semaphore()
    for dev in (sib, right, left, across):
        pl.semaphore_signal(barrier, inc=1, device_id={"sp": dev}, device_id_type=MESH)
    pl.semaphore_wait(barrier, 4)

    h_plan = (
        (0, 0, None, sib),
        (0, 1, 0, right), (0, 2, 1, left), (0, 1, 1, right), (0, 2, 0, left),
        (1, 3, 0, right), (2, 3, 1, left),
        (1, 1, None, sib), (2, 2, None, sib), (3, 3, 0, sib), (3, 3, 1, sib),
    )
    n_h = len(h_plan)

    def h_copy(l, k):
        s, d, part, dev = h_plan[k]
        rr = my_rows if part is None else piece(h, part)
        return remote(hbuf.at[l, s, rr], hbuf.at[l, d, rr], h_ss.at[k], h_rs.at[l, k], dev)

    def h_wait(l, k):
        s, d, part, dev = h_plan[k]
        core = 1 - h if k in (0, 7, 8, 9, 10) else h
        rr = pl.ds(pl.multiple_of(core * rows, rows), rows) if part is None else piece(core, part)
        ref = hbuf.at[l, d, rr]
        remote(ref, ref, h_ss.at[k], h_rs.at[l, k], sib).wait_recv()

    mem_cut = (pl.ds(0, 16), pl.ds(16, mem_rows - 16))
    mem_send = [remote(mbuf.at[0, rr], mbuf.at[1, rr], m_ss.at[i], m_rs.at[i], sib) for i, rr in enumerate(mem_cut)]

    def att_copy(l, k, p):
        ref = att.at[l, k, pl.ds(pl.multiple_of(h * half_w + p * pw, pw), pw)]
        return remote(ref, ref, a_ss.at[k, p], a_rs.at[l, k, p], sib)

    def att_wait(l, k, p):
        ref = att.at[l, k, pl.ds(pl.multiple_of((1 - h) * half_w + p * pw, pw), pw)]
        remote(ref, ref, a_ss.at[k, p], a_rs.at[l, k, p], sib).wait_recv()

    def pair_rows(p):
        return pl.ds(pl.multiple_of(p * pw, pw), pw)

    def q_copy(l, k, p):
        dev = (None, right, left)[k]
        return remote(qc.at[l, 0, pair_rows(p)], qc.at[l, k, pair_rows(p)], q_ss.at[k, p], q_rs.at[l, k, p], dev)

    def q_relay(l, k, p):
        rr = pl.ds(pl.multiple_of(p * pw + (k - 1) * head_dim, head_dim), head_dim)
        dev = (None, right, left)[k]
        return remote(qc.at[l, k, rr], qc.at[l, 3, rr], q_ss.at[2 + k, p], q_rs.at[l, 2 + k, p], dev)

    def q_relay_wait(l, p):
        for k in (1, 2):
            rr = pl.ds(pl.multiple_of(p * pw + (k - 1) * head_dim, head_dim), head_dim)
            ref = qc.at[l, 3, rr]
            remote(ref, ref, q_ss.at[2 + k, p], q_rs.at[l, 2 + k, p], sib).wait_recv()

    def q_wait(l, k, p):
        ref = qc.at[l, k, pair_rows(p)]
        remote(ref, ref, q_ss.at[k, p], q_rs.at[l, k, p], sib).wait_recv()

    def head_rows(p, odd):
        return pl.ds(pl.multiple_of(p * pw + odd * head_dim, head_dim), head_dim)

    def r_copies(l, k, p, odd):
        slot, dev = ((2, left), (1, right))[k - 1]
        rr, hd = head_rows(p, odd), p * 2 + odd
        a, b = (k - 1) * 2 + odd, (slot - 1) * 2 + odd
        return (remote(res_s.at[l, k, rr], res_r.at[l, slot, rr], r_ss.at[a, p], r_rs.at[l, b, p], dev),
                remote(st_s.at[l, k, hd], st_r.at[l, slot, hd], r_ss.at[4 + a, p], r_rs.at[l, 4 + b, p], dev))

    def r_wait(l, slot, p, odd):
        a, b = res_r.at[l, slot, head_rows(p, odd)], st_r.at[l, slot, p * 2 + odd]
        i = (slot - 1) * 2 + odd
        remote(a, a, r_ss.at[i, p], r_rs.at[l, i, p], sib).wait_recv()
        remote(b, b, r_ss.at[4 + i, p], r_rs.at[l, 4 + i, p], sib).wait_recv()

    def x_copies(l, odd, p):
        dev = (right, left)[odd]
        return (remote(res_s.at[l, 3, head_rows(p, odd)], rx_o.at[l, odd, p], x_ss.at[odd, p], x_rs.at[l, odd, p], dev),
                remote(st_s.at[l, 3, p * 2 + odd], rx_st.at[l, odd, p], x_ss.at[2 + odd, p], x_rs.at[l, 2 + odd, p], dev))

    def x_wait(l, odd, p):
        a, b = rx_o.at[l, odd, p], rx_st.at[l, odd, p]
        remote(a, a, x_ss.at[odd, p], x_rs.at[l, odd, p], sib).wait_recv()
        remote(b, b, x_ss.at[2 + odd, p], x_rs.at[l, 2 + odd, p], sib).wait_recv()

    def mlp_copy(l):
        return remote(mlp_s.at[l, 0], mlp_r.at[l], f_ss.at[l], f_rs.at[l], sib)

    def split_rhs(q, odd):
        q = q.astype(F32) * exp_c
        hi = q.astype(BF16)
        lo = (q - hi.astype(F32)).astype(BF16)
        z = jnp.zeros_like(hi)
        return jnp.concatenate([z, hi, z, lo] if odd else [hi, z, lo, z], axis=0)

    def attend(BIG, SMALL, items, item, qref, kref, vref, nk, allowed, keep, finish, before, put, after):
        def rhs_of(t, odd):
            block, pair = item(t)
            start = pl.multiple_of(pair * pw + odd * head_dim, head_dim)
            return split_rhs(qref[block, pl.ds(start, head_dim), :], odd)

        def score(pair, rhs, s_ref, j, top):
            k = kref[pair, j * BIG:(j + 1) * BIG, :]
            s = mm(jnp.concatenate([k, k], axis=1), rhs)
            if allowed is not None:
                s = jnp.where(allowed(j * BIG, BIG), s, neg)
            s_ref[j * BIG:(j + 1) * BIG, :] = s
            t = jnp.max(s.reshape(BIG // 8, 8, T), axis=0)
            return t if top is None else jnp.maximum(top, t)

        def accumulate(head, s_ref, j, top, total, o):
            p = jnp.exp2(s_ref[j * SMALL:(j + 1) * SMALL, :] - top)
            t = jnp.sum(p.reshape(SMALL // 8, 8, T), axis=0)
            if keep is not None:
                t = t * keep(j * SMALL, SMALL)
            vt = jnp.concatenate([vref[head, j * (SMALL // 128) + i] for i in range(SMALL // 128)], axis=1)
            v = mm(vt, p.astype(BF16))
            return (t, v) if total is None else (total + t, o + v)

        def step(nxt, nxt_odd, nxt_ref, cur, cur_odd, cur_ref, cur_top):
            rhs = rhs_of(nxt, nxt_odd)
            nxt_pair = item(nxt)[1]
            head = item(cur)[1] * 2 + cur_odd
            top = total = o = None
            for j in range(nk // BIG):
                top = score(nxt_pair, rhs, nxt_ref, j, top)
                for i in range(BIG // SMALL):
                    total, o = accumulate(head, cur_ref, j * (BIG // SMALL) + i, cur_top, total, o)
            total = jnp.sum(total, axis=0, keepdims=True)
            if finish is not None:
                cur_top, total = finish(cur_ref, cur_top, total)
            put(cur, cur_odd, o, cur_top, total)
            return jnp.max(top, axis=0, keepdims=True)

        before(0)
        rhs0 = rhs_of(0, 0)
        top = None
        for j in range(nk // BIG):
            top = score(item(0)[1], rhs0, s_even, j, top)
        top = jnp.max(top, axis=0, keepdims=True)

        def body(t, top_even):
            last = t == items - 1
            nxt = jnp.where(last, t, t + 1)

            @pl.when(jnp.logical_not(last))
            def _():
                before(t + 1)

            top_odd = step(t, 1, s_odd, t, 0, s_even, top_even)
            top_next = step(nxt, 0, s_even, t, 1, s_odd, top_odd)
            after(t)
            return top_next

        lax.fori_loop(0, items, body, top)

    def gain(ref, l):
        g = ref[0:1, :].astype(F32)
        for i in range(1, layers):
            g = jnp.where(l == i, ref[i:i + 1, :].astype(F32), g)
        return g

    def store_kv(kref, vref, row0, tile0, k, v, n):
        for p in range(pairs):
            kref[p, pl.ds(row0, n), :] = k[:, p * pw:(p + 1) * pw]
        v = v.reshape(hl, head_dim, n)
        for i in range(n // 128):
            vref[:, pl.ds(tile0 + i, 1)] = v[:, None, :, i * 128:(i + 1) * 128]

    def layer(l, carry):
        first = l == 0
        with jax.named_scope("gather_send"):
            @pl.when(first)
            def _():
                hid_cp.wait()

            for k in range(5):
                h_copy(l, k).start()

            @pl.when(first)
            def _():
                mem_cp.wait()
                for cp in mem_send:
                    cp.start()
                for l0 in range(layers):
                    for k in range(len(plans)):
                        if l0 > 0 or k > CV:
                            w_copy(k, l0).start()

        with jax.named_scope("w_wait"):
            w_copy(CK, l).wait()
            w_copy(CV, l).wait()
            wvt[...] = wcv[l].T

        blk = 512

        def mem_proj(part):
            core = h if part == 0 else 1 - h

            def body(b, cc):
                r0 = pl.multiple_of(b * blk, blk)
                m = mbuf[part, pl.ds(r0, blk), :]
                left_valid = limit - ((2 * c + core) * mem_rows + b * blk)
                m = jnp.where(lax.broadcasted_iota(jnp.int32, (blk, width), 0) < left_valid, m, mbuf[h, 0:1, :])
                k = mm(m, wck[l]).astype(BF16)
                v = mm_nt(wvt[...], m)
                v = jnp.where(lax.broadcasted_iota(jnp.int32, (half_w, blk), 1) < left_valid, v, 0.0).astype(BF16)
                d0 = pl.multiple_of(part * mem_rows + b * blk, blk)
                store_kv(kc, vc, d0, (part * mem_rows + b * blk) // 128, k, v, blk)
                return cc

            lax.fori_loop(0, mem_rows // blk, body, 0)

        with jax.named_scope("mem_wait"):
            @pl.when(first)
            def _():
                mem_send[0].wait_recv()
                for cp in small:
                    cp.wait()

        limit = mem_len[0]
        with jax.named_scope("mem_proj0"):
            mem_proj(0)

        with jax.named_scope("mem_wait1"):
            @pl.when(first)
            def _():
                mem_send[1].wait_recv()

        with jax.named_scope("mem_proj1"):
            mem_proj(1)

        def self_proj(r, with_q):
            x = rms_norm(hbuf[l, r], gain(norm_self, l))
            if r > 0:
                x = jnp.where(chip_of[r] > c, rms_norm(hbuf[l, 0, 0:1, :], gain(norm_self, l)), x)
            k = mm(x, wsk[l]).astype(BF16)
            v = mm_nt(wvt[...], x)
            if r > 0:
                v = jnp.where(chip_of[r] > c, 0.0, v)
            v = v.astype(BF16)
            store_kv(kself, vself, r * T, r * (T // 128), k, v, T)
            if with_q:
                qself[0] = mm(x, wsq[l]).astype(BF16).T

        with jax.named_scope("gather_wait1"):
            for k in (SK, SV, SQ):
                w_copy(k, l).wait()
            wvt[...] = wsv[l].T
            h_wait(l, 1)
            h_copy(l, 5).start()
            h_wait(l, 2)
            h_copy(l, 6).start()
            h_wait(l, 0)
        with jax.named_scope("self_proj0"):
            self_proj(0, True)
        with jax.named_scope("gather_wait2"):
            h_wait(l, 3)
            h_copy(l, 7).start()
            h_wait(l, 4)
            h_copy(l, 8).start()
            h_wait(l, 7)
        with jax.named_scope("self_proj1"):
            self_proj(1, False)
            h_wait(l, 8)
            self_proj(2, False)
        def self_rhs(hd):
            return split_rhs(qself[0, hd * head_dim:(hd + 1) * head_dim, :], hd % 2)

        def self_score(hd, rhs, r):
            k = kself[hd // 2, r * T:(r + 1) * T, :]
            sc = mm(jnp.concatenate([k, k], axis=1), rhs)
            if r == 0:
                kio = lax.broadcasted_iota(jnp.int32, (T, T), 0)
                qio = lax.broadcasted_iota(jnp.int32, (T, T), 1)
                sc = jnp.where(kio <= qio, sc, neg)
            s_self[hd, r * T:(r + 1) * T, :] = sc
            return jnp.max(sc.reshape(T // 8, 8, T), axis=0)

        with jax.named_scope("self_score"):
            for hd in range(hl):
                rhs = self_rhs(hd)
                t_self[hd] = functools.reduce(jnp.maximum, [self_score(hd, rhs, r) for r in (0, 1, 2)])
        with jax.named_scope("gather_wait3"):
            h_wait(l, 5)
            h_copy(l, 9).start()
            h_wait(l, 6)
            h_copy(l, 10).start()
            h_wait(l, 9)
            h_wait(l, 10)
        with jax.named_scope("self_proj3"):
            self_proj(3, False)

        def att_rows(t, odd):
            return pl.ds(pl.multiple_of(h * half_w + t * pw + odd * head_dim, head_dim), head_dim)

        with jax.named_scope("self_attend"):
            seen = [None] + [jnp.where(chip_of[r] > c, 0.0, 1.0).astype(F32) for r in (1, 2, 3)]

            def self_top(hd):
                top = jnp.maximum(t_self[hd], self_score(hd, self_rhs(hd), 3))
                return jnp.max(top, axis=0, keepdims=True)

            top = self_top(0)
            for hd in range(hl):
                ahead = self_top(hd + 1) if hd + 1 < hl else None
                total = o = None
                for r in range(n_chips):
                    p = jnp.exp2(s_self[hd, r * T:(r + 1) * T, :] - top)
                    t = jnp.sum(p.reshape(T // 8, 8, T), axis=0)
                    if r > 0:
                        t = t * seen[r]
                    v = mm(jnp.concatenate([vself[hd, r * (T // 128) + i] for i in range(T // 128)], axis=1), p.astype(BF16))
                    total, o = (t, v) if total is None else (total + t, o + v)
                total = jnp.sum(total, axis=0, keepdims=True)
                att[l, 0, att_rows(hd // 2, hd % 2), :] = (o / total).astype(BF16)
                top = ahead
            for p in range(pairs):
                att_copy(l, 0, p).start()
        with jax.named_scope("att0_exchange"):
            w_copy(SO, l).wait()
            w_copy(CQ, l).wait()
            for p in range(pairs):
                att_wait(l, 0, p)
        with jax.named_scope("self_o_q"):
            y = (hbuf[l, 0].astype(F32) + mm(att[l, 0].T, wso[l])).astype(BF16)
            ybuf[...] = y
            x = rms_norm(y, gain(norm_cross, l))
            qc[l, 0] = mm(x, wcq[l]).astype(BF16).T
            for p in range(pairs):
                for k in (1, 2):
                    q_copy(l, k, p).start()

        def invalid_in(start, size):
            core = h if start < mem_rows else 1 - h
            end = (2 * c + core) * mem_rows + start % mem_rows + size
            return jnp.clip(end - limit, 0, size)

        def keep(start, size):
            return jnp.where(invalid_in(start, size) < size, 1.0, 0.0).astype(F32)

        extra = jnp.int32(0)
        for start in range(0, mem_all, CS):
            bad = invalid_in(start, CS)
            extra = extra + jnp.where(bad < CS, bad, 0)
        extra = extra.astype(F32)
        any_valid = 2 * c * mem_rows < limit

        def finish(s_ref, top, total):
            first_row = s_ref[pl.ds(pl.multiple_of(h * mem_rows, 8), 1), :]
            total = total - extra * jnp.exp2(first_row - top)
            return jnp.where(any_valid, top, neg), jnp.where(any_valid, total, 0.0)

        n_items = 4 * pairs
        lead = pairs - 1

        def item(t):
            t = jnp.int32(t)
            u = t - lead
            far = jnp.logical_and(t >= lead, t < n_items - 1)
            turn = u // pairs
            block = jnp.where(far, jnp.where(turn == 0, 1, jnp.where(turn == 1, 3, 2)), 0)
            pair = jnp.where(far, u % pairs, jnp.where(t == n_items - 1, pairs - 1, t))
            return block, pair

        def before(t):
            block, pair = item(t)
            @pl.when(block == 1)
            def _():
                for k in (1, 2):
                    q_wait(l, k, pair)
                    q_relay(l, k, pair).start()

            @pl.when(block == 3)
            def _():
                q_relay_wait(l, pair)

        def put_cross(t, odd, o, top, total):
            block, pair = item(t)
            part_o[block, head_rows(pair, odd), :] = o
            part_st[block, pair * 2 + odd, 0:1, :] = top
            part_st[block, pair * 2 + odd, 1:2, :] = total

        def stage(k, p, odd):
            res_s[l, k, head_rows(p, odd), :] = part_o[k, head_rows(p, odd), :].astype(BF16)
            st_s[l, k, p * 2 + odd] = part_st[k, p * 2 + odd]

        def join(k, p, odd):
            hd = p * 2 + odd
            m1, m2 = part_st[k, hd, 0:1, :], rx_st[l, odd, p, 0:1, :]
            top = jnp.maximum(m1, m2)
            a, b = jnp.exp2(m1 - top), jnp.exp2(m2 - top)
            num = part_o[k, head_rows(p, odd), :] * a + rx_o[l, odd, p].astype(F32) * b
            res_s[l, k, head_rows(p, odd), :] = num.astype(BF16)
            st_s[l, k, hd, 0:1, :] = top
            st_s[l, k, hd, 1:2, :] = part_st[k, hd, 1:2, :] * a + rx_st[l, odd, p, 1:2, :] * b

        def start(copies):
            for cp in copies:
                cp.start()

        def after(t):
            block, pair = item(t)

            @pl.when(block == 1)
            def _():
                stage(1, pair, 0)
                start(r_copies(l, 1, pair, 0))

            @pl.when(block == 3)
            def _():
                for odd in (0, 1):
                    stage(3, pair, odd)
                    start(x_copies(l, odd, pair))

            @pl.when(block == 2)
            def _():
                stage(2, pair, 1)
                start(r_copies(l, 2, pair, 1))
                x_wait(l, 0, pair)
                join(2, pair, 0)
                start(r_copies(l, 2, pair, 0))
                x_wait(l, 1, pair)
                join(1, pair, 1)
                start(r_copies(l, 1, pair, 1))

        with jax.named_scope("cross"):
            attend(CB, CS, lead, item, qc.at[l], kc, vc, mem_all, None, keep, finish, lambda t: None, put_cross, lambda t: None)
            attend(CB, CS, n_items - lead, lambda t: item(t + lead), qc.at[l], kc, vc, mem_all, None, keep, finish,
                   lambda t: before(t + lead), lambda t, *rest: put_cross(t + lead, *rest), lambda t: after(t + lead))

        for k in range(n_h):
            h_copy(l, k).wait_send()
        for p in range(pairs):
            att_copy(l, 0, p).wait_send()
            for k in (1, 2):
                q_copy(l, k, p).wait_send()
                q_relay(l, k, p).wait_send()
        for p in range(pairs):
            with jax.named_scope(f"res_wait{p}"):
                for slot in (1, 2):
                    for odd in (0, 1):
                        r_wait(l, slot, p, odd)
            with jax.named_scope(f"combine{p}"):
                for odd in (0, 1):
                    hs, hd = slice(p * pw + odd * head_dim, p * pw + (odd + 1) * head_dim), p * 2 + odd
                    tops = [part_st[0, hd, 0:1, :]] + [st_r[l, slot, hd, 0:1, :] for slot in (1, 2)]
                    sums = [part_st[0, hd, 1:2, :]] + [st_r[l, slot, hd, 1:2, :] for slot in (1, 2)]
                    nums = [part_o[0, hs, :]] + [res_r[l, slot, hs, :].astype(F32) for slot in (1, 2)]
                    top = functools.reduce(jnp.maximum, tops)
                    scale = [jnp.exp2(t - top) for t in tops]
                    den = sum(s * t for s, t in zip(scale, sums))
                    num = sum(s * t for s, t in zip(scale, nums))
                    att[l, 1, att_rows(p, odd), :] = (num / den).astype(BF16)
                att_copy(l, 1, p).start()
        with jax.named_scope("att1_exchange"):
            w_copy(CO, l).wait()
            w_copy(G, l).wait()
            w_copy(U, l).wait()
            w_copy(DN, l).wait()
            for p in range(pairs):
                att_wait(l, 1, p)
        with jax.named_scope("mlp"):
            y = (ybuf[...].astype(F32) + mm(att[l, 1].T, wco[l])).astype(BF16)
            ybuf[...] = y
            x = rms_norm(y, gain(norm_mlp, l))
            step = 512
            for s in range(ffl // step):
                sl = slice(s * step, (s + 1) * step)
                gate = mm(x, wg[l, :, sl])
                act[:, sl] = (jax.nn.silu(gate) * mm(x, wu[l, :, sl])).astype(BF16)

            def down(i, cc):
                core = jnp.where(i == 0, 1 - h, h)
                mlp_s[l, i] = mm(act[pl.ds(pl.multiple_of(core * rows, rows), rows), :], wd[l])

                @pl.when(i == 0)
                def _():
                    mlp_copy(l).start()

                return cc

            lax.fori_loop(0, 2, down, 0)
        for p in range(pairs):
            att_copy(l, 1, p).wait_send()
            for odd in (0, 1):
                for cp in r_copies(l, 1, p, odd) + r_copies(l, 2, p, odd) + x_copies(l, odd, p):
                    cp.wait_send()
        with jax.named_scope("mlp_exchange"):
            mlp_copy(l).wait_recv()
            hbuf[l + 1, 0, my_rows, :] = (ybuf[my_rows, :].astype(F32) + (mlp_s[l, 1] + mlp_r[l])).astype(BF16)
        return carry

    lax.fori_loop(0, layers, layer, 0)
    out_cp = pltpu.make_async_copy(hbuf.at[layers, 0, my_rows], out, l_sem.at[2])
    out_cp.start()

    for cp in mem_send:
        cp.wait_send()

    for l in range(layers):
        mlp_copy(l).wait_send()
    out_cp.wait()


def solution(mesh):
    group = mesh.shape["sp"]
    n_chips = group // 2
    row_spec = P(("dp", "sp"), None)

    def local_step(hidden, memory, mem_len, norm_self, norm_cross, norm_mlp, self_q, self_k, self_v, self_o, cross_q, cross_k, cross_v, cross_o, mlp_gate, mlp_up, mlp_down):
        rows, width = hidden.shape
        mem_rows = memory.shape[0]
        layers, heads, head_dim = self_o.shape[:3]
        ffl = mlp_gate.shape[2] // 2
        half_w = width // 2
        hl = heads // 2
        pairs = hl // 2
        T = 2 * rows
        mem_all = 2 * mem_rows
        wso = self_o.reshape(layers, heads * head_dim, width)
        wco = cross_o.reshape(layers, heads * head_dim, width)
        dims = (n_chips, layers, rows, width, heads, head_dim, mem_rows, ffl)
        dma = pltpu.SemaphoreType.DMA
        anyspace = pl.BlockSpec(memory_space=pl.ANY)
        call = pl.pallas_call(
            functools.partial(decoder_kernel, dims),
            out_shape=jax.ShapeDtypeStruct(hidden.shape, BF16),
            in_specs=[anyspace] * 17,
            out_specs=anyspace,
            scratch_shapes=[
                pltpu.VMEM((layers, width, half_w), BF16),
                pltpu.VMEM((layers, width, half_w), BF16),
                pltpu.VMEM((layers, width, half_w), BF16),
                pltpu.VMEM((layers, width, width), BF16),
                pltpu.VMEM((layers, width, half_w), BF16),
                pltpu.VMEM((layers, width, half_w), BF16),
                pltpu.VMEM((layers, width, half_w), BF16),
                pltpu.VMEM((layers, width, width), BF16),
                pltpu.VMEM((layers, width, ffl), BF16),
                pltpu.VMEM((layers, width, ffl), BF16),
                pltpu.VMEM((layers, ffl, width), BF16),
                pltpu.VMEM((layers, width), BF16),
                pltpu.VMEM((layers, width), BF16),
                pltpu.VMEM((layers, width), BF16),
                pltpu.SMEM((1,), jnp.int32),
                pltpu.VMEM((layers + 1, n_chips, T, width), BF16),
                pltpu.VMEM((2, mem_rows, width), BF16),
                pltpu.VMEM((T, width), BF16),
                pltpu.VMEM((half_w, width), BF16),
                pltpu.VMEM((1, half_w, T), BF16),
                pltpu.VMEM((pairs, n_chips * T, 128), BF16),
                pltpu.VMEM((hl, n_chips * T // 128, head_dim, 128), BF16),
                pltpu.VMEM((pairs, mem_all, 128), BF16),
                pltpu.VMEM((hl, mem_all // 128, head_dim, 128), BF16),
                pltpu.VMEM((layers, 4, half_w, T), BF16),
                pltpu.VMEM((mem_all, T), F32),
                pltpu.VMEM((mem_all, T), F32),
                pltpu.VMEM((hl, n_chips * T, T), F32),
                pltpu.VMEM((hl, 8, T), F32),
                pltpu.VMEM((4, half_w, T), F32),
                pltpu.VMEM((4, hl, 2, T), F32),
                pltpu.VMEM((layers, 4, half_w, T), BF16),
                pltpu.VMEM((layers, 4, hl, 2, T), F32),
                pltpu.VMEM((layers, 3, half_w, T), BF16),
                pltpu.VMEM((layers, 3, hl, 2, T), F32),
                pltpu.VMEM((layers, 2, pairs, head_dim, T), BF16),
                pltpu.VMEM((layers, 2, pairs, 2, T), F32),
                pltpu.VMEM((layers, 2, width, T), BF16),
                pltpu.VMEM((T, ffl), BF16),
                pltpu.VMEM((layers, 2, rows, width), F32),
                pltpu.VMEM((layers, rows, width), F32),
                dma((layers, 11)),
                dma((7,)),
                dma((11,)), dma((layers, 11)),
                dma((2,)), dma((2,)),
                dma((2, pairs)), dma((layers, 2, pairs)),
                dma((5, pairs)), dma((layers, 5, pairs)),
                dma((8, pairs)), dma((layers, 8, pairs)),
                dma((4, pairs)), dma((layers, 4, pairs)),
                dma((layers,)), dma((layers,)),
            ],
            compiler_params=pltpu.CompilerParams(collective_id=0, has_side_effects=True, vmem_limit_bytes=67043328),
            name="decoder",
        )
        return call(hidden, memory, mem_len, norm_self, norm_cross, norm_mlp, self_q, self_k, self_v, wso, cross_q, cross_k, cross_v, wco, mlp_gate, mlp_up, mlp_down)

    return jax.shard_map(local_step, mesh=mesh, in_specs=(row_spec, row_spec, P("dp")) + (P(),) * 14, out_specs=row_spec, check_vma=False)
```
